256 devices in a mesh: groups: 2 (over y), tensor: 128 (over x, z, core).
Axes of the slice: x: 4, y: 2, z: 16, core: 2. Of those that a mesh axis runs over, the one named last changes fastest.
The devices are a block of a 4x16x16 slice.
Arguments:
- hidden_in: bfloat16 [32, 16384], P('groups', 'tensor'), parts along dimension 0, may hold values from -0.59765625 to 0.59765625
- norm_gain: bfloat16 [16384], P('tensor'), may hold values from 0.5 to 1.5
- w_q: bfloat16 [16384, 16384], P('tensor'), may hold values from -1 to 256
- w_kv: bfloat16 [16384, 2048], P('tensor'), may hold values from -0.046875 to 0.046875
- w_o: bfloat16 [16384, 16384], P(None, 'tensor'), may hold values from -0.046875 to 0.046875
- kv_cache: bfloat16 [8, 32, 2, 4096, 128], P(None, 'groups', None, 'tensor'), parts along dimension 1, may hold values from -8 to 8
- lengths: int32 [32], P('groups'), parts along dimension 0, may hold values from 2 to 4096, as said below
- slab_index: int32 [8, 32], P(None, 'groups'), parts along dimension 1, may hold values from 0 to 15, each once within a row
Outputs:
- hidden_out: bfloat16 [32, 16384], P('groups', 'tensor'), parts along dimension 0
The draws below stay inside these ranges and needn't reach their ends.
There are 2 independent parts, one for each index of `groups`. The reference program is written for one: setup_inputs(seed, part) draws one part's arguments, and reference() takes and returns one part's arrays. A program takes and returns all parts, laid end to end along the dimension named above; an argument that names none is the same for every part. Nothing has to cross between parts.
Inputs may be any that keep to these rules, and one draw needn't show every extreme that they name: `lengths`: one request in every draw has exactly 4096 cached tokens.
All inputs are finite; a program needn't handle non-finite values.
Results may differ from the reference program's by a relative error of at most 0.0085.
The reference program's roundings to bfloat16 on the way count: a program that leaves them out, or rounds other values in their place, can miss the bound.
Values may be sent and summed in bfloat16 or wider, within the bound.
No kernel may reach another device: no remote copies, remote signals or barrier semaphores. Data moves between devices by JAX's collectives and lax.ppermute only.
A program may use at most 64 MiB of HBM per device.

```python
import jax
import jax.numpy as jnp
from jax import lax

KVH = 8
HD = 128
GROUP = 16
D = 16384
CTX = 4096
BATCH = 16


def draw_lengths(key, part):
    picked = jax.random.randint(jax.random.fold_in(key, 11), (BATCH,), 2, CTX + 1)
    longest = jax.random.randint(jax.random.fold_in(key, 12), (), 0, BATCH)
    return jnp.where(jnp.arange(BATCH) == longest, CTX, picked).astype(jnp.int32)


def draw_w_q(key, part):
    weight_scale = D ** (-0.5)
    base = jax.random.normal(jax.random.fold_in(key, 31), (D, D), jnp.float32) * weight_scale
    base = jnp.clip(base, -6.0 * weight_scale, 6.0 * weight_scale)
    return base.astype(jnp.bfloat16)


def draw_kv_cache(key, part):
    base = 2.0 * jax.random.normal(jax.random.fold_in(key, 21), (KVH, BATCH, 2, CTX, HD), jnp.float32)
    return jnp.clip(base, -8.0, 8.0).astype(jnp.bfloat16)


def block_levels(rng, dims, shards, smallest, largest):
    level = 1.0
    for axis_at, blocks in shards:
        heights = jax.random.uniform(jax.random.fold_in(jax.random.fold_in(rng, 6), axis_at), (blocks,), jnp.float32, smallest / len(shards), largest / len(shards))
        level = level * jnp.repeat(jnp.exp(heights), dims[axis_at] // blocks).reshape((-1,) + (1,) * (len(dims) - 1 - axis_at))
    return level


def noise(rng, dims, width, reach, pieces=(), held_as=jnp.bfloat16):
    gain = block_levels(rng, dims, pieces, -0.22, 0.18) if pieces else 1.0
    values = jax.random.normal(rng, dims, jnp.float32) * width * gain
    return jnp.minimum(jnp.maximum(values, -reach), reach).astype(held_as)


def setup_inputs(seed: int = 0, part: int = 0) -> dict:
    key_of = jax.random.split(jax.random.key(seed), 9)
    own_keys = jax.random.split(jax.random.fold_in(key_of[8], part), 9)
    return {
        "hidden_in": noise(own_keys[0], (BATCH, D), 0.1, 0.59765625, ((1, 128),)),
        "norm_gain": jnp.clip(1.0 + 0.1 * jax.random.normal(key_of[1], (D,), jnp.float32), 0.5, 1.5).astype(jnp.bfloat16),
        "w_q": draw_w_q(jax.random.fold_in(key_of[8], 71), part),
        "w_kv": noise(key_of[3], (D, 2 * KVH * HD), D ** -0.5, 0.046875, ((0, 128),)),
        "w_o": noise(key_of[4], (D, D), D ** -0.5, 0.046875, ((1, 128),)),
        "kv_cache": draw_kv_cache(jax.random.fold_in(jax.random.fold_in(key_of[8], part), 71), part),
        "lengths": draw_lengths(jax.random.fold_in(jax.random.fold_in(key_of[8], part), 71), part),
        "slab_index": jax.vmap(lambda own: jax.random.permutation(own, BATCH))(jax.random.split(own_keys[7], KVH)).reshape((KVH, BATCH)).astype(jnp.int32),
    }


epsilon = 1e-05
rope_base = 500000.0

def rotate(values, position):
    head_dim = values.shape[-1]
    half_dim = head_dim // 2
    frequency = rope_base ** (-2.0 * jnp.arange(half_dim, dtype=jnp.float32) / head_dim)
    angles = position[..., None] * frequency
    cosine = jnp.cos(angles)
    sines = jnp.sin(angles)
    lower_half = values[..., :half_dim]
    upper_half = values[..., half_dim:]
    return jnp.concatenate([lower_half * cosine - upper_half * sines, upper_half * cosine + lower_half * sines], axis=-1)

def reference(hidden_in, norm_gain, w_q, w_kv, w_o, kv_cache, lengths, slab_index):
    stream = hidden_in.astype(jnp.float32)
    squares = lax.optimization_barrier(jnp.mean(stream * stream, axis=1, keepdims=True))
    normed = (stream * lax.rsqrt(squares + epsilon) * norm_gain.astype(jnp.float32)).astype(jnp.bfloat16)
    proj_q = jnp.dot(normed, w_q, preferred_element_type=jnp.float32)
    proj_kv = jnp.dot(normed, w_kv, preferred_element_type=jnp.float32)
    position = lengths.astype(jnp.float32)
    queries = rotate(proj_q.reshape(BATCH, KVH, GROUP, HD), position[:, None, None]).astype(jnp.bfloat16)
    kv_parts = proj_kv.reshape(BATCH, 2, KVH, HD)
    new_keys = rotate(kv_parts[:, 0], position[:, None]).astype(jnp.bfloat16)
    new_values = kv_parts[:, 1].astype(jnp.bfloat16)
    visible = jnp.arange(CTX, dtype=jnp.int32)[None, :] < lengths[:, None]
    score_scale = 1.0 / HD ** 0.5

    def attend_head(kv_head):
        cache_head = kv_cache[kv_head][slab_index[kv_head]]
        key_cache = cache_head[:, 0].astype(jnp.float32)
        value_cache = cache_head[:, 1].astype(jnp.float32)
        head_queries = queries[:, kv_head].astype(jnp.float32)
        scores = jnp.einsum('bgd,bpd->bgp', head_queries, key_cache) * score_scale
        new_score = jnp.einsum('bgd,bd->bg', head_queries, new_keys[:, kv_head].astype(jnp.float32)) * score_scale
        row_max = jnp.maximum(lax.optimization_barrier(jnp.max(jnp.where(visible[:, None, :], scores, -1e+30), axis=2)), new_score)
        weights = jnp.where(visible[:, None, :], jnp.exp(scores - row_max[..., None]), 0.0)
        new_weight = jnp.exp(new_score - row_max)
        denominator = lax.optimization_barrier(jnp.sum(weights, axis=2)) + new_weight
        weighted = jnp.einsum('bgp,bpd->bgd', weights.astype(jnp.bfloat16).astype(jnp.float32), value_cache)
        weighted = weighted + new_weight.astype(jnp.bfloat16).astype(jnp.float32)[..., None] * new_values[:, kv_head].astype(jnp.float32)[:, None, :]
        return (weighted / denominator[..., None]).astype(jnp.bfloat16)
    heads_out = lax.map(attend_head, jnp.arange(KVH, dtype=jnp.int32))
    attention = jnp.transpose(heads_out, (1, 0, 2, 3)).reshape(BATCH, D)
    result = stream + jnp.dot(attention, w_o, preferred_element_type=jnp.float32)
    return result.astype(jnp.bfloat16)
```

```python
import functools

import jax
import jax.numpy as jnp
from jax import lax
from jax.experimental import pallas as pl
from jax.experimental.pallas import tpu as pltpu
from jax.sharding import Mesh
from jax.sharding import PartitionSpec as P

NX, NZ, NC = 4, 16, 2
KVH = NX * NC
HD = 128
GROUP = 16
ROWS = GROUP + 2
QW = GROUP * HD
PW = ROWS * HD
MODEL = KVH * QW
TENSOR = ("x", "z", "c")

EPS = 1e-05
ROPE_BASE = 500000.0
SCALE = 1.0 / HD**0.5
NEG = -1e30


F32, BF16 = jnp.float32, jnp.bfloat16
VMEM = pl.BlockSpec(memory_space=pltpu.VMEM)


def diagonal(rows):
    lane = lax.broadcasted_iota(jnp.int32, (rows, HD), 1)
    return lane == lax.broadcasted_iota(jnp.int32, (rows, HD), 0)


def column(row, mask):
    return jnp.sum(jnp.where(mask, row, 0.0), axis=1, keepdims=True)


def as_row(col, mask):
    return jnp.sum(jnp.where(mask, col, 0.0), axis=0, keepdims=True)


def project_kernel(heads, sums, x, gain, wq, wk, wv, out):
    n = x.shape[0]
    squares = column(jnp.sum(sums[...], axis=0, keepdims=True), diagonal(n))
    stream = x[...].astype(F32)
    normed = (stream * lax.rsqrt(squares / MODEL + EPS) * gain[...].astype(F32)).astype(BF16)
    out[0, :, :QW] = jnp.dot(normed, wq[...], preferred_element_type=F32)
    out[0, :, QW : QW + HD] = jnp.dot(normed, wk[...], preferred_element_type=F32)
    out[0, :, QW + HD :] = jnp.dot(normed, wv[...], preferred_element_type=F32)


def project(heads, sums, x, gain, w_q, w_kv):
    n, depth = x.shape
    count = heads.shape[0]
    full = lambda shape: pl.BlockSpec(shape, lambda i, heads: (0,) * len(shape))
    return pl.pallas_call(
        project_kernel,
        grid_spec=pltpu.PrefetchScalarGridSpec(
            num_scalar_prefetch=1,
            grid=(count,),
            in_specs=[
                full(sums.shape),
                full(x.shape),
                full(gain.shape),
                pl.BlockSpec((depth, QW), lambda i, heads: (0, heads[i])),
                pl.BlockSpec((depth, HD), lambda i, heads: (0, heads[i])),
                pl.BlockSpec((depth, HD), lambda i, heads: (0, KVH + heads[i])),
            ],
            out_specs=pl.BlockSpec((1, n, PW), lambda i, heads: (i, 0, 0)),
        ),
        out_shape=jax.ShapeDtypeStruct((count, n, PW), F32),
    )(heads, sums, x, gain, w_q, w_kv, w_kv)


def pair_sum_kernel(a, b, *outs):
    for k, out in enumerate(outs):
        out[...] = a[k] + b[k]


def pair_sum(a, b):
    block = jax.ShapeDtypeStruct(a.shape[1:], F32)
    return pl.pallas_call(
        pair_sum_kernel,
        in_specs=[VMEM] * 2,
        out_specs=[VMEM] * NX,
        out_shape=[block] * NX,
    )(a, b)


def x_sum_kernel(a, b, c, d, out):
    for k in range(ROWS):
        cut = slice(k * HD, (k + 1) * HD)
        out[:, k, :] = (a[:, cut] + b[:, cut]) + (c[:, cut] + d[:, cut])


def x_sum(parts):
    n = parts[0].shape[0]
    return pl.pallas_call(
        x_sum_kernel,
        in_specs=[VMEM] * NX,
        out_specs=VMEM,
        out_shape=jax.ShapeDtypeStruct((n, ROWS, HD), F32),
    )(*parts)


def queries_kernel(parts, cosine, sine, q_out, new_score, new_value):
    total = jnp.sum(parts[...], axis=0)
    lead = total[: GROUP + 1]
    turned = lead * cosine[...] + pltpu.roll(lead, HD // 2, 1) * sine[...]
    turned = turned.astype(BF16)
    q = turned[:GROUP]
    q_out[...] = jnp.broadcast_to(q[None], q_out.shape)
    key = turned[GROUP : GROUP + 1].astype(F32)
    score = jnp.sum(q.astype(F32) * key, axis=1, keepdims=True) * SCALE
    new_score[...] = as_row(score, diagonal(GROUP))
    new_value[...] = total[GROUP + 1 :].astype(BF16).astype(F32)


def make_queries(parts, cosine, sine):
    row = jax.ShapeDtypeStruct((1, HD), F32)
    return pl.pallas_call(
        queries_kernel,
        in_specs=[VMEM] * 3,
        out_specs=[VMEM] * 3,
        out_shape=[jax.ShapeDtypeStruct((parts.shape[0], GROUP, HD), BF16), row, row],
    )(parts, cosine, sine)


def attend_kernel(per_step, where, lengths, place, q, kv, out):
    step = pl.program_id(0)
    sources, _, _, local, _ = kv.shape
    count = sources * local
    index = lax.broadcasted_iota(jnp.int32, (1, count), 1)
    source = index // local
    block = ((source // NC) * NZ + place[0]) * NC + source % NC
    position = block * local + index % local
    mask = diagonal(GROUP)
    for k in range(per_step):
        request = where[step * per_step + k]
        keys = kv[:, k, 0].reshape(count, HD)
        values = kv[:, k, 1].reshape(count, HD)
        scores = SCALE * lax.dot_general(
            q[request], keys, (((1,), (1,)), ((), ())), preferred_element_type=F32
        )
        visible = position < lengths[request]
        top = jnp.max(jnp.where(visible, scores, NEG), axis=1, keepdims=True)
        weights = jnp.where(visible, jnp.exp(scores - top), 0.0)
        total = jnp.sum(weights, axis=1, keepdims=True)
        out[request, :GROUP] = jnp.dot(
            weights.astype(BF16), values, preferred_element_type=F32
        )
        out[request, GROUP : GROUP + 1] = as_row(top, mask)
        out[request, GROUP + 1 :] = as_row(total, mask)


def attend(where, lengths, place, q, kv, steps=4):
    n = q.shape[0]
    per_step = n // steps
    sources, _, two, local, _ = kv.shape
    return pl.pallas_call(
        functools.partial(attend_kernel, per_step),
        grid_spec=pltpu.PrefetchScalarGridSpec(
            num_scalar_prefetch=3,
            grid=(steps,),
            in_specs=[
                pl.BlockSpec(q.shape, lambda i, *_: (0, 0, 0)),
                pl.BlockSpec(
                    (sources, per_step, two, local, HD), lambda i, *_: (0, i, 0, 0, 0)
                ),
            ],
            out_specs=pl.BlockSpec((n, ROWS, HD), lambda i, *_: (0, 0, 0)),
        ),
        out_shape=jax.ShapeDtypeStruct((n, ROWS, HD), F32),
    )(where, lengths, place, q, kv)


def combine_kernel(parts, new_score, new_value, out):
    mask = diagonal(GROUP)
    lanes = lax.broadcasted_iota(jnp.int32, (1, HD), 1) < GROUP
    tops = parts[:, GROUP, :]
    fresh = new_score[...]
    top = jnp.maximum(jnp.max(tops, axis=0, keepdims=True), fresh)
    share = jnp.where(lanes, jnp.exp(tops - top), 0.0)
    fresh_weight = jnp.where(lanes, jnp.exp(fresh - top), 0.0)
    total = jnp.sum(share * parts[:, GROUP + 1, :], axis=0, keepdims=True) + fresh_weight
    weighted = column(fresh_weight, mask).astype(BF16).astype(F32) * new_value[...]
    for k in range(parts.shape[0]):
        weighted = weighted + column(share[k : k + 1], mask) * parts[k, :GROUP]
    done = (weighted / column(total, mask)).astype(BF16)
    out[...] = jnp.broadcast_to(done[None], out.shape)


def combine(parts, new_score, new_value):
    return pl.pallas_call(
        combine_kernel,
        in_specs=[VMEM] * 3,
        out_specs=VMEM,
        out_shape=jax.ShapeDtypeStruct((parts.shape[0], GROUP, HD), BF16),
    )(parts, new_score, new_value)


def rows_kernel(heads, out, wide):
    wide[...] = heads[...].astype(F32)
    for k in range(GROUP):
        out[:, k * HD : (k + 1) * HD] = wide[:, k, :].astype(BF16)


def as_rows(heads):
    n = heads.shape[0]
    return pl.pallas_call(
        rows_kernel,
        in_specs=[VMEM],
        out_specs=VMEM,
        out_shape=jax.ShapeDtypeStruct((n, QW), BF16),
        scratch_shapes=[pltpu.VMEM(heads.shape, F32)],
    )(heads)


def output_kernel(order, a, b, c, d, w, x, out, total):
    step = pl.program_id(0)

    @pl.when(step == 0)
    def _():
        total[...] = x[...].astype(F32)

    for k, block in enumerate((a, b, c, d)):

        @pl.when(step == k)
        def _(block=block):
            add = jnp.dot(block[0], w[:QW], preferred_element_type=F32)
            total[...] += add + jnp.dot(block[1], w[QW:], preferred_element_type=F32)

    @pl.when(step == NX - 1)
    def _():
        out[...] = total[...].astype(BF16)


def output(order, blocks, w_o, x):
    full = lambda shape: pl.BlockSpec(shape, lambda i, order: (0,) * len(shape))
    return pl.pallas_call(
        output_kernel,
        grid_spec=pltpu.PrefetchScalarGridSpec(
            num_scalar_prefetch=1,
            grid=(NX,),
            in_specs=[full(blocks[0].shape)] * NX
            + [
                pl.BlockSpec((NC * QW, w_o.shape[1]), lambda i, order: (order[i], 0)),
                full(x.shape),
            ],
            out_specs=full(x.shape),
            scratch_shapes=[pltpu.VMEM(x.shape, F32)],
        ),
        out_shape=jax.ShapeDtypeStruct(x.shape, BF16),
    )(order, *blocks, w_o, x)


def shift_x(value, by):
    return lax.ppermute(value, "x", [(i, (i + by) % NX) for i in range(NX)])


def body(hidden_in, norm_gain, w_q, w_kv, w_o, kv_cache, lengths, slab_index):
    my_x, my_z, my_c = (lax.axis_index(a) for a in TENSOR)
    n = hidden_in.shape[0]
    members = NX * NZ * NC
    order = ((my_x + jnp.arange(NX)) % NX).astype(jnp.int32)
    theirs = order * NC + (1 - my_c)
    mine = order * NC + my_c

    position = lengths[my_z].astype(F32)
    frequency = ROPE_BASE ** (-2.0 * jnp.arange(HD // 2, dtype=F32) / HD)
    angles = position * frequency
    cosine, sine = jnp.cos(angles), jnp.sin(angles)
    cosine = jnp.concatenate([cosine, cosine])[None]
    sine = jnp.concatenate([-sine, sine])[None]
    slabs = slab_index[my_x * NC + my_c]
    counter = jnp.arange(n, dtype=jnp.int32)
    where = jnp.sum((slabs[None, :] == counter[:, None]) * counter[None, :], axis=1)
    where = where.astype(jnp.int32)
    place = my_z.astype(jnp.int32).reshape(1)

    stream = hidden_in.astype(F32)
    squares = jnp.pad(jnp.sum(stream * stream, axis=1), (0, HD - n))
    sums = lax.all_to_all(
        jnp.broadcast_to(squares, (members, 1, HD)), TENSOR, 0, 0, tiled=True
    ).reshape(members, HD)

    gain = norm_gain[None]
    sent = project(theirs, sums, hidden_in, gain, w_q, w_kv)
    got = lax.ppermute(sent, "c", [(0, 1), (1, 0)])
    kept = project(mine, sums, hidden_in, gain, w_q, w_kv)
    blocks = pair_sum(kept, got)
    parts = [blocks[0]] + [shift_x(blocks[k], k) for k in (1, 3, 2)]
    rows = x_sum(parts)
    cache, rows = lax.optimization_barrier((kv_cache, rows))
    cache = lax.all_to_all(cache, ("x", "c"), 0, 0, tiled=True)
    rows = lax.all_to_all(rows, "z", 0, 0, tiled=True)
    q, new_score, new_value = make_queries(rows, cosine, sine)
    q = lax.all_to_all(q, "z", 0, 0, tiled=True)

    partial = attend(where, lengths, place, q, cache)
    partial = lax.all_to_all(partial, "z", 0, 0, tiled=True)
    done = combine(partial, new_score, new_value)
    done = as_rows(lax.all_to_all(done, "z", 0, 0, tiled=True))
    both = lax.all_gather(done, "c")
    blocks = [both] + [shift_x(both, -k) for k in (1, 3, 2)]
    blocks = [blocks[0], blocks[1], blocks[3], blocks[2]]
    return output(order, blocks, w_o, hidden_in)


def solution(mesh):
    torus = Mesh(
        mesh.devices.reshape(mesh.shape["groups"], NX, NZ, NC),
        ("groups",) + TENSOR,
    )
    placed = (
        P("groups", TENSOR),
        P(TENSOR),
        P(TENSOR, None),
        P(TENSOR, None),
        P(None, TENSOR),
        P(None, "groups", None, TENSOR, None),
        P("groups"),
        P(None, "groups"),
    )
    return jax.shard_map(
        body, mesh=torus, in_specs=placed, out_specs=P("groups", TENSOR), check_vma=False
    )
```

```python
import functools

import jax
import jax.numpy as jnp
from jax import lax
from jax.experimental import pallas as pl
from jax.experimental.pallas import tpu as pltpu
from jax.sharding import Mesh
from jax.sharding import PartitionSpec as P

NX, NZ, NC = 4, 16, 2
KVH = NX * NC
HD = 128
GROUP = 16
ROWS = GROUP + 2
QW = GROUP * HD
PW = ROWS * HD
MODEL = KVH * QW
TENSOR = ("x", "z", "c")
MOVES = ((0, 0), (1, 0), (3, 0), (2, 0), (0, 1), (1, 1), (3, 1), (2, 1))

EPS = 1e-05
ROPE_BASE = 500000.0
SCALE = 1.0 / HD**0.5
NEG = -1e30


F32, BF16 = jnp.float32, jnp.bfloat16
VMEM = pl.BlockSpec(memory_space=pltpu.VMEM)
SMEM = pl.BlockSpec(memory_space=pltpu.SMEM)
HBM = pl.BlockSpec(memory_space=pltpu.HBM)
LIMIT = pltpu.CompilerParams(vmem_limit_bytes=16 * 2**20)


def struct(shape, dtype):
    return jax.ShapeDtypeStruct(shape, dtype)


def call(kernel, out, specs, *args, scratch=()):
    outs = jax.tree.map(lambda _: VMEM, out)
    return pl.pallas_call(
        kernel,
        in_specs=specs,
        out_specs=outs,
        out_shape=out,
        scratch_shapes=scratch,
        compiler_params=LIMIT,
    )(*args)


def diagonal(rows):
    lane = lax.broadcasted_iota(jnp.int32, (rows, HD), 1)
    return lane == lax.broadcasted_iota(jnp.int32, (rows, HD), 0)


def column(row, mask):
    return jnp.sum(jnp.where(mask, row, 0.0), axis=1, keepdims=True)


def as_row(col, mask):
    return jnp.sum(jnp.where(mask, col, 0.0), axis=0, keepdims=True)


def squares_kernel(x, out):
    stream = x[...].astype(F32)
    total = jnp.sum(stream * stream, axis=1, keepdims=True)
    out[...] = jnp.broadcast_to(as_row(total, diagonal(x.shape[0])), out.shape)


def fetch_in_kernel(place, wq, wkv, theirs, mine, sems):
    copies = []
    for k in range(2 * NX):
        out = theirs if k < NX else mine
        core = 1 - place[2] if k < NX else place[2]
        head = lax.rem(place[0] + k % NX, NX) * NC + core
        for part, (source, start, width, at) in enumerate(
            (
                (wq, head * QW, QW, 0),
                (wkv, head * HD, HD, QW),
                (wkv, (KVH + head) * HD, HD, QW + HD),
            )
        ):
            copy = pltpu.make_async_copy(
                source.at[:, pl.ds(pl.multiple_of(start, HD), width)],
                out.at[k % NX, :, pl.ds(at, width)],
                sems.at[k, part],
            )
            copy.start()
            copies.append(copy)
    for copy in copies:
        copy.wait()


def fetch_out_kernel(other, place, wo, out, sems):
    copies = []
    for k in range(NX):
        core = 1 - place[2] if other else place[2]
        head = lax.rem(place[0] + k, NX) * NC + core
        copy = pltpu.make_async_copy(
            wo.at[pl.ds(pl.multiple_of(head * QW, HD), QW)], out.at[k], sems.at[k]
        )
        copy.start()
        copies.append(copy)
    for copy in copies:
        copy.wait()


def fetch_cache_kernel(place, cache, *refs):
    outs, sems = refs[:-1], refs[-1]
    copies = []
    for k, (j, d) in enumerate(MOVES):
        core = 1 - place[2] if d else place[2]
        head = lax.rem(place[0] + j, NX) * NC + core
        copy = pltpu.make_async_copy(cache.at[head], outs[k], sems.at[k])
        copy.start()
        copies.append(copy)
    for copy in copies:
        copy.wait()


def project_first_kernel(sums, x, gain, w, normed_out, out):
    squares = column(jnp.sum(sums[...], axis=0, keepdims=True), diagonal(x.shape[0]))
    stream = x[...].astype(F32)
    normed = (stream * lax.rsqrt(squares / MODEL + EPS) * gain[...].astype(F32)).astype(BF16)
    normed_out[...] = normed
    for k in range(NX):
        out[k] = jnp.dot(normed, w[k], preferred_element_type=F32)


def project_kernel(normed, w, out):
    for k in range(NX):
        out[k] = jnp.dot(normed[...], w[k], preferred_element_type=F32)


def pair_sum_kernel(a, b, *outs):
    for k, out in enumerate(outs):
        out[...] = a[k] + b[k]


def x_sum_kernel(a, b, c, d, out):
    n = a.shape[0]
    for k in range(ROWS):
        cut = slice(k * HD, (k + 1) * HD)
        total = (a[:, cut] + b[:, cut]) + (c[:, cut] + d[:, cut])
        out[pl.ds(k, n, stride=ROWS), :] = total


def queries_kernel(parts, cosine, sine, q_out, new_score, new_value):
    n = parts.shape[0] // ROWS
    total = parts[:ROWS]
    for k in range(1, n):
        total = total + parts[k * ROWS : (k + 1) * ROWS]
    lead = total[: GROUP + 1]
    turned = lead * cosine[...] + pltpu.roll(lead, HD // 2, 1) * sine[...]
    turned = turned.astype(BF16)
    q = turned[:GROUP]
    q_out[...] = jnp.broadcast_to(q[None], q_out.shape)
    key = turned[GROUP : GROUP + 1].astype(F32)
    score = jnp.sum(q.astype(F32) * key, axis=1, keepdims=True) * SCALE
    new_score[...] = as_row(score, diagonal(GROUP))
    new_value[...] = total[GROUP + 1 :].astype(BF16).astype(F32)


def attend_kernel(lengths, place, slabs, q, *refs):
    caches, out = refs[:-1], refs[-1]
    local = caches[0].shape[2]
    count = len(caches) * local
    head = place[0] * NC + place[2]
    index = lax.broadcasted_iota(jnp.int32, (1, count), 1)
    start = jnp.zeros_like(index)
    for k, (j, d) in enumerate(MOVES):
        core = 1 - place[2] if d else place[2]
        block = (lax.rem(place[0] + (NX - j), NX) * NZ + place[1]) * NC + core
        start = jnp.where(index // local == k, block * local, start)
    position = start + index % local
    mask = diagonal(GROUP)
    for b in range(q.shape[0]):
        slab = slabs[head, b]
        keys = jnp.concatenate([cache[slab, 0] for cache in caches], axis=0)
        values = jnp.concatenate([cache[slab, 1] for cache in caches], axis=0)
        scores = SCALE * lax.dot_general(
            q[b], keys, (((1,), (1,)), ((), ())), preferred_element_type=F32
        )
        visible = position < lengths[b]
        top = jnp.max(jnp.where(visible, scores, NEG), axis=1, keepdims=True)
        weights = jnp.where(visible, jnp.exp(scores - top), 0.0)
        total = jnp.sum(weights, axis=1, keepdims=True)
        at = b * ROWS
        out[at : at + GROUP] = jnp.dot(
            weights.astype(BF16), values, preferred_element_type=F32
        )
        out[at + GROUP : at + GROUP + 1] = as_row(top, mask)
        out[at + GROUP + 1 : at + ROWS] = as_row(total, mask)


def combine_kernel(parts, new_score, new_value, out):
    n = parts.shape[0] // ROWS
    mask = diagonal(GROUP)
    lanes = lax.broadcasted_iota(jnp.int32, (1, HD), 1) < GROUP
    tops = parts[pl.ds(GROUP, n, stride=ROWS), :]
    totals = parts[pl.ds(GROUP + 1, n, stride=ROWS), :]
    fresh = new_score[...]
    top = jnp.maximum(jnp.max(tops, axis=0, keepdims=True), fresh)
    share = jnp.where(lanes, jnp.exp(tops - top), 0.0)
    fresh_weight = jnp.where(lanes, jnp.exp(fresh - top), 0.0)
    total = jnp.sum(share * totals, axis=0, keepdims=True) + fresh_weight
    weighted = column(fresh_weight, mask).astype(BF16).astype(F32) * new_value[...]
    for k in range(n):
        at = k * ROWS
        weighted = weighted + column(share[k : k + 1], mask) * parts[at : at + GROUP]
    done = (weighted / column(total, mask)).astype(BF16)
    out[...] = jnp.broadcast_to(done[None], out.shape)


def rows_kernel(heads, out, wide):
    wide[...] = heads[...].astype(F32)
    for k in range(GROUP):
        out[:, k * HD : (k + 1) * HD] = wide[:, k, :].astype(BF16)


def output_kernel(a, b, c, d, e, f, g, h, w_mine, w_theirs, x, out):
    total = x[...].astype(F32)
    for k, rows in enumerate((a, b, c, d)):
        total = total + jnp.dot(rows[...], w_mine[k], preferred_element_type=F32)
    for k, rows in enumerate((e, f, g, h)):
        total = total + jnp.dot(rows[...], w_theirs[k], preferred_element_type=F32)
    out[...] = total.astype(BF16)


def shift_x(value, by):
    return lax.ppermute(value, "x", [(i, (i + by) % NX) for i in range(NX)])


def swap_c(value):
    return lax.ppermute(value, "c", [(0, 1), (1, 0)])


def across_z(value):
    return lax.all_to_all(value, "z", 0, 0, tiled=True)


def step(hidden_in, norm_gain, w_q, w_kv, w_o, kv_cache, lengths, slab_index):
    n, depth = hidden_in.shape
    members = NX * NZ * NC
    w_q, w_kv, w_o, kv_cache = (
        pltpu.with_memory_space_constraint(v, pltpu.HBM) for v in (w_q, w_kv, w_o, kv_cache)
    )
    place = jnp.stack([lax.axis_index(a) for a in TENSOR]).astype(jnp.int32)

    position = lengths[lax.axis_index("z")].astype(F32)
    frequency = ROPE_BASE ** (-2.0 * jnp.arange(HD // 2, dtype=F32) / HD)
    angles = position * frequency
    cosine, sine = jnp.cos(angles), jnp.sin(angles)
    cosine = jnp.concatenate([cosine, cosine])[None]
    sine = jnp.concatenate([-sine, sine])[None]

    sums = call(squares_kernel, struct((members, HD), F32), [VMEM], hidden_in)
    sums = lax.all_to_all(
        sums.reshape(members, 1, HD), TENSOR, 0, 0, tiled=True
    ).reshape(members, HD)

    half = struct((NX, depth, PW), BF16)
    w_theirs, w_mine = call(
        fetch_in_kernel,
        [half, half],
        [SMEM, HBM, HBM],
        place,
        w_q,
        w_kv,
        scratch=[pltpu.SemaphoreType.DMA((2 * NX, 3))],
    )

    cache = list(call(
        fetch_cache_kernel,
        [struct(kv_cache.shape[1:], BF16)] * len(MOVES),
        [SMEM, HBM],
        place,
        kv_cache,
        scratch=[pltpu.SemaphoreType.DMA((len(MOVES),))],
    ))

    product = struct((NX, n, PW), F32)
    normed, sent = call(
        project_first_kernel,
        [struct((n, depth), BF16), product],
        [VMEM] * 4,
        sums,
        hidden_in,
        norm_gain[None],
        w_theirs,
    )
    got = swap_c(sent)
    kept = call(project_kernel, product, [VMEM] * 2, normed, w_mine)
    blocks = call(pair_sum_kernel, [struct((n, PW), F32)] * NX, [VMEM] * 2, kept, got)
    parts = [blocks[0]]
    for k in (1, 3, 2):
        parts.append(shift_x(blocks[k], k))
    rows = call(x_sum_kernel, struct((n * ROWS, HD), F32), [VMEM] * NX, *parts)
    for k, (j, d) in enumerate(MOVES[1:], 1):
        pairs = [
            (x * NC + c, (x + j) % NX * NC + (c + d) % NC)
            for x in range(NX)
            for c in range(NC)
        ]
        cache[k] = lax.ppermute(cache[k], ("x", "c"), pairs)
    rows = across_z(rows.reshape(n, 1, PW)).reshape(n * ROWS, HD)
    w_rows = []
    for other in (0, 1):
        w_rows.append(
            call(
                functools.partial(fetch_out_kernel, other),
                struct((NX, QW, w_o.shape[1]), BF16),
                [SMEM, HBM],
                place,
                w_o,
                scratch=[pltpu.SemaphoreType.DMA((NX,))],
            )
        )
    q, new_score, new_value = call(
        queries_kernel,
        [struct((n, GROUP, HD), BF16), struct((1, HD), F32), struct((1, HD), F32)],
        [VMEM] * 3,
        rows,
        cosine,
        sine,
    )
    q = across_z(q)

    partial = call(
        attend_kernel,
        struct((n * ROWS, HD), F32),
        [SMEM, SMEM, SMEM] + [VMEM] * (1 + len(MOVES)),
        lengths,
        place,
        slab_index,
        q,
        *cache,
    )
    partial = across_z(partial.reshape(n, 1, PW)).reshape(n * ROWS, HD)
    done = call(
        combine_kernel, struct((n, GROUP, HD), BF16), [VMEM] * 3, partial, new_score, new_value
    )
    done = across_z(done)
    done = call(
        rows_kernel,
        struct((n, QW), BF16),
        [VMEM],
        done,
        scratch=[pltpu.VMEM((n, GROUP, HD), F32)],
    )
    beside = {0: done}
    for k in (1, 3, 2):
        beside[k] = shift_x(done, -k)
    mine = [beside[k] for k in range(NX)]
    theirs = [swap_c(block) for block in mine]
    return call(
        output_kernel, struct((n, depth), BF16), [VMEM] * 11, *mine, *theirs, *w_rows, hidden_in
    )


def solution(mesh):
    torus = Mesh(
        mesh.devices.reshape(mesh.shape["groups"], NX, NZ, NC),
        ("groups",) + TENSOR,
    )
    placed = (
        P("groups", TENSOR),
        P(TENSOR),
        P(TENSOR, None),
        P(TENSOR, None),
        P(None, TENSOR),
        P(None, "groups", None, TENSOR, None),
        P("groups"),
        P(None, "groups"),
    )
    return jax.shard_map(
        step, mesh=torus, in_specs=placed, out_specs=P("groups", TENSOR), check_vma=False
    )
```

```python
import functools

import jax
import jax.numpy as jnp
from jax import lax
from jax.experimental import pallas as pl
from jax.experimental.pallas import tpu as pltpu
from jax.sharding import Mesh
from jax.sharding import PartitionSpec as P

NX, NZ, NC = 4, 16, 2
KVH = NX * NC
HD = 128
GROUP = 16
ROWS = GROUP + 2
QW = GROUP * HD
PW = ROWS * HD
MODEL = KVH * QW
TENSOR = ("x", "z", "c")
NEAR = ((0, 0), (0, 1))
FAR = ((1, 0), (3, 0), (2, 0), (1, 1), (3, 1), (2, 1))
MOVES = ((0, 0), (1, 0), (3, 0), (2, 0), (0, 1), (1, 1), (3, 1), (2, 1))

EPS = 1e-05
ROPE_BASE = 500000.0
SCALE = 1.0 / HD**0.5
NEG = -1e30


F32, BF16 = jnp.float32, jnp.bfloat16
VMEM = pl.BlockSpec(memory_space=pltpu.VMEM)
SMEM = pl.BlockSpec(memory_space=pltpu.SMEM)
HBM = pl.BlockSpec(memory_space=pltpu.HBM)
LIMIT = pltpu.CompilerParams(vmem_limit_bytes=16 * 2**20)


def struct(shape, dtype):
    return jax.ShapeDtypeStruct(shape, dtype)


def call(kernel, out, specs, *args, scratch=()):
    outs = jax.tree.map(lambda _: VMEM, out)
    return pl.pallas_call(
        kernel,
        in_specs=specs,
        out_specs=outs,
        out_shape=out,
        scratch_shapes=scratch,
        compiler_params=LIMIT,
    )(*args)


def diagonal(rows):
    lane = lax.broadcasted_iota(jnp.int32, (rows, HD), 1)
    return lane == lax.broadcasted_iota(jnp.int32, (rows, HD), 0)


def column(row, mask):
    return jnp.sum(jnp.where(mask, row, 0.0), axis=1, keepdims=True)


def as_row(col, mask):
    return jnp.sum(jnp.where(mask, col, 0.0), axis=0, keepdims=True)


def squares_kernel(x, out):
    stream = x[...].astype(F32)
    total = jnp.sum(stream * stream, axis=1, keepdims=True)
    out[...] = jnp.broadcast_to(as_row(total, diagonal(x.shape[0])), out.shape)


def head_of(place, j, d):
    core = 1 - place[2] if d else place[2]
    return lax.rem(place[0] + j, NX) * NC + core


def in_copies(place, d, wq, wkv, out, sems):
    copies = []
    for k in range(NX):
        head = head_of(place, k, d)
        for part, (source, start, width, at) in enumerate(
            (
                (wq, head * QW, QW, 0),
                (wkv, head * HD, HD, QW),
                (wkv, (KVH + head) * HD, HD, QW + HD),
            )
        ):
            copies.append(
                pltpu.make_async_copy(
                    source.at[:, pl.ds(pl.multiple_of(start, HD), width)],
                    out.at[k, :, pl.ds(at, width)],
                    sems.at[k, part],
                )
            )
    return copies


def out_copies(place, moves, wo, out, sems):
    return [
        pltpu.make_async_copy(
            wo.at[pl.ds(pl.multiple_of(head_of(place, j, d) * QW, HD), QW)],
            out.at[k],
            sems.at[k],
        )
        for k, (j, d) in enumerate(moves)
    ]


def run_all(copies):
    for copy in copies:
        copy.start()
    for copy in copies:
        copy.wait()


def fetch_in_kernel(place, wq, wkv, out, sems):
    run_all(in_copies(place, 1, wq, wkv, out, sems))


def fetch_out_kernel(place, wo, out, sems):
    run_all(out_copies(place, FAR, wo, out, sems))


def fetch_cache_kernel(place, cache, *refs):
    outs, sems = refs[:-1], refs[-1]
    run_all(
        [
            pltpu.make_async_copy(cache.at[head_of(place, j, d)], outs[k], sems.at[k])
            for k, (j, d) in enumerate(MOVES)
        ]
    )


def project_first_kernel(sums, x, gain, w, normed_out, out):
    squares = column(jnp.sum(sums[...], axis=0, keepdims=True), diagonal(x.shape[0]))
    stream = x[...].astype(F32)
    normed = (stream * lax.rsqrt(squares / MODEL + EPS) * gain[...].astype(F32)).astype(BF16)
    normed_out[...] = normed
    for k in range(NX):
        out[k] = jnp.dot(normed, w[k], preferred_element_type=F32)


def project_kernel(place, normed, wq, wkv, out, w, sems):
    copies = in_copies(place, 0, wq, wkv, w, sems)
    for copy in copies:
        copy.start()
    for k in range(NX):
        for copy in copies[3 * k : 3 * k + 3]:
            copy.wait()
        out[k] = jnp.dot(normed[...], w[k], preferred_element_type=F32)


def pair_sum_kernel(a, b, *outs):
    for k, out in enumerate(outs):
        out[...] = a[k] + b[k]


def x_sum_kernel(a, b, c, d, out):
    n = a.shape[0]
    for k in range(ROWS):
        cut = slice(k * HD, (k + 1) * HD)
        total = (a[:, cut] + b[:, cut]) + (c[:, cut] + d[:, cut])
        out[pl.ds(k, n, stride=ROWS), :] = total


def queries_kernel(parts, cosine, sine, q_out, new_score, new_value):
    n = parts.shape[0] // ROWS
    total = parts[:ROWS]
    for k in range(1, n):
        total = total + parts[k * ROWS : (k + 1) * ROWS]
    lead = total[: GROUP + 1]
    turned = lead * cosine[...] + pltpu.roll(lead, HD // 2, 1) * sine[...]
    turned = turned.astype(BF16)
    q = turned[:GROUP]
    q_out[...] = jnp.broadcast_to(q[None], q_out.shape)
    key = turned[GROUP : GROUP + 1].astype(F32)
    score = jnp.sum(q.astype(F32) * key, axis=1, keepdims=True) * SCALE
    new_score[...] = as_row(score, diagonal(GROUP))
    new_value[...] = total[GROUP + 1 :].astype(BF16).astype(F32)


def positions_kernel(local, place, out):
    index = lax.broadcasted_iota(jnp.int32, out.shape, 1)
    start = jnp.zeros_like(index)
    for k, (j, d) in enumerate(MOVES):
        core = 1 - place[2] if d else place[2]
        block = (lax.rem(place[0] + (NX - j), NX) * NZ + place[1]) * NC + core
        start = jnp.where(index // local == k, block * local, start)
    out[...] = start + index % local


def attend_kernel(lengths, place, slabs, positions, q, *refs):
    caches, out, scores, weights = refs[: len(MOVES)], *refs[len(MOVES) :]
    n = q.shape[0]
    head = place[0] * NC + place[2]
    mask = diagonal(GROUP)
    for b in range(n):
        slab = slabs[head, b]
        keys = jnp.concatenate([cache[slab, 0] for cache in caches], axis=0)
        scores[b * GROUP : (b + 1) * GROUP] = SCALE * lax.dot_general(
            q[b], keys, (((1,), (1,)), ((), ())), preferred_element_type=F32
        )
    for b in range(n):
        rows = slice(b * GROUP, (b + 1) * GROUP)
        visible = positions[...] < lengths[b]
        score = jnp.where(visible, scores[rows], NEG)
        top = jnp.max(score, axis=1, keepdims=True)
        weight = jnp.where(visible, jnp.exp(score - top), 0.0)
        total = jnp.sum(weight, axis=1, keepdims=True)
        weights[rows] = weight.astype(BF16)
        at = b * ROWS + GROUP
        out[at : at + 1] = as_row(top, mask)
        out[at + 1 : at + 2] = as_row(total, mask)
    for b in range(n):
        slab = slabs[head, b]
        values = jnp.concatenate([cache[slab, 1] for cache in caches], axis=0)
        out[b * ROWS : b * ROWS + GROUP] = jnp.dot(
            weights[b * GROUP : (b + 1) * GROUP], values, preferred_element_type=F32
        )


def combine_kernel(parts, new_score, new_value, out):
    n = parts.shape[0] // ROWS
    mask = diagonal(GROUP)
    lanes = lax.broadcasted_iota(jnp.int32, (1, HD), 1) < GROUP
    tops = parts[pl.ds(GROUP, n, stride=ROWS), :]
    totals = parts[pl.ds(GROUP + 1, n, stride=ROWS), :]
    fresh = new_score[...]
    top = jnp.maximum(jnp.max(tops, axis=0, keepdims=True), fresh)
    share = jnp.where(lanes, jnp.exp(tops - top), 0.0)
    fresh_weight = jnp.where(lanes, jnp.exp(fresh - top), 0.0)
    total = jnp.sum(share * totals, axis=0, keepdims=True) + fresh_weight
    weighted = column(fresh_weight, mask).astype(BF16).astype(F32) * new_value[...]
    for k in range(n):
        at = k * ROWS
        weighted = weighted + column(share[k : k + 1], mask) * parts[at : at + GROUP]
    done = (weighted / column(total, mask)).astype(BF16)
    out[...] = jnp.broadcast_to(done[None], out.shape)


def rows_kernel(heads, out, wide):
    wide[...] = heads[...].astype(F32)
    for k in range(GROUP):
        out[:, k * HD : (k + 1) * HD] = wide[:, k, :].astype(BF16)


def output_near_kernel(place, a, b, wo, x, out, w, sems):
    run_all(out_copies(place, NEAR, wo, w, sems))
    total = x[...].astype(F32)
    for k, rows in enumerate((a, b)):
        total = total + jnp.dot(rows[...], w[k], preferred_element_type=F32)
    out[...] = total


def output_far_kernel(*refs):
    near, *rows, w, out = refs
    total = near[...]
    for k, block in enumerate(rows):
        total = total + jnp.dot(block[...], w[k], preferred_element_type=F32)
    out[...] = total.astype(BF16)


def shift_x(value, by):
    return lax.ppermute(value, "x", [(i, (i + by) % NX) for i in range(NX)])


def swap_c(value):
    return lax.ppermute(value, "c", [(0, 1), (1, 0)])


def across_z(value):
    return lax.all_to_all(value, "z", 0, 0, tiled=True)


def step(hidden_in, norm_gain, w_q, w_kv, w_o, kv_cache, lengths, slab_index):
    n, depth = hidden_in.shape
    members = NX * NZ * NC
    w_q, w_kv, w_o, kv_cache = (
        pltpu.with_memory_space_constraint(v, pltpu.HBM) for v in (w_q, w_kv, w_o, kv_cache)
    )
    place = jnp.stack([lax.axis_index(a) for a in TENSOR]).astype(jnp.int32)

    mine = jnp.arange(n, dtype=jnp.int32) == lax.axis_index("z")
    position = jnp.sum(jnp.where(mine, lengths, 0)).astype(F32)
    lane = jnp.arange(HD, dtype=jnp.int32)[None]
    frequency = ROPE_BASE ** (-2.0 * (lane % (HD // 2)).astype(F32) / HD)
    angles = position * frequency
    cosine = jnp.cos(angles)
    sine = jnp.sin(angles) * jnp.where(lane < HD // 2, -1.0, 1.0)

    sums = call(squares_kernel, struct((members, HD), F32), [VMEM], hidden_in)
    sums = lax.all_to_all(
        sums.reshape(members, 1, HD), TENSOR, 0, 0, tiled=True
    ).reshape(members, HD)

    half = struct((NX, depth, PW), BF16)
    dmas = pltpu.SemaphoreType.DMA((NX, 3))
    w_theirs = call(fetch_in_kernel, half, [SMEM, HBM, HBM], place, w_q, w_kv, scratch=[dmas])

    cache = list(call(
        fetch_cache_kernel,
        [struct(kv_cache.shape[1:], BF16)] * len(MOVES),
        [SMEM, HBM],
        place,
        kv_cache,
        scratch=[pltpu.SemaphoreType.DMA((len(MOVES),))],
    ))

    product = struct((NX, n, PW), F32)
    normed, sent = call(
        project_first_kernel,
        [struct((n, depth), BF16), product],
        [VMEM] * 4,
        sums,
        hidden_in,
        norm_gain[None],
        w_theirs,
    )
    got = swap_c(sent)
    kept = call(
        project_kernel,
        product,
        [SMEM, VMEM, HBM, HBM],
        place,
        normed,
        w_q,
        w_kv,
        scratch=[pltpu.VMEM(half.shape, BF16), dmas],
    )
    blocks = call(pair_sum_kernel, [struct((n, PW), F32)] * NX, [VMEM] * 2, kept, got)
    parts = [blocks[0]]
    for k in (1, 3, 2):
        parts.append(shift_x(blocks[k], k))
    rows = call(x_sum_kernel, struct((n * ROWS, HD), F32), [VMEM] * NX, *parts)
    for k, (j, d) in enumerate(MOVES[1:], 1):
        pairs = [
            (x * NC + c, (x + j) % NX * NC + (c + d) % NC)
            for x in range(NX)
            for c in range(NC)
        ]
        cache[k] = pltpu.with_memory_space_constraint(cache[k], pltpu.HBM)
        cache[k] = lax.ppermute(cache[k], ("x", "c"), pairs)
    local = kv_cache.shape[3]
    seen = len(MOVES) * local
    positions = call(
        functools.partial(positions_kernel, local),
        struct((1, seen), jnp.int32),
        [SMEM],
        place,
    )
    rows = across_z(rows.reshape(n, 1, PW)).reshape(n * ROWS, HD)
    w_far = call(
        fetch_out_kernel,
        struct((len(FAR), QW, w_o.shape[1]), BF16),
        [SMEM, HBM],
        place,
        w_o,
        scratch=[pltpu.SemaphoreType.DMA((len(FAR),))],
    )
    q, new_score, new_value = call(
        queries_kernel,
        [struct((n, GROUP, HD), BF16), struct((1, HD), F32), struct((1, HD), F32)],
        [VMEM] * 3,
        rows,
        cosine,
        sine,
    )
    q = across_z(q)

    partial = call(
        attend_kernel,
        struct((n * ROWS, HD), F32),
        [SMEM, SMEM, SMEM] + [VMEM] * (2 + len(MOVES)),
        lengths,
        place,
        slab_index,
        positions,
        q,
        *cache,
        scratch=[pltpu.VMEM((n * GROUP, seen), F32), pltpu.VMEM((n * GROUP, seen), BF16)],
    )
    partial = across_z(partial.reshape(n, 1, PW)).reshape(n * ROWS, HD)
    done = call(
        combine_kernel, struct((n, GROUP, HD), BF16), [VMEM] * 3, partial, new_score, new_value
    )
    done = across_z(done)
    done = call(
        rows_kernel,
        struct((n, QW), BF16),
        [VMEM],
        done,
        scratch=[pltpu.VMEM((n, GROUP, HD), F32)],
    )
    rows = {(0, 0): done}
    for k in (1, 3, 2):
        rows[k, 0] = shift_x(done, -k)
    for k in (0, 1, 3, 2):
        rows[k, 1] = swap_c(rows[k, 0])
    total = call(
        output_near_kernel,
        struct((n, depth), F32),
        [SMEM, VMEM, VMEM, HBM, VMEM],
        place,
        *(rows[move] for move in NEAR),
        w_o,
        hidden_in,
        scratch=[
            pltpu.VMEM((len(NEAR), QW, w_o.shape[1]), BF16),
            pltpu.SemaphoreType.DMA((len(NEAR),)),
        ],
    )
    return call(
        output_far_kernel,
        struct((n, depth), BF16),
        [VMEM] * (2 + len(FAR)),
        total,
        *(rows[move] for move in FAR),
        w_far,
    )


def solution(mesh):
    torus = Mesh(
        mesh.devices.reshape(mesh.shape["groups"], NX, NZ, NC),
        ("groups",) + TENSOR,
    )
    placed = (
        P("groups", TENSOR),
        P(TENSOR),
        P(TENSOR, None),
        P(TENSOR, None),
        P(None, TENSOR),
        P(None, "groups", None, TENSOR, None),
        P("groups"),
        P(None, "groups"),
    )
    return jax.shard_map(
        step, mesh=torus, in_specs=placed, out_specs=P("groups", TENSOR), check_vma=False
    )
```

```python
import functools

import jax
import jax.numpy as jnp
from jax import lax
from jax.experimental import pallas as pl
from jax.experimental.pallas import tpu as pltpu
from jax.sharding import Mesh
from jax.sharding import PartitionSpec as P

NX, NZ, NC = 4, 16, 2
KVH = NX * NC
HD = 128
GROUP = 16
ROWS = GROUP + 2
QW = GROUP * HD
PW = ROWS * HD
MODEL = KVH * QW
TENSOR = ("x", "z", "c")
NEAR = ((0, 0), (0, 1))
FAR = ((1, 0), (3, 0), (2, 0), (1, 1), (3, 1), (2, 1))
MOVES = ((0, 0), (1, 0), (3, 0), (2, 0), (0, 1), (1, 1), (3, 1), (2, 1))

EPS = 1e-05
ROPE_BASE = 500000.0
SCALE = 1.0 / HD**0.5
NEG = -1e30


F32, BF16 = jnp.float32, jnp.bfloat16
VMEM = pl.BlockSpec(memory_space=pltpu.VMEM)
SMEM = pl.BlockSpec(memory_space=pltpu.SMEM)
HBM = pl.BlockSpec(memory_space=pltpu.HBM)
LIMIT = pltpu.CompilerParams(vmem_limit_bytes=16 * 2**20)


def struct(shape, dtype):
    return jax.ShapeDtypeStruct(shape, dtype)


def call(kernel, out, specs, *args, scratch=()):
    is_out = lambda v: not isinstance(v, (list, tuple))
    outs = jax.tree.map(lambda v: VMEM if isinstance(v, jax.ShapeDtypeStruct) else HBM, out, is_leaf=is_out)
    return pl.pallas_call(
        kernel,
        in_specs=specs,
        out_specs=outs,
        out_shape=out,
        scratch_shapes=scratch,
        compiler_params=LIMIT,
    )(*args)


def diagonal(rows):
    lane = lax.broadcasted_iota(jnp.int32, (rows, HD), 1)
    return lane == lax.broadcasted_iota(jnp.int32, (rows, HD), 0)


def column(row, mask):
    return jnp.sum(jnp.where(mask, row, 0.0), axis=1, keepdims=True)


def as_row(col, mask):
    return jnp.sum(jnp.where(mask, col, 0.0), axis=0, keepdims=True)


def squares_kernel(x, out):
    stream = x[...].astype(F32)
    total = jnp.sum(stream * stream, axis=1, keepdims=True)
    out[...] = jnp.broadcast_to(as_row(total, diagonal(x.shape[0])), out.shape)


def head_of(place, j, d):
    core = 1 - place[2] if d else place[2]
    return lax.rem(place[0] + j, NX) * NC + core


def in_copies(place, d, wq, wkv, out, sems):
    copies = []
    for k in range(NX):
        head = head_of(place, k, d)
        for part, (source, start, width, at) in enumerate(
            (
                (wq, head * QW, QW, 0),
                (wkv, head * HD, HD, QW),
                (wkv, (KVH + head) * HD, HD, QW + HD),
            )
        ):
            copies.append(
                pltpu.make_async_copy(
                    source.at[:, pl.ds(pl.multiple_of(start, HD), width)],
                    out.at[k, :, pl.ds(at, width)],
                    sems.at[k, part],
                )
            )
    return copies


def out_copies(place, moves, wo, out, sems):
    return [
        pltpu.make_async_copy(
            wo.at[pl.ds(pl.multiple_of(head_of(place, j, d) * QW, HD), QW)],
            out.at[k],
            sems.at[k],
        )
        for k, (j, d) in enumerate(moves)
    ]


def run_all(copies):
    for copy in copies:
        copy.start()
    for copy in copies:
        copy.wait()


def fetch_in_kernel(place, wq, wkv, out, sems):
    run_all(in_copies(place, 1, wq, wkv, out, sems))


def fetch_cache_kernel(place, cache, *refs):
    outs, sems = refs[:-1], refs[-1]
    run_all(
        [
            pltpu.make_async_copy(cache.at[head_of(place, j, d)], outs[k], sems.at[k])
            for k, (j, d) in enumerate(MOVES)
        ]
    )


def project_first_kernel(sums, x, gain, w, normed_out, out):
    squares = column(jnp.sum(sums[...], axis=0, keepdims=True), diagonal(x.shape[0]))
    stream = x[...].astype(F32)
    normed = (stream * lax.rsqrt(squares / MODEL + EPS) * gain[...].astype(F32)).astype(BF16)
    normed_out[...] = normed
    for k in range(NX):
        out[k] = jnp.dot(normed, w[k], preferred_element_type=F32)


def project_kernel(place, normed, wq, wkv, out, w, sems):
    copies = in_copies(place, 0, wq, wkv, w, sems)
    for copy in copies:
        copy.start()
    for k in range(NX):
        for copy in copies[3 * k : 3 * k + 3]:
            copy.wait()
        out[k] = jnp.dot(normed[...], w[k], preferred_element_type=F32)


def pair_sum_kernel(a, b, *outs):
    for k, out in enumerate(outs):
        out[...] = a[k] + b[k]


def x_sum_kernel(a, b, c, d, out):
    n = a.shape[0]
    for k in range(ROWS):
        cut = slice(k * HD, (k + 1) * HD)
        total = (a[:, cut] + b[:, cut]) + (c[:, cut] + d[:, cut])
        out[pl.ds(k, n, stride=ROWS), :] = total


def queries_kernel(parts, cosine, sine, q_out, new_score, new_value):
    n = parts.shape[0] // ROWS
    total = parts[:ROWS]
    for k in range(1, n):
        total = total + parts[k * ROWS : (k + 1) * ROWS]
    lead = total[: GROUP + 1]
    turned = lead * cosine[...] + pltpu.roll(lead, HD // 2, 1) * sine[...]
    turned = turned.astype(BF16)
    q = turned[:GROUP]
    q_out[...] = jnp.broadcast_to(q[None], q_out.shape)
    key = turned[GROUP : GROUP + 1].astype(F32)
    score = jnp.sum(q.astype(F32) * key, axis=1, keepdims=True) * SCALE
    new_score[...] = as_row(score, diagonal(GROUP))
    new_value[...] = total[GROUP + 1 :].astype(BF16).astype(F32)


def positions_kernel(local, place, out):
    index = lax.broadcasted_iota(jnp.int32, out.shape, 1)
    start = jnp.zeros_like(index)
    for k, (j, d) in enumerate(MOVES):
        core = 1 - place[2] if d else place[2]
        block = (lax.rem(place[0] + (NX - j), NX) * NZ + place[1]) * NC + core
        start = jnp.where(index // local == k, block * local, start)
    out[...] = start + index % local


def attend_kernel(lengths, place, slabs, positions, q, *refs):
    caches, out, scores, weights = refs[: len(MOVES)], *refs[len(MOVES) :]
    n = q.shape[0]
    head = place[0] * NC + place[2]
    mask = diagonal(GROUP)
    for b in range(n):
        slab = slabs[head, b]
        keys = jnp.concatenate([cache[slab, 0] for cache in caches], axis=0)
        scores[b * GROUP : (b + 1) * GROUP] = SCALE * lax.dot_general(
            q[b], keys, (((1,), (1,)), ((), ())), preferred_element_type=F32
        )
    for b in range(n):
        rows = slice(b * GROUP, (b + 1) * GROUP)
        visible = positions[...] < lengths[b]
        score = jnp.where(visible, scores[rows], NEG)
        top = jnp.max(score, axis=1, keepdims=True)
        weight = jnp.where(visible, jnp.exp(score - top), 0.0)
        total = jnp.sum(weight, axis=1, keepdims=True)
        weights[rows] = weight.astype(BF16)
        at = b * ROWS + GROUP
        out[at : at + 1] = as_row(top, mask)
        out[at + 1 : at + 2] = as_row(total, mask)
    for b in range(n):
        slab = slabs[head, b]
        values = jnp.concatenate([cache[slab, 1] for cache in caches], axis=0)
        out[b * ROWS : b * ROWS + GROUP] = jnp.dot(
            weights[b * GROUP : (b + 1) * GROUP], values, preferred_element_type=F32
        )


def combine_kernel(parts, new_score, new_value, out):
    n = parts.shape[0] // ROWS
    mask = diagonal(GROUP)
    lanes = lax.broadcasted_iota(jnp.int32, (1, HD), 1) < GROUP
    tops = parts[pl.ds(GROUP, n, stride=ROWS), :]
    totals = parts[pl.ds(GROUP + 1, n, stride=ROWS), :]
    fresh = new_score[...]
    top = jnp.maximum(jnp.max(tops, axis=0, keepdims=True), fresh)
    share = jnp.where(lanes, jnp.exp(tops - top), 0.0)
    fresh_weight = jnp.where(lanes, jnp.exp(fresh - top), 0.0)
    total = jnp.sum(share * totals, axis=0, keepdims=True) + fresh_weight
    weighted = column(fresh_weight, mask).astype(BF16).astype(F32) * new_value[...]
    for k in range(n):
        at = k * ROWS
        weighted = weighted + column(share[k : k + 1], mask) * parts[at : at + GROUP]
    done = (weighted / column(total, mask)).astype(BF16)
    out[...] = jnp.broadcast_to(done[None], out.shape)


def rows_kernel(heads, out, wide):
    wide[...] = heads[...].astype(F32)
    for k in range(GROUP):
        out[:, k * HD : (k + 1) * HD] = wide[:, k, :].astype(BF16)


def output_near_kernel(place, a, b, wo, x, out, w_far, w, sems, far_sems):
    near = out_copies(place, NEAR, wo, w, sems)
    far = out_copies(place, FAR, wo, w_far, far_sems)
    for copy in near + far:
        copy.start()
    for copy in near:
        copy.wait()
    total = x[...].astype(F32)
    for k, rows in enumerate((a, b)):
        total = total + jnp.dot(rows[...], w[k], preferred_element_type=F32)
    out[...] = total
    for copy in far:
        copy.wait()


def output_far_kernel(*refs):
    near, *rows, w, out = refs
    total = near[...]
    for k, block in enumerate(rows):
        total = total + jnp.dot(block[...], w[k], preferred_element_type=F32)
    out[...] = total.astype(BF16)


def shift_x(value, by):
    return lax.ppermute(value, "x", [(i, (i + by) % NX) for i in range(NX)])


def swap_c(value):
    return lax.ppermute(value, "c", [(0, 1), (1, 0)])


def across_z(value):
    return lax.all_to_all(value, "z", 0, 0, tiled=True)


def step(hidden_in, norm_gain, w_q, w_kv, w_o, kv_cache, lengths, slab_index):
    n, depth = hidden_in.shape
    members = NX * NZ * NC
    w_q, w_kv, w_o, kv_cache = (
        pltpu.with_memory_space_constraint(v, pltpu.HBM) for v in (w_q, w_kv, w_o, kv_cache)
    )
    place = jnp.stack([lax.axis_index(a) for a in TENSOR]).astype(jnp.int32)

    mine = jnp.arange(n, dtype=jnp.int32) == lax.axis_index("z")
    position = jnp.sum(jnp.where(mine, lengths, 0)).astype(F32)
    lane = jnp.arange(HD, dtype=jnp.int32)[None]
    frequency = ROPE_BASE ** (-2.0 * (lane % (HD // 2)).astype(F32) / HD)
    angles = position * frequency
    cosine = jnp.cos(angles)
    sine = jnp.sin(angles) * jnp.where(lane < HD // 2, -1.0, 1.0)

    sums = call(squares_kernel, struct((members, HD), F32), [VMEM], hidden_in)
    sums = lax.all_to_all(
        sums.reshape(members, 1, HD), TENSOR, 0, 0, tiled=True
    ).reshape(members, HD)

    half = struct((NX, depth, PW), BF16)
    dmas = pltpu.SemaphoreType.DMA((NX, 3))
    w_theirs = call(fetch_in_kernel, half, [SMEM, HBM, HBM], place, w_q, w_kv, scratch=[dmas])

    cache = list(call(
        fetch_cache_kernel,
        [pltpu.HBM(kv_cache.shape[1:], BF16)] * len(MOVES),
        [SMEM, HBM],
        place,
        kv_cache,
        scratch=[pltpu.SemaphoreType.DMA((len(MOVES),))],
    ))

    product = struct((NX, n, PW), F32)
    normed, sent = call(
        project_first_kernel,
        [struct((n, depth), BF16), product],
        [VMEM] * 4,
        sums,
        hidden_in,
        norm_gain[None],
        w_theirs,
    )
    got = swap_c(sent)
    kept = call(
        project_kernel,
        product,
        [SMEM, VMEM, HBM, HBM],
        place,
        normed,
        w_q,
        w_kv,
        scratch=[pltpu.VMEM(half.shape, BF16), dmas],
    )
    blocks = call(pair_sum_kernel, [struct((n, PW), F32)] * NX, [VMEM] * 2, kept, got)
    parts = [blocks[0]]
    for k in (2, 1, 3):
        parts.append(shift_x(blocks[k], k))
    rows = call(x_sum_kernel, struct((n * ROWS, HD), F32), [VMEM] * NX, *parts)
    for k, (j, d) in enumerate(MOVES[1:], 1):
        pairs = [
            (x * NC + c, (x + j) % NX * NC + (c + d) % NC)
            for x in range(NX)
            for c in range(NC)
        ]
        cache[k] = lax.ppermute(cache[k], ("x", "c"), pairs)
    local = kv_cache.shape[3]
    seen = len(MOVES) * local
    positions = call(
        functools.partial(positions_kernel, local),
        struct((1, seen), jnp.int32),
        [SMEM],
        place,
    )
    rows = across_z(rows.reshape(n, 1, PW)).reshape(n * ROWS, HD)
    q, new_score, new_value = call(
        queries_kernel,
        [struct((n, GROUP, HD), BF16), struct((1, HD), F32), struct((1, HD), F32)],
        [VMEM] * 3,
        rows,
        cosine,
        sine,
    )
    q = across_z(q)

    partial = call(
        attend_kernel,
        struct((n * ROWS, HD), F32),
        [SMEM, SMEM, SMEM] + [VMEM] * (2 + len(MOVES)),
        lengths,
        place,
        slab_index,
        positions,
        q,
        *cache,
        scratch=[pltpu.VMEM((n * GROUP, seen), F32), pltpu.VMEM((n * GROUP, seen), BF16)],
    )
    partial = across_z(partial.reshape(n, 1, PW)).reshape(n * ROWS, HD)
    done = call(
        combine_kernel, struct((n, GROUP, HD), BF16), [VMEM] * 3, partial, new_score, new_value
    )
    done = across_z(done)
    done = call(
        rows_kernel,
        struct((n, QW), BF16),
        [VMEM],
        done,
        scratch=[pltpu.VMEM((n, GROUP, HD), F32)],
    )
    rows = {(0, 0): done}
    for k in (1, 3, 2):
        rows[k, 0] = shift_x(done, -k)
    for k in (0, 1, 3, 2):
        rows[k, 1] = swap_c(rows[k, 0])
    total, w_far = call(
        output_near_kernel,
        [struct((n, depth), F32), struct((len(FAR), QW, w_o.shape[1]), BF16)],
        [SMEM, VMEM, VMEM, HBM, VMEM],
        place,
        *(rows[move] for move in NEAR),
        w_o,
        hidden_in,
        scratch=[
            pltpu.VMEM((len(NEAR), QW, w_o.shape[1]), BF16),
            pltpu.SemaphoreType.DMA((len(NEAR),)),
            pltpu.SemaphoreType.DMA((len(FAR),)),
        ],
    )
    return call(
        output_far_kernel,
        struct((n, depth), BF16),
        [VMEM] * (2 + len(FAR)),
        total,
        *(rows[move] for move in FAR),
        w_far,
    )


def solution(mesh):
    torus = Mesh(
        mesh.devices.reshape(mesh.shape["groups"], NX, NZ, NC),
        ("groups",) + TENSOR,
    )
    placed = (
        P("groups", TENSOR),
        P(TENSOR),
        P(TENSOR, None),
        P(TENSOR, None),
        P(None, TENSOR),
        P(None, "groups", None, TENSOR, None),
        P("groups"),
        P(None, "groups"),
    )
    return jax.shard_map(
        step, mesh=torus, in_specs=placed, out_specs=P("groups", TENSOR), check_vma=False
    )
```

```python
import functools

import jax
import jax.numpy as jnp
from jax import lax
from jax.experimental import pallas as pl
from jax.experimental.pallas import tpu as pltpu
from jax.sharding import Mesh
from jax.sharding import PartitionSpec as P

NX, NZ, NC = 4, 16, 2
KVH = NX * NC
HD = 128
GROUP = 16
ROWS = GROUP + 2
QW = GROUP * HD
PW = ROWS * HD
MODEL = KVH * QW
TENSOR = ("x", "z", "c")
NEAR = ((0, 0), (0, 1))
FAR = ((1, 0), (3, 0), (2, 0), (1, 1), (3, 1), (2, 1))
MOVES = ((0, 0), (1, 0), (3, 0), (2, 0), (0, 1), (1, 1), (3, 1), (2, 1))

EPS = 1e-05
ROPE_BASE = 500000.0
SCALE = 1.0 / HD**0.5
NEG = -1e30


F32, BF16 = jnp.float32, jnp.bfloat16
VMEM = pl.BlockSpec(memory_space=pltpu.VMEM)
SMEM = pl.BlockSpec(memory_space=pltpu.SMEM)
HBM = pl.BlockSpec(memory_space=pltpu.HBM)
LIMIT = pltpu.CompilerParams(vmem_limit_bytes=16 * 2**20)


def struct(shape, dtype):
    return jax.ShapeDtypeStruct(shape, dtype)


def call(kernel, out, specs, *args, scratch=()):
    is_out = lambda v: not isinstance(v, (list, tuple))
    outs = jax.tree.map(lambda v: VMEM if isinstance(v, jax.ShapeDtypeStruct) else HBM, out, is_leaf=is_out)
    return pl.pallas_call(
        kernel,
        in_specs=specs,
        out_specs=outs,
        out_shape=out,
        scratch_shapes=scratch,
        compiler_params=LIMIT,
    )(*args)


def diagonal(rows):
    lane = lax.broadcasted_iota(jnp.int32, (rows, HD), 1)
    return lane == lax.broadcasted_iota(jnp.int32, (rows, HD), 0)


def column(row, mask):
    return jnp.sum(jnp.where(mask, row, 0.0), axis=1, keepdims=True)


def as_row(col, mask):
    return jnp.sum(jnp.where(mask, col, 0.0), axis=0, keepdims=True)


def squares_kernel(x, out):
    stream = x[...].astype(F32)
    total = jnp.sum(stream * stream, axis=1, keepdims=True)
    out[...] = jnp.broadcast_to(as_row(total, diagonal(x.shape[0])), out.shape)


def head_of(place, j, d):
    core = 1 - place[2] if d else place[2]
    return lax.rem(place[0] + j, NX) * NC + core


def in_copies(place, d, wq, wkv, out, sems):
    copies = []
    for k in range(NX):
        head = head_of(place, k, d)
        for part, (source, start, width, at) in enumerate(
            (
                (wq, head * QW, QW, 0),
                (wkv, head * HD, HD, QW),
                (wkv, (KVH + head) * HD, HD, QW + HD),
            )
        ):
            copies.append(
                pltpu.make_async_copy(
                    source.at[:, pl.ds(pl.multiple_of(start, HD), width)],
                    out.at[k, :, pl.ds(at, width)],
                    sems.at[k, part],
                )
            )
    return copies


def out_copies(place, moves, wo, out, sems):
    return [
        pltpu.make_async_copy(
            wo.at[pl.ds(pl.multiple_of(head_of(place, j, d) * QW, HD), QW)],
            out.at[k],
            sems.at[k],
        )
        for k, (j, d) in enumerate(moves)
    ]


def run_all(copies):
    for copy in copies:
        copy.start()
    for copy in copies:
        copy.wait()


def fetch_in_kernel(place, wq, wkv, out, sems):
    run_all(in_copies(place, 1, wq, wkv, out, sems))


def fetch_cache_kernel(place, cache, *refs):
    outs, held, sems, out_sems = refs[:-3], *refs[-3:]
    first, second = [], []
    for k, (j, d) in enumerate(MOVES):
        to = outs[k] if k == 0 else held.at[k]
        first.append(pltpu.make_async_copy(cache.at[head_of(place, j, d)], to, sems.at[k]))
        first[k].start()
    for k in range(1, len(MOVES)):
        first[k].wait()
        second.append(pltpu.make_async_copy(held.at[k], outs[k], out_sems.at[k]))
        second[-1].start()
    first[0].wait()
    for copy in second:
        copy.wait()


def project_first_kernel(sums, x, gain, w, normed_out, out):
    squares = column(jnp.sum(sums[...], axis=0, keepdims=True), diagonal(x.shape[0]))
    stream = x[...].astype(F32)
    normed = (stream * lax.rsqrt(squares / MODEL + EPS) * gain[...].astype(F32)).astype(BF16)
    normed_out[...] = normed
    for k in range(NX):
        out[k] = jnp.dot(normed, w[k], preferred_element_type=F32)


def project_kernel(place, normed, wq, wkv, out, w, sems):
    copies = in_copies(place, 0, wq, wkv, w, sems)
    for copy in copies:
        copy.start()
    for k in range(NX):
        for copy in copies[3 * k : 3 * k + 3]:
            copy.wait()
        out[k] = jnp.dot(normed[...], w[k], preferred_element_type=F32)


def pair_sum_kernel(a, b, *outs):
    for k, out in enumerate(outs):
        out[...] = a[k] + b[k]


def x_sum_kernel(a, b, c, d, out):
    n = a.shape[0]
    for k in range(ROWS):
        cut = slice(k * HD, (k + 1) * HD)
        total = (a[:, cut] + b[:, cut]) + (c[:, cut] + d[:, cut])
        out[pl.ds(k, n, stride=ROWS), :] = total


def queries_kernel(parts, cosine, sine, q_out, new_score, new_value):
    n = parts.shape[0] // ROWS
    total = parts[:ROWS]
    for k in range(1, n):
        total = total + parts[k * ROWS : (k + 1) * ROWS]
    lead = total[: GROUP + 1]
    turned = lead * cosine[...] + pltpu.roll(lead, HD // 2, 1) * sine[...]
    turned = turned.astype(BF16)
    q = turned[:GROUP]
    q_out[...] = jnp.broadcast_to(q[None], q_out.shape)
    key = turned[GROUP : GROUP + 1].astype(F32)
    score = jnp.sum(q.astype(F32) * key, axis=1, keepdims=True) * SCALE
    new_score[...] = as_row(score, diagonal(GROUP))
    new_value[...] = total[GROUP + 1 :].astype(BF16).astype(F32)


def positions_kernel(local, place, out):
    index = lax.broadcasted_iota(jnp.int32, out.shape, 1)
    start = jnp.zeros_like(index)
    for k, (j, d) in enumerate(MOVES):
        core = 1 - place[2] if d else place[2]
        block = (lax.rem(place[0] + (NX - j), NX) * NZ + place[1]) * NC + core
        start = jnp.where(index // local == k, block * local, start)
    out[...] = start + index % local


def attend_kernel(lengths, place, slabs, positions, q, *refs):
    caches, out, scores, weights = refs[: len(MOVES)], *refs[len(MOVES) :]
    n = q.shape[0]
    head = place[0] * NC + place[2]
    mask = diagonal(GROUP)
    for b in range(n):
        slab = slabs[head, b]
        keys = jnp.concatenate([cache[slab, 0] for cache in caches], axis=0)
        scores[b * GROUP : (b + 1) * GROUP] = SCALE * lax.dot_general(
            q[b], keys, (((1,), (1,)), ((), ())), preferred_element_type=F32
        )
    for b in range(n):
        rows = slice(b * GROUP, (b + 1) * GROUP)
        visible = positions[...] < lengths[b]
        score = jnp.where(visible, scores[rows], NEG)
        top = jnp.max(score, axis=1, keepdims=True)
        weight = jnp.where(visible, jnp.exp(score - top), 0.0)
        total = jnp.sum(weight, axis=1, keepdims=True)
        weights[rows] = weight.astype(BF16)
        at = b * ROWS + GROUP
        out[at : at + 1] = as_row(top, mask)
        out[at + 1 : at + 2] = as_row(total, mask)
    for b in range(n):
        slab = slabs[head, b]
        values = jnp.concatenate([cache[slab, 1] for cache in caches], axis=0)
        out[b * ROWS : b * ROWS + GROUP] = jnp.dot(
            weights[b * GROUP : (b + 1) * GROUP], values, preferred_element_type=F32
        )


def combine_kernel(parts, new_score, new_value, out):
    n = parts.shape[0] // ROWS
    mask = diagonal(GROUP)
    lanes = lax.broadcasted_iota(jnp.int32, (1, HD), 1) < GROUP
    tops = parts[pl.ds(GROUP, n, stride=ROWS), :]
    totals = parts[pl.ds(GROUP + 1, n, stride=ROWS), :]
    fresh = new_score[...]
    top = jnp.maximum(jnp.max(tops, axis=0, keepdims=True), fresh)
    share = jnp.where(lanes, jnp.exp(tops - top), 0.0)
    fresh_weight = jnp.where(lanes, jnp.exp(fresh - top), 0.0)
    total = jnp.sum(share * totals, axis=0, keepdims=True) + fresh_weight
    weighted = column(fresh_weight, mask).astype(BF16).astype(F32) * new_value[...]
    for k in range(n):
        at = k * ROWS
        weighted = weighted + column(share[k : k + 1], mask) * parts[at : at + GROUP]
    done = (weighted / column(total, mask)).astype(BF16)
    out[...] = jnp.broadcast_to(done[None], out.shape)


def rows_kernel(heads, out, wide):
    wide[...] = heads[...].astype(F32)
    for k in range(GROUP):
        out[:, k * HD : (k + 1) * HD] = wide[:, k, :].astype(BF16)


def output_near_kernel(place, a, b, wo, x, out, w_far, w, sems, far_sems):
    near = out_copies(place, NEAR, wo, w, sems)
    far = out_copies(place, FAR, wo, w_far, far_sems)
    for copy in near + far:
        copy.start()
    for copy in near:
        copy.wait()
    total = x[...].astype(F32)
    for k, rows in enumerate((a, b)):
        total = total + jnp.dot(rows[...], w[k], preferred_element_type=F32)
    out[...] = total
    for copy in far:
        copy.wait()


def output_far_kernel(*refs):
    near, *rows, w, out = refs
    total = near[...]
    for k, block in enumerate(rows):
        total = total + jnp.dot(block[...], w[k], preferred_element_type=F32)
    out[...] = total.astype(BF16)


def shift_x(value, by):
    return lax.ppermute(value, "x", [(i, (i + by) % NX) for i in range(NX)])


def swap_c(value):
    return lax.ppermute(value, "c", [(0, 1), (1, 0)])


def across_z(value):
    return lax.all_to_all(value, "z", 0, 0, tiled=True)


def step(hidden_in, norm_gain, w_q, w_kv, w_o, kv_cache, lengths, slab_index):
    n, depth = hidden_in.shape
    members = NX * NZ * NC
    w_q, w_kv, w_o, kv_cache = (
        pltpu.with_memory_space_constraint(v, pltpu.HBM) for v in (w_q, w_kv, w_o, kv_cache)
    )
    place = jnp.stack([lax.axis_index(a) for a in TENSOR]).astype(jnp.int32)

    mine = jnp.arange(n, dtype=jnp.int32) == lax.axis_index("z")
    position = jnp.sum(jnp.where(mine, lengths, 0)).astype(F32)
    lane = jnp.arange(HD, dtype=jnp.int32)[None]
    frequency = ROPE_BASE ** (-2.0 * (lane % (HD // 2)).astype(F32) / HD)
    angles = position * frequency
    cosine = jnp.cos(angles)
    sine = jnp.sin(angles) * jnp.where(lane < HD // 2, -1.0, 1.0)

    sums = call(squares_kernel, struct((members, HD), F32), [VMEM], hidden_in)
    sums = lax.all_to_all(
        sums.reshape(members, 1, HD), TENSOR, 0, 0, tiled=True
    ).reshape(members, HD)

    half = struct((NX, depth, PW), BF16)
    dmas = pltpu.SemaphoreType.DMA((NX, 3))
    w_theirs = call(fetch_in_kernel, half, [SMEM, HBM, HBM], place, w_q, w_kv, scratch=[dmas])

    cache = list(call(
        fetch_cache_kernel,
        [struct(kv_cache.shape[1:], BF16)]
        + [pltpu.HBM(kv_cache.shape[1:], BF16)] * (len(MOVES) - 1),
        [SMEM, HBM],
        place,
        kv_cache,
        scratch=[
            pltpu.VMEM(kv_cache.shape, BF16),
            pltpu.SemaphoreType.DMA((len(MOVES),)),
            pltpu.SemaphoreType.DMA((len(MOVES),)),
        ],
    ))

    product = struct((NX, n, PW), F32)
    normed, sent = call(
        project_first_kernel,
        [struct((n, depth), BF16), product],
        [VMEM] * 4,
        sums,
        hidden_in,
        norm_gain[None],
        w_theirs,
    )
    got = swap_c(sent)
    kept = call(
        project_kernel,
        product,
        [SMEM, VMEM, HBM, HBM],
        place,
        normed,
        w_q,
        w_kv,
        scratch=[pltpu.VMEM(half.shape, BF16), dmas],
    )
    blocks = call(pair_sum_kernel, [struct((n, PW), F32)] * NX, [VMEM] * 2, kept, got)
    parts = [blocks[0]]
    for k in (1, 3, 2):
        parts.append(shift_x(blocks[k], k))
    rows = call(x_sum_kernel, struct((n * ROWS, HD), F32), [VMEM] * NX, *parts)
    for k, (j, d) in enumerate(MOVES[1:], 1):
        pairs = [
            (x * NC + c, (x + j) % NX * NC + (c + d) % NC)
            for x in range(NX)
            for c in range(NC)
        ]
        cache[k] = lax.ppermute(cache[k], ("x", "c"), pairs)
    local = kv_cache.shape[3]
    seen = len(MOVES) * local
    positions = call(
        functools.partial(positions_kernel, local),
        struct((1, seen), jnp.int32),
        [SMEM],
        place,
    )
    rows = across_z(rows.reshape(n, 1, PW)).reshape(n * ROWS, HD)
    q, new_score, new_value = call(
        queries_kernel,
        [struct((n, GROUP, HD), BF16), struct((1, HD), F32), struct((1, HD), F32)],
        [VMEM] * 3,
        rows,
        cosine,
        sine,
    )
    q = across_z(q)

    partial = call(
        attend_kernel,
        struct((n * ROWS, HD), F32),
        [SMEM, SMEM, SMEM] + [VMEM] * (2 + len(MOVES)),
        lengths,
        place,
        slab_index,
        positions,
        q,
        *cache,
        scratch=[pltpu.VMEM((n * GROUP, seen), F32), pltpu.VMEM((n * GROUP, seen), BF16)],
    )
    partial = across_z(partial.reshape(n, 1, PW)).reshape(n * ROWS, HD)
    done = call(
        combine_kernel, struct((n, GROUP, HD), BF16), [VMEM] * 3, partial, new_score, new_value
    )
    done = across_z(done)
    done = call(
        rows_kernel,
        struct((n, QW), BF16),
        [VMEM],
        done,
        scratch=[pltpu.VMEM((n, GROUP, HD), F32)],
    )
    rows = {(0, 0): done}
    for k in (1, 3, 2):
        rows[k, 0] = shift_x(done, -k)
    for k in (0, 1, 3, 2):
        rows[k, 1] = swap_c(rows[k, 0])
    total, w_far = call(
        output_near_kernel,
        [struct((n, depth), F32), struct((len(FAR), QW, w_o.shape[1]), BF16)],
        [SMEM, VMEM, VMEM, HBM, VMEM],
        place,
        *(rows[move] for move in NEAR),
        w_o,
        hidden_in,
        scratch=[
            pltpu.VMEM((len(NEAR), QW, w_o.shape[1]), BF16),
            pltpu.SemaphoreType.DMA((len(NEAR),)),
            pltpu.SemaphoreType.DMA((len(FAR),)),
        ],
    )
    return call(
        output_far_kernel,
        struct((n, depth), BF16),
        [VMEM] * (2 + len(FAR)),
        total,
        *(rows[move] for move in FAR),
        w_far,
    )


def solution(mesh):
    torus = Mesh(
        mesh.devices.reshape(mesh.shape["groups"], NX, NZ, NC),
        ("groups",) + TENSOR,
    )
    placed = (
        P("groups", TENSOR),
        P(TENSOR),
        P(TENSOR, None),
        P(TENSOR, None),
        P(None, TENSOR),
        P(None, "groups", None, TENSOR, None),
        P("groups"),
        P(None, "groups"),
    )
    return jax.shard_map(
        step, mesh=torus, in_specs=placed, out_specs=P("groups", TENSOR), check_vma=False
    )
```

```python
import functools

import jax
import jax.numpy as jnp
from jax import lax
from jax.experimental import pallas as pl
from jax.experimental.pallas import tpu as pltpu
from jax.sharding import Mesh
from jax.sharding import PartitionSpec as P

NX, NZ, NC = 4, 16, 2
KVH = NX * NC
HD = 128
GROUP = 16
ROWS = GROUP + 2
QW = GROUP * HD
PW = ROWS * HD
MODEL = KVH * QW
TENSOR = ("x", "z", "c")
NEAR = ((0, 0), (0, 1))
FAR = ((1, 0), (3, 0), (2, 0), (1, 1), (3, 1), (2, 1))
MOVES = ((0, 0), (0, 1), (1, 0), (3, 0), (2, 0), (1, 1), (3, 1), (2, 1))
EARLY = 4

EPS = 1e-05
ROPE_BASE = 500000.0
SCALE = 1.0 / HD**0.5
NEG = -1e30


F32, BF16 = jnp.float32, jnp.bfloat16
VMEM = pl.BlockSpec(memory_space=pltpu.VMEM)
SMEM = pl.BlockSpec(memory_space=pltpu.SMEM)
HBM = pl.BlockSpec(memory_space=pltpu.HBM)
LIMIT = pltpu.CompilerParams(vmem_limit_bytes=16 * 2**20)


def struct(shape, dtype):
    return jax.ShapeDtypeStruct(shape, dtype)


def call(kernel, out, specs, *args, scratch=(), params=LIMIT):
    is_out = lambda v: not isinstance(v, (list, tuple))
    outs = jax.tree.map(lambda v: VMEM if isinstance(v, jax.ShapeDtypeStruct) else HBM, out, is_leaf=is_out)
    return pl.pallas_call(
        kernel,
        in_specs=specs,
        out_specs=outs,
        out_shape=out,
        scratch_shapes=scratch,
        compiler_params=params,
    )(*args)


def diagonal(rows):
    lane = lax.broadcasted_iota(jnp.int32, (rows, HD), 1)
    return lane == lax.broadcasted_iota(jnp.int32, (rows, HD), 0)


def column(row, mask):
    return jnp.sum(jnp.where(mask, row, 0.0), axis=1, keepdims=True)


def as_row(col, mask):
    return jnp.sum(jnp.where(mask, col, 0.0), axis=0, keepdims=True)


def squares_kernel(x, out):
    stream = x[...].astype(F32)
    total = jnp.sum(stream * stream, axis=1, keepdims=True)
    out[...] = jnp.broadcast_to(as_row(total, diagonal(x.shape[0])), out.shape)


def head_of(place, j, d):
    core = 1 - place[2] if d else place[2]
    return lax.rem(place[0] + j, NX) * NC + core


def in_copies(place, d, wq, wkv, out, sems):
    copies = []
    for k in range(NX):
        head = head_of(place, k, d)
        for part, (source, start, width, at) in enumerate(
            (
                (wq, head * QW, QW, 0),
                (wkv, head * HD, HD, QW),
                (wkv, (KVH + head) * HD, HD, QW + HD),
            )
        ):
            copies.append(
                pltpu.make_async_copy(
                    source.at[:, pl.ds(pl.multiple_of(start, HD), width)],
                    out.at[k, :, pl.ds(at, width)],
                    sems.at[k, part],
                )
            )
    return copies


def out_copies(place, moves, wo, out, sems):
    return [
        pltpu.make_async_copy(
            wo.at[pl.ds(pl.multiple_of(head_of(place, j, d) * QW, HD), QW)],
            out.at[k],
            sems.at[k],
        )
        for k, (j, d) in enumerate(moves)
    ]


def run_all(copies):
    for copy in copies:
        copy.start()
    for copy in copies:
        copy.wait()


def fetch_in_kernel(place, wq, wkv, out, sems):
    run_all(in_copies(place, 1, wq, wkv, out, sems))


def fetch_cache_kernel(moves, place, cache, *refs):
    outs, held, sems, out_sems = refs[:-3], *refs[-3:]
    first, second = [], []
    for k, (j, d) in enumerate(moves):
        stays = (j, d) == (0, 0)
        to = outs[k] if stays else held.at[k]
        first.append(pltpu.make_async_copy(cache.at[head_of(place, j, d)], to, sems.at[k]))
        first[k].start()
    for k, move in enumerate(moves):
        first[k].wait()
        if move != (0, 0):
            second.append(pltpu.make_async_copy(held.at[k], outs[k], out_sems.at[k]))
            second[-1].start()
    for copy in second:
        copy.wait()


def project_first_kernel(sums, x, gain, w, normed_out, out):
    squares = column(jnp.sum(sums[...], axis=0, keepdims=True), diagonal(x.shape[0]))
    stream = x[...].astype(F32)
    normed = (stream * lax.rsqrt(squares / MODEL + EPS) * gain[...].astype(F32)).astype(BF16)
    normed_out[...] = normed
    for k in range(NX):
        out[k] = jnp.dot(normed, w[k], preferred_element_type=F32)


def project_kernel(place, normed, wq, wkv, out, w, sems):
    copies = in_copies(place, 0, wq, wkv, w, sems)
    for copy in copies:
        copy.start()
    for k in range(NX):
        for copy in copies[3 * k : 3 * k + 3]:
            copy.wait()
        out[k] = jnp.dot(normed[...], w[k], preferred_element_type=F32)


def pair_sum_kernel(a, b, *outs):
    for k, out in enumerate(outs):
        out[...] = a[k] + b[k]


def x_sum_kernel(a, b, c, d, out):
    n = a.shape[0]
    for k in range(ROWS):
        cut = slice(k * HD, (k + 1) * HD)
        total = (a[:, cut] + b[:, cut]) + (c[:, cut] + d[:, cut])
        out[pl.ds(k, n, stride=ROWS), :] = total


def queries_kernel(parts, cosine, sine, q_out, new_score, new_value):
    n = parts.shape[0] // ROWS
    total = parts[:ROWS]
    for k in range(1, n):
        total = total + parts[k * ROWS : (k + 1) * ROWS]
    lead = total[: GROUP + 1]
    turned = lead * cosine[...] + pltpu.roll(lead, HD // 2, 1) * sine[...]
    turned = turned.astype(BF16)
    q = turned[:GROUP]
    q_out[...] = jnp.broadcast_to(q[None], q_out.shape)
    key = turned[GROUP : GROUP + 1].astype(F32)
    score = jnp.sum(q.astype(F32) * key, axis=1, keepdims=True) * SCALE
    new_score[...] = as_row(score, diagonal(GROUP))
    new_value[...] = total[GROUP + 1 :].astype(BF16).astype(F32)


def positions_kernel(local, first, last, place, base, out):
    index = lax.broadcasted_iota(jnp.int32, out.shape, 1)
    start = base[...]
    for k, (j, d) in list(enumerate(MOVES))[first:last]:
        core = 1 - place[2] if d else place[2]
        block = (lax.rem(place[0] + (NX - j), NX) * NZ + place[1]) * NC + core
        start = jnp.where(index // local == k, block * local, start)
    out[...] = start


def visible_kernel(local, lengths, positions, q, out):
    del q
    here = positions[...] + lax.broadcasted_iota(jnp.int32, positions.shape, 1) % local
    for b in range(out.shape[0]):
        out[b : b + 1] = (here < lengths[b]).astype(F32)


def attend_kernel(place, slabs, seen, q, *refs):
    caches, out, scores, weights = refs[: len(MOVES)], *refs[len(MOVES) :]
    n = q.shape[0]
    head = place[0] * NC + place[2]
    mask = diagonal(GROUP)
    for b in range(n):
        slab = slabs[head, b]
        keys = jnp.concatenate([cache[slab, 0] for cache in caches], axis=0)
        scores[b * GROUP : (b + 1) * GROUP] = SCALE * lax.dot_general(
            q[b], keys, (((1,), (1,)), ((), ())), preferred_element_type=F32
        )
    for b in range(n):
        rows = slice(b * GROUP, (b + 1) * GROUP)
        visible = seen[b : b + 1] > 0
        score = jnp.where(visible, scores[rows], NEG)
        top = jnp.max(score, axis=1, keepdims=True)
        weight = jnp.where(visible, jnp.exp(score - top), 0.0)
        total = jnp.sum(weight, axis=1, keepdims=True)
        weights[rows] = weight.astype(BF16)
        at = b * ROWS + GROUP
        out[at : at + 1] = as_row(top, mask)
        out[at + 1 : at + 2] = as_row(total, mask)
    for b in range(n):
        slab = slabs[head, b]
        values = jnp.concatenate([cache[slab, 1] for cache in caches], axis=0)
        out[b * ROWS : b * ROWS + GROUP] = jnp.dot(
            weights[b * GROUP : (b + 1) * GROUP], values, preferred_element_type=F32
        )


def combine_kernel(parts, new_score, new_value, out):
    n = parts.shape[0] // ROWS
    mask = diagonal(GROUP)
    lanes = lax.broadcasted_iota(jnp.int32, (1, HD), 1) < GROUP
    tops = parts[pl.ds(GROUP, n, stride=ROWS), :]
    totals = parts[pl.ds(GROUP + 1, n, stride=ROWS), :]
    fresh = new_score[...]
    top = jnp.maximum(jnp.max(tops, axis=0, keepdims=True), fresh)
    share = jnp.where(lanes, jnp.exp(tops - top), 0.0)
    fresh_weight = jnp.where(lanes, jnp.exp(fresh - top), 0.0)
    total = jnp.sum(share * totals, axis=0, keepdims=True) + fresh_weight
    weighted = column(fresh_weight, mask).astype(BF16).astype(F32) * new_value[...]
    for k in range(n):
        at = k * ROWS
        weighted = weighted + column(share[k : k + 1], mask) * parts[at : at + GROUP]
    done = (weighted / column(total, mask)).astype(BF16)
    out[...] = jnp.broadcast_to(done[None], out.shape)


def rows_kernel(heads, out, wide):
    wide[...] = heads[...].astype(F32)
    for k in range(GROUP):
        out[:, k * HD : (k + 1) * HD] = wide[:, k, :].astype(BF16)


def output_near_kernel(place, a, b, wo, x, out, w_far, w, sems, far_sems):
    near = out_copies(place, NEAR, wo, w, sems)
    far = out_copies(place, FAR, wo, w_far, far_sems)
    for copy in near + far:
        copy.start()
    for copy in near:
        copy.wait()
    total = x[...].astype(F32)
    for k, rows in enumerate((a, b)):
        total = total + jnp.dot(rows[...], w[k], preferred_element_type=F32)
    out[...] = total
    for copy in far:
        copy.wait()


def output_far_kernel(*refs):
    near, *rows, w, out = refs
    total = near[...]
    for k, block in enumerate(rows):
        total = total + jnp.dot(block[...], w[k], preferred_element_type=F32)
    out[...] = total.astype(BF16)


def shift_x(value, by):
    return lax.ppermute(value, "x", [(i, (i + by) % NX) for i in range(NX)])


def swap_c(value):
    return lax.ppermute(value, "c", [(0, 1), (1, 0)])


def across_z(value):
    return lax.all_to_all(value, "z", 0, 0, tiled=True)


def step(hidden_in, norm_gain, w_q, w_kv, w_o, kv_cache, lengths, slab_index):
    n, depth = hidden_in.shape
    members = NX * NZ * NC
    w_q, w_kv, w_o, kv_cache = (
        pltpu.with_memory_space_constraint(v, pltpu.HBM) for v in (w_q, w_kv, w_o, kv_cache)
    )
    place = jnp.stack([lax.axis_index(a) for a in TENSOR]).astype(jnp.int32)

    mine = jnp.arange(n, dtype=jnp.int32) == lax.axis_index("z")
    position = jnp.sum(jnp.where(mine, lengths, 0)).astype(F32)
    lane = jnp.arange(HD, dtype=jnp.int32)[None]
    frequency = ROPE_BASE ** (-2.0 * (lane % (HD // 2)).astype(F32) / HD)
    angles = position * frequency
    cosine = jnp.cos(angles)
    sine = jnp.sin(angles) * jnp.where(lane < HD // 2, -1.0, 1.0)

    sums = call(squares_kernel, struct((members, HD), F32), [VMEM], hidden_in, params=None)
    sums = lax.all_to_all(
        sums.reshape(members, 1, HD), TENSOR, 0, 0, tiled=True
    ).reshape(members, HD)

    half = struct((NX, depth, PW), BF16)
    dmas = pltpu.SemaphoreType.DMA((NX, 3))
    w_theirs = call(fetch_in_kernel, half, [SMEM, HBM, HBM], place, w_q, w_kv, scratch=[dmas])

    cache = []
    for moves in (MOVES[:EARLY], MOVES[EARLY:]):
        block = kv_cache.shape[1:]
        cache += call(
            functools.partial(fetch_cache_kernel, moves),
            [struct(block, BF16) if move == (0, 0) else pltpu.HBM(block, BF16) for move in moves],
            [SMEM, HBM],
            place,
            kv_cache,
            scratch=[
                pltpu.VMEM((len(moves),) + block, BF16),
                pltpu.SemaphoreType.DMA((len(moves),)),
                pltpu.SemaphoreType.DMA((len(moves),)),
            ],
        )

    local = kv_cache.shape[3]
    seen = len(MOVES) * local
    positions = call(
        functools.partial(positions_kernel, local, 0, EARLY),
        struct((1, seen), jnp.int32),
        [SMEM, VMEM],
        place,
        jnp.zeros((1, seen), jnp.int32),
    )

    product = struct((NX, n, PW), F32)
    normed, sent = call(
        project_first_kernel,
        [struct((n, depth), BF16), product],
        [VMEM] * 4,
        sums,
        hidden_in,
        norm_gain[None],
        w_theirs,
    )
    got = swap_c(sent)
    kept = call(
        project_kernel,
        product,
        [SMEM, VMEM, HBM, HBM],
        place,
        normed,
        w_q,
        w_kv,
        scratch=[pltpu.VMEM(half.shape, BF16), dmas],
    )
    blocks = call(pair_sum_kernel, [struct((n, PW), F32)] * NX, [VMEM] * 2, kept, got)
    parts = [blocks[0]]
    for k in (1, 3, 2):
        parts.append(shift_x(blocks[k], k))
    rows = call(x_sum_kernel, struct((n * ROWS, HD), F32), [VMEM] * NX, *parts)
    for k, (j, d) in enumerate(MOVES[1:], 1):
        pairs = [
            (x * NC + c, (x + j) % NX * NC + (c + d) % NC)
            for x in range(NX)
            for c in range(NC)
        ]
        cache[k] = lax.ppermute(cache[k], ("x", "c"), pairs)
    positions = call(
        functools.partial(positions_kernel, local, EARLY, len(MOVES)),
        struct((1, seen), jnp.int32),
        [SMEM, VMEM],
        place,
        positions,
    )
    rows = across_z(rows.reshape(n, 1, PW)).reshape(n * ROWS, HD)
    q, new_score, new_value = call(
        queries_kernel,
        [struct((n, GROUP, HD), BF16), struct((1, HD), F32), struct((1, HD), F32)],
        [VMEM] * 3,
        rows,
        cosine,
        sine,
    )
    q = across_z(q)

    visible = call(
        functools.partial(visible_kernel, local),
        struct((n, seen), F32),
        [SMEM, VMEM, VMEM],
        lengths,
        positions,
        q,
    )
    partial = call(
        attend_kernel,
        struct((n * ROWS, HD), F32),
        [SMEM, SMEM] + [VMEM] * (2 + len(MOVES)),
        place,
        slab_index,
        visible,
        q,
        *cache,
        scratch=[pltpu.VMEM((n * GROUP, seen), F32), pltpu.VMEM((n * GROUP, seen), BF16)],
    )
    partial = across_z(partial.reshape(n, 1, PW)).reshape(n * ROWS, HD)
    done = call(
        combine_kernel, struct((n, GROUP, HD), BF16), [VMEM] * 3, partial, new_score, new_value
    )
    done = across_z(done)
    done = call(
        rows_kernel,
        struct((n, QW), BF16),
        [VMEM],
        done,
        scratch=[pltpu.VMEM((n, GROUP, HD), F32)],
    )
    rows = {(0, 0): done}
    for k in (1, 3, 2):
        rows[k, 0] = shift_x(done, -k)
    for k in (0, 1, 3, 2):
        rows[k, 1] = swap_c(rows[k, 0])
    total, w_far = call(
        output_near_kernel,
        [struct((n, depth), F32), struct((len(FAR), QW, w_o.shape[1]), BF16)],
        [SMEM, VMEM, VMEM, HBM, VMEM],
        place,
        *(rows[move] for move in NEAR),
        w_o,
        hidden_in,
        scratch=[
            pltpu.VMEM((len(NEAR), QW, w_o.shape[1]), BF16),
            pltpu.SemaphoreType.DMA((len(NEAR),)),
            pltpu.SemaphoreType.DMA((len(FAR),)),
        ],
    )
    return call(
        output_far_kernel,
        struct((n, depth), BF16),
        [VMEM] * (2 + len(FAR)),
        total,
        *(rows[move] for move in FAR),
        w_far,
    )


def solution(mesh):
    torus = Mesh(
        mesh.devices.reshape(mesh.shape["groups"], NX, NZ, NC),
        ("groups",) + TENSOR,
    )
    placed = (
        P("groups", TENSOR),
        P(TENSOR),
        P(TENSOR, None),
        P(TENSOR, None),
        P(None, TENSOR),
        P(None, "groups", None, TENSOR, None),
        P("groups"),
        P(None, "groups"),
    )
    return jax.shard_map(
        step, mesh=torus, in_specs=placed, out_specs=P("groups", TENSOR), check_vma=False
    )
```

```python
import functools

import jax
import jax.numpy as jnp
from jax import lax
from jax.experimental import pallas as pl
from jax.experimental.pallas import tpu as pltpu
from jax.sharding import Mesh
from jax.sharding import PartitionSpec as P

NX, NZ, NC = 4, 16, 2
KVH = NX * NC
HD = 128
GROUP = 16
ROWS = GROUP + 2
QW = GROUP * HD
PW = ROWS * HD
MODEL = KVH * QW
TENSOR = ("x", "z", "c")
FIRST = ((0, 1), (1, 1), (2, 1), (3, 1))
REST = ((0, 0), (1, 0), (2, 0), (3, 0))
NEAR = ((0, 0), (0, 1))
FAR = ((1, 0), (3, 0), (2, 0), (1, 1), (3, 1), (2, 1))
MOVES = ((0, 0), (0, 1), (1, 0), (3, 0), (2, 0), (1, 1), (3, 1), (2, 1))
EARLY = 4

EPS = 1e-05
ROPE_BASE = 500000.0
SCALE = 1.0 / HD**0.5
NEG = -1e30


F32, BF16 = jnp.float32, jnp.bfloat16
VMEM = pl.BlockSpec(memory_space=pltpu.VMEM)
SMEM = pl.BlockSpec(memory_space=pltpu.SMEM)
HBM = pl.BlockSpec(memory_space=pltpu.HBM)
LIMIT = pltpu.CompilerParams(vmem_limit_bytes=16 * 2**20)


def struct(shape, dtype):
    return jax.ShapeDtypeStruct(shape, dtype)


def call(kernel, out, specs, *args, scratch=(), params=LIMIT):
    is_out = lambda v: not isinstance(v, (list, tuple))
    outs = jax.tree.map(lambda v: VMEM if isinstance(v, jax.ShapeDtypeStruct) else HBM, out, is_leaf=is_out)
    return pl.pallas_call(
        kernel,
        in_specs=specs,
        out_specs=outs,
        out_shape=out,
        scratch_shapes=scratch,
        compiler_params=params,
    )(*args)


def diagonal(rows):
    lane = lax.broadcasted_iota(jnp.int32, (rows, HD), 1)
    return lane == lax.broadcasted_iota(jnp.int32, (rows, HD), 0)


def column(row, mask):
    return jnp.sum(jnp.where(mask, row, 0.0), axis=1, keepdims=True)


def as_row(col, mask):
    return jnp.sum(jnp.where(mask, col, 0.0), axis=0, keepdims=True)


def squares_kernel(x, out):
    stream = x[...].astype(F32)
    total = jnp.sum(stream * stream, axis=1, keepdims=True)
    out[...] = as_row(total, diagonal(x.shape[0]))


def spread_kernel(a, b, c, d, out):
    out[...] = jnp.broadcast_to((a[...] + b[...]) + (c[...] + d[...]), out.shape)


def head_of(place, j, d):
    core = 1 - place[2] if d else place[2]
    return lax.rem(place[0] + j, NX) * NC + core


def in_copies(place, moves, wq, wkv, out, sems):
    copies = []
    for k, (j, d) in enumerate(moves):
        head = head_of(place, j, d)
        for part, (source, start, width, at) in enumerate(
            (
                (wq, head * QW, QW, 0),
                (wkv, head * HD, HD, QW),
                (wkv, (KVH + head) * HD, HD, QW + HD),
            )
        ):
            copies.append(
                pltpu.make_async_copy(
                    source.at[:, pl.ds(pl.multiple_of(start, HD), width)],
                    out.at[k, :, pl.ds(at, width)],
                    sems.at[k, part],
                )
            )
    return copies


def out_copies(place, moves, wo, out, sems):
    return [
        pltpu.make_async_copy(
            wo.at[pl.ds(pl.multiple_of(head_of(place, j, d) * QW, HD), QW)],
            out.at[k],
            sems.at[k],
        )
        for k, (j, d) in enumerate(moves)
    ]


def run_all(copies):
    for copy in copies:
        copy.start()
    for copy in copies:
        copy.wait()


def fetch_in_kernel(place, wq, wkv, out, sems):
    run_all(in_copies(place, FIRST, wq, wkv, out, sems))


def fetch_cache_kernel(moves, place, cache, *refs):
    outs, held, sems, out_sems = refs[:-3], *refs[-3:]
    first, second = [], []
    for k, (j, d) in enumerate(moves):
        stays = (j, d) == (0, 0)
        to = outs[k] if stays else held.at[k]
        first.append(pltpu.make_async_copy(cache.at[head_of(place, j, d)], to, sems.at[k]))
        first[k].start()
    for k, move in enumerate(moves):
        first[k].wait()
        if move != (0, 0):
            second.append(pltpu.make_async_copy(held.at[k], outs[k], out_sems.at[k]))
            second[-1].start()
    for copy in second:
        copy.wait()


def project_first_kernel(sums, x, gain, w, normed_out, out):
    squares = column(jnp.sum(sums[...], axis=0, keepdims=True), diagonal(x.shape[0]))
    stream = x[...].astype(F32)
    normed = (stream * lax.rsqrt(squares / MODEL + EPS) * gain[...].astype(F32)).astype(BF16)
    normed_out[...] = normed
    for k in range(NX):
        out[k] = jnp.dot(normed, w[k], preferred_element_type=F32)


def project_kernel(place, normed, wq, wkv, out, w, sems):
    copies = in_copies(place, REST, wq, wkv, w, sems)
    for copy in copies:
        copy.start()
    for k in range(NX):
        for copy in copies[3 * k : 3 * k + 3]:
            copy.wait()
        out[k] = jnp.dot(normed[...], w[k], preferred_element_type=F32)


def pair_sum_kernel(a, b, *outs):
    for k, out in enumerate(outs):
        out[...] = a[k] + b[k]


def x_sum_kernel(a, b, c, d, out):
    n = a.shape[0]
    for k in range(ROWS):
        cut = slice(k * HD, (k + 1) * HD)
        total = (a[:, cut] + b[:, cut]) + (c[:, cut] + d[:, cut])
        out[pl.ds(k, n, stride=ROWS), :] = total


def queries_kernel(parts, cosine, sine, q_out, new_score, new_value):
    n = parts.shape[0] // ROWS
    total = parts[:ROWS]
    for k in range(1, n):
        total = total + parts[k * ROWS : (k + 1) * ROWS]
    lead = total[: GROUP + 1]
    turned = lead * cosine[...] + pltpu.roll(lead, HD // 2, 1) * sine[...]
    turned = turned.astype(BF16)
    q = turned[:GROUP]
    q_out[...] = jnp.broadcast_to(q[None], q_out.shape)
    key = turned[GROUP : GROUP + 1].astype(F32)
    score = jnp.sum(q.astype(F32) * key, axis=1, keepdims=True) * SCALE
    new_score[...] = as_row(score, diagonal(GROUP))
    new_value[...] = total[GROUP + 1 :].astype(BF16).astype(F32)


def positions_kernel(local, first, last, place, base, out):
    index = lax.broadcasted_iota(jnp.int32, out.shape, 1)
    start = base[...]
    for k, (j, d) in list(enumerate(MOVES))[first:last]:
        core = 1 - place[2] if d else place[2]
        block = (lax.rem(place[0] + (NX - j), NX) * NZ + place[1]) * NC + core
        start = jnp.where(index // local == k, block * local, start)
    out[...] = start


def visible_kernel(local, lengths, positions, q, out):
    del q
    here = positions[...] + lax.broadcasted_iota(jnp.int32, positions.shape, 1) % local
    for b in range(out.shape[0]):
        out[b : b + 1] = (here < lengths[b]).astype(F32)


def attend_kernel(place, slabs, seen, q, *refs):
    caches, out, scores, weights = refs[: len(MOVES)], *refs[len(MOVES) :]
    n = q.shape[0]
    head = place[0] * NC + place[2]
    mask = diagonal(GROUP)
    for b in range(n):
        slab = slabs[head, b]
        keys = jnp.concatenate([cache[slab, 0] for cache in caches], axis=0)
        scores[b * GROUP : (b + 1) * GROUP] = SCALE * lax.dot_general(
            q[b], keys, (((1,), (1,)), ((), ())), preferred_element_type=F32
        )
    for b in range(n):
        rows = slice(b * GROUP, (b + 1) * GROUP)
        visible = seen[b : b + 1] > 0
        score = jnp.where(visible, scores[rows], NEG)
        top = jnp.max(score, axis=1, keepdims=True)
        weight = jnp.where(visible, jnp.exp(score - top), 0.0)
        total = jnp.sum(weight, axis=1, keepdims=True)
        weights[rows] = weight.astype(BF16)
        at = b * ROWS + GROUP
        out[at : at + 1] = as_row(top, mask)
        out[at + 1 : at + 2] = as_row(total, mask)
    for b in range(n):
        slab = slabs[head, b]
        values = jnp.concatenate([cache[slab, 1] for cache in caches], axis=0)
        out[b * ROWS : b * ROWS + GROUP] = jnp.dot(
            weights[b * GROUP : (b + 1) * GROUP], values, preferred_element_type=F32
        )


def combine_kernel(parts, new_score, new_value, out):
    n = parts.shape[0] // ROWS
    mask = diagonal(GROUP)
    lanes = lax.broadcasted_iota(jnp.int32, (1, HD), 1) < GROUP
    tops = parts[pl.ds(GROUP, n, stride=ROWS), :]
    totals = parts[pl.ds(GROUP + 1, n, stride=ROWS), :]
    fresh = new_score[...]
    top = jnp.maximum(jnp.max(tops, axis=0, keepdims=True), fresh)
    share = jnp.where(lanes, jnp.exp(tops - top), 0.0)
    fresh_weight = jnp.where(lanes, jnp.exp(fresh - top), 0.0)
    total = jnp.sum(share * totals, axis=0, keepdims=True) + fresh_weight
    weighted = column(fresh_weight, mask).astype(BF16).astype(F32) * new_value[...]
    for k in range(n):
        at = k * ROWS
        weighted = weighted + column(share[k : k + 1], mask) * parts[at : at + GROUP]
    done = (weighted / column(total, mask)).astype(BF16)
    out[...] = jnp.broadcast_to(done[None], out.shape)


def rows_kernel(heads, out, wide):
    wide[...] = heads[...].astype(F32)
    for k in range(GROUP):
        out[:, k * HD : (k + 1) * HD] = wide[:, k, :].astype(BF16)


def output_near_kernel(place, a, b, wo, x, out, w_far, w, sems, far_sems):
    near = out_copies(place, NEAR, wo, w, sems)
    far = out_copies(place, FAR, wo, w_far, far_sems)
    for copy in near + far:
        copy.start()
    for copy in near:
        copy.wait()
    total = x[...].astype(F32)
    for k, rows in enumerate((a, b)):
        total = total + jnp.dot(rows[...], w[k], preferred_element_type=F32)
    out[...] = total
    for copy in far:
        copy.wait()


def output_far_kernel(*refs):
    near, *rows, w, out = refs
    total = near[...]
    for k, block in enumerate(rows):
        total = total + jnp.dot(block[...], w[k], preferred_element_type=F32)
    out[...] = total.astype(BF16)


def shift_x(value, by):
    return lax.ppermute(value, "x", [(i, (i + by) % NX) for i in range(NX)])


def swap_c(value):
    return lax.ppermute(value, "c", [(0, 1), (1, 0)])


def across_z(value):
    return lax.all_to_all(value, "z", 0, 0, tiled=True)


def step(hidden_in, norm_gain, w_q, w_kv, w_o, kv_cache, lengths, slab_index):
    n, depth = hidden_in.shape
    w_q, w_kv, w_o, kv_cache = (
        pltpu.with_memory_space_constraint(v, pltpu.HBM) for v in (w_q, w_kv, w_o, kv_cache)
    )
    place = jnp.stack([lax.axis_index(a) for a in TENSOR]).astype(jnp.int32)

    mine = jnp.arange(n, dtype=jnp.int32) == lax.axis_index("z")
    position = jnp.sum(jnp.where(mine, lengths, 0)).astype(F32)
    lane = jnp.arange(HD, dtype=jnp.int32)[None]
    frequency = ROPE_BASE ** (-2.0 * (lane % (HD // 2)).astype(F32) / HD)
    angles = position * frequency
    cosine = jnp.cos(angles)
    sine = jnp.sin(angles) * jnp.where(lane < HD // 2, -1.0, 1.0)

    line = struct((1, HD), F32)
    own = call(squares_kernel, line, [VMEM], hidden_in, params=None)
    lines = [own]
    for k in (1, 3, 2):
        lines.append(shift_x(own, k))
    sums = call(spread_kernel, struct((NZ * NC, HD), F32), [VMEM] * NX, *lines)
    sums = lax.all_to_all(
        sums.reshape(NZ * NC, 1, HD), ("z", "c"), 0, 0, tiled=True
    ).reshape(NZ * NC, HD)

    dmas = lambda moves: pltpu.SemaphoreType.DMA((len(moves), 3))
    held = call(
        fetch_in_kernel,
        struct((len(FIRST), depth, PW), BF16),
        [SMEM, HBM, HBM],
        place,
        w_q,
        w_kv,
        scratch=[dmas(FIRST)],
    )

    cache = []
    for moves in (MOVES[:EARLY], MOVES[EARLY:]):
        block = kv_cache.shape[1:]
        cache += call(
            functools.partial(fetch_cache_kernel, moves),
            [struct(block, BF16) if move == (0, 0) else pltpu.HBM(block, BF16) for move in moves],
            [SMEM, HBM],
            place,
            kv_cache,
            scratch=[
                pltpu.VMEM((len(moves),) + block, BF16),
                pltpu.SemaphoreType.DMA((len(moves),)),
                pltpu.SemaphoreType.DMA((len(moves),)),
            ],
        )

    local = kv_cache.shape[3]
    seen = len(MOVES) * local
    positions = call(
        functools.partial(positions_kernel, local, 0, EARLY),
        struct((1, seen), jnp.int32),
        [SMEM, VMEM],
        place,
        jnp.zeros((1, seen), jnp.int32),
    )

    product = struct((NX, n, PW), F32)
    normed, sent = call(
        project_first_kernel,
        [struct((n, depth), BF16), product],
        [VMEM] * 4,
        sums,
        hidden_in,
        norm_gain[None],
        held,
    )
    got = swap_c(sent)
    kept = call(
        project_kernel,
        product,
        [SMEM, VMEM, HBM, HBM],
        place,
        normed,
        w_q,
        w_kv,
        scratch=[pltpu.VMEM((len(REST), depth, PW), BF16), dmas(REST)],
    )
    blocks = call(pair_sum_kernel, [struct((n, PW), F32)] * NX, [VMEM] * 2, kept, got)
    parts = [blocks[0]]
    for k in (1, 3, 2):
        parts.append(shift_x(blocks[k], k))
    rows = call(x_sum_kernel, struct((n * ROWS, HD), F32), [VMEM] * NX, *parts)
    for k, (j, d) in enumerate(MOVES[1:], 1):
        pairs = [
            (x * NC + c, (x + j) % NX * NC + (c + d) % NC)
            for x in range(NX)
            for c in range(NC)
        ]
        cache[k] = lax.ppermute(cache[k], ("x", "c"), pairs)
    positions = call(
        functools.partial(positions_kernel, local, EARLY, len(MOVES)),
        struct((1, seen), jnp.int32),
        [SMEM, VMEM],
        place,
        positions,
    )
    rows = across_z(rows.reshape(n, 1, PW)).reshape(n * ROWS, HD)
    q, new_score, new_value = call(
        queries_kernel,
        [struct((n, GROUP, HD), BF16), struct((1, HD), F32), struct((1, HD), F32)],
        [VMEM] * 3,
        rows,
        cosine,
        sine,
    )
    q = across_z(q)

    visible = call(
        functools.partial(visible_kernel, local),
        struct((n, seen), F32),
        [SMEM, VMEM, VMEM],
        lengths,
        positions,
        q,
    )
    partial = call(
        attend_kernel,
        struct((n * ROWS, HD), F32),
        [SMEM, SMEM] + [VMEM] * (2 + len(MOVES)),
        place,
        slab_index,
        visible,
        q,
        *cache,
        scratch=[pltpu.VMEM((n * GROUP, seen), F32), pltpu.VMEM((n * GROUP, seen), BF16)],
    )
    partial = across_z(partial.reshape(n, 1, PW)).reshape(n * ROWS, HD)
    done = call(
        combine_kernel, struct((n, GROUP, HD), BF16), [VMEM] * 3, partial, new_score, new_value
    )
    done = across_z(done)
    done = call(
        rows_kernel,
        struct((n, QW), BF16),
        [VMEM],
        done,
        scratch=[pltpu.VMEM((n, GROUP, HD), F32)],
    )
    rows = {(0, 0): done}
    for k in (1, 3, 2):
        rows[k, 0] = shift_x(done, -k)
    for k in (0, 1, 3, 2):
        rows[k, 1] = swap_c(rows[k, 0])
    total, w_far = call(
        output_near_kernel,
        [struct((n, depth), F32), struct((len(FAR), QW, w_o.shape[1]), BF16)],
        [SMEM, VMEM, VMEM, HBM, VMEM],
        place,
        *(rows[move] for move in NEAR),
        w_o,
        hidden_in,
        scratch=[
            pltpu.VMEM((len(NEAR), QW, w_o.shape[1]), BF16),
            pltpu.SemaphoreType.DMA((len(NEAR),)),
            pltpu.SemaphoreType.DMA((len(FAR),)),
        ],
    )
    return call(
        output_far_kernel,
        struct((n, depth), BF16),
        [VMEM] * (2 + len(FAR)),
        total,
        *(rows[move] for move in FAR),
        w_far,
    )


def solution(mesh):
    torus = Mesh(
        mesh.devices.reshape(mesh.shape["groups"], NX, NZ, NC),
        ("groups",) + TENSOR,
    )
    placed = (
        P("groups", TENSOR),
        P(TENSOR),
        P(TENSOR, None),
        P(TENSOR, None),
        P(None, TENSOR),
        P(None, "groups", None, TENSOR, None),
        P("groups"),
        P(None, "groups"),
    )
    return jax.shard_map(
        step, mesh=torus, in_specs=placed, out_specs=P("groups", TENSOR), check_vma=False
    )
```

```python
import functools

import jax
import jax.numpy as jnp
from jax import lax
from jax.experimental import pallas as pl
from jax.experimental.pallas import tpu as pltpu
from jax.sharding import Mesh
from jax.sharding import PartitionSpec as P

NX, NZ, NC = 4, 16, 2
KVH = NX * NC
HD = 128
GROUP = 16
ROWS = GROUP + 2
QW = GROUP * HD
PW = ROWS * HD
MODEL = KVH * QW
TENSOR = ("x", "z", "c")
FIRST = ((0, 1), (1, 1), (2, 1), (3, 1))
REST = ((0, 0), (1, 0), (2, 0), (3, 0))
NEAR = ((0, 0), (0, 1))
SIDE = ((1, 0), (3, 0), (2, 0))
ACROSS = ((1, 1), (3, 1), (2, 1))
MOVES = ((0, 0), (0, 1), (1, 0), (3, 0), (2, 0), (1, 1), (3, 1), (2, 1))
EARLY = 4

EPS = 1e-05
ROPE_BASE = 500000.0
SCALE = 1.0 / HD**0.5
NEG = -1e30


F32, BF16 = jnp.float32, jnp.bfloat16
VMEM = pl.BlockSpec(memory_space=pltpu.VMEM)
SMEM = pl.BlockSpec(memory_space=pltpu.SMEM)
HBM = pl.BlockSpec(memory_space=pltpu.HBM)
LIMIT = pltpu.CompilerParams(vmem_limit_bytes=16 * 2**20)


def struct(shape, dtype):
    return jax.ShapeDtypeStruct(shape, dtype)


def call(kernel, out, specs, *args, scratch=(), params=LIMIT):
    is_out = lambda v: not isinstance(v, (list, tuple))
    outs = jax.tree.map(lambda v: VMEM if isinstance(v, jax.ShapeDtypeStruct) else HBM, out, is_leaf=is_out)
    return pl.pallas_call(
        kernel,
        in_specs=specs,
        out_specs=outs,
        out_shape=out,
        scratch_shapes=scratch,
        compiler_params=params,
    )(*args)


def diagonal(rows):
    lane = lax.broadcasted_iota(jnp.int32, (rows, HD), 1)
    return lane == lax.broadcasted_iota(jnp.int32, (rows, HD), 0)


def column(row, mask):
    return jnp.sum(jnp.where(mask, row, 0.0), axis=1, keepdims=True)


def as_row(col, mask):
    return jnp.sum(jnp.where(mask, col, 0.0), axis=0, keepdims=True)


def squares_kernel(x, out):
    stream = x[...].astype(F32)
    total = jnp.sum(stream * stream, axis=1, keepdims=True)
    out[...] = as_row(total, diagonal(x.shape[0]))


def spread_kernel(a, b, c, d, out):
    out[...] = jnp.broadcast_to((a[...] + b[...]) + (c[...] + d[...]), out.shape)


def head_of(place, j, d):
    core = 1 - place[2] if d else place[2]
    return lax.rem(place[0] + j, NX) * NC + core


def in_copies(place, moves, wq, wkv, out, sems):
    copies = []
    for k, (j, d) in enumerate(moves):
        head = head_of(place, j, d)
        for part, (source, start, width, at) in enumerate(
            (
                (wq, head * QW, QW, 0),
                (wkv, head * HD, HD, QW),
                (wkv, (KVH + head) * HD, HD, QW + HD),
            )
        ):
            copies.append(
                pltpu.make_async_copy(
                    source.at[:, pl.ds(pl.multiple_of(start, HD), width)],
                    out.at[k, :, pl.ds(at, width)],
                    sems.at[k, part],
                )
            )
    return copies


def out_copies(place, moves, wo, out, sems):
    return [
        pltpu.make_async_copy(
            wo.at[pl.ds(pl.multiple_of(head_of(place, j, d) * QW, HD), QW)],
            out.at[k],
            sems.at[k],
        )
        for k, (j, d) in enumerate(moves)
    ]


def run_all(copies):
    for copy in copies:
        copy.start()
    for copy in copies:
        copy.wait()


def fetch_in_kernel(place, wq, wkv, out, sems):
    run_all(in_copies(place, FIRST, wq, wkv, out, sems))


def fetch_cache_kernel(moves, staged, place, cache, *refs):
    outs, held, sems, out_sems = refs[:-3], *refs[-3:]
    first, second = [], []
    for k, (j, d) in enumerate(moves):
        to = held.at[k] if k in staged else outs[k]
        first.append(pltpu.make_async_copy(cache.at[head_of(place, j, d)], to, sems.at[k]))
        first[k].start()
    for k in range(len(moves)):
        first[k].wait()
        if k in staged:
            second.append(pltpu.make_async_copy(held.at[k], outs[k], out_sems.at[k]))
            second[-1].start()
    for copy in second:
        copy.wait()


def project_first_kernel(sums, x, gain, w, normed_out, out):
    squares = column(jnp.sum(sums[...], axis=0, keepdims=True), diagonal(x.shape[0]))
    stream = x[...].astype(F32)
    normed = (stream * lax.rsqrt(squares / MODEL + EPS) * gain[...].astype(F32)).astype(BF16)
    normed_out[...] = normed
    for k in range(NX):
        out[k] = jnp.dot(normed, w[k], preferred_element_type=F32)


def project_kernel(place, normed, wq, wkv, out, w, sems):
    copies = in_copies(place, REST, wq, wkv, w, sems)
    for copy in copies:
        copy.start()
    for k in range(NX):
        for copy in copies[3 * k : 3 * k + 3]:
            copy.wait()
        out[k] = jnp.dot(normed[...], w[k], preferred_element_type=F32)


def pair_sum_kernel(a, b, *outs):
    for k, out in enumerate(outs):
        out[...] = a[k] + b[k]


def x_sum_kernel(a, b, c, d, out):
    n = a.shape[0]
    for k in range(ROWS):
        cut = slice(k * HD, (k + 1) * HD)
        total = (a[:, cut] + b[:, cut]) + (c[:, cut] + d[:, cut])
        out[pl.ds(k, n, stride=ROWS), :] = total


def queries_kernel(place, parts, cosine, sine, q_out, new_score, new_value):
    n = parts.shape[0] // ROWS
    total = parts[:ROWS]
    for k in range(1, n):
        total = total + parts[k * ROWS : (k + 1) * ROWS]
    lead = total[: GROUP + 1]
    mine = pl.ds(place[1], 1)
    turned = lead * cosine[mine] + pltpu.roll(lead, HD // 2, 1) * sine[mine]
    turned = turned.astype(BF16)
    q = turned[:GROUP]
    q_out[...] = jnp.broadcast_to(q[None], q_out.shape)
    key = turned[GROUP : GROUP + 1].astype(F32)
    score = jnp.sum(q.astype(F32) * key, axis=1, keepdims=True) * SCALE
    new_score[...] = as_row(score, diagonal(GROUP))
    new_value[...] = total[GROUP + 1 :].astype(BF16).astype(F32)


def visible_kernel(local, place, lengths, q, out):
    del q
    index = lax.broadcasted_iota(jnp.int32, (1, out.shape[1]), 1)
    position = index % local
    for k, (j, d) in enumerate(MOVES):
        core = 1 - place[2] if d else place[2]
        block = (lax.rem(place[0] + (NX - j), NX) * NZ + place[1]) * NC + core
        position = jnp.where(index // local == k, position + block * local, position)
    for b in range(out.shape[0]):
        out[b : b + 1] = (position < lengths[b]).astype(F32)


def attend_kernel(place, slabs, seen, q, *refs):
    caches, out, scores, weights = refs[: len(MOVES)], *refs[len(MOVES) :]
    n = q.shape[0]
    head = place[0] * NC + place[2]
    mask = diagonal(GROUP)
    for b in range(n):
        slab = slabs[head, b]
        keys = jnp.concatenate([cache[slab, 0] for cache in caches], axis=0)
        scores[b * GROUP : (b + 1) * GROUP] = SCALE * lax.dot_general(
            q[b], keys, (((1,), (1,)), ((), ())), preferred_element_type=F32
        )
    for b in range(n):
        rows = slice(b * GROUP, (b + 1) * GROUP)
        visible = seen[b : b + 1] > 0
        score = jnp.where(visible, scores[rows], NEG)
        top = jnp.max(score, axis=1, keepdims=True)
        weight = jnp.where(visible, jnp.exp(score - top), 0.0)
        total = jnp.sum(weight, axis=1, keepdims=True)
        weights[rows] = weight.astype(BF16)
        at = b * ROWS + GROUP
        out[at : at + 1] = as_row(top, mask)
        out[at + 1 : at + 2] = as_row(total, mask)
    for b in range(n):
        slab = slabs[head, b]
        values = jnp.concatenate([cache[slab, 1] for cache in caches], axis=0)
        out[b * ROWS : b * ROWS + GROUP] = jnp.dot(
            weights[b * GROUP : (b + 1) * GROUP], values, preferred_element_type=F32
        )


def combine_kernel(parts, new_score, new_value, out):
    n = parts.shape[0] // ROWS
    mask = diagonal(GROUP)
    lanes = lax.broadcasted_iota(jnp.int32, (1, HD), 1) < GROUP
    tops = parts[pl.ds(GROUP, n, stride=ROWS), :]
    totals = parts[pl.ds(GROUP + 1, n, stride=ROWS), :]
    fresh = new_score[...]
    top = jnp.maximum(jnp.max(tops, axis=0, keepdims=True), fresh)
    share = jnp.where(lanes, jnp.exp(tops - top), 0.0)
    fresh_weight = jnp.where(lanes, jnp.exp(fresh - top), 0.0)
    total = jnp.sum(share * totals, axis=0, keepdims=True) + fresh_weight
    weighted = column(fresh_weight, mask).astype(BF16).astype(F32) * new_value[...]
    for k in range(n):
        at = k * ROWS
        weighted = weighted + column(share[k : k + 1], mask) * parts[at : at + GROUP]
    done = (weighted / column(total, mask)).astype(BF16)
    out[...] = jnp.broadcast_to(done[None], out.shape)


def rows_kernel(heads, out, wide):
    wide[...] = heads[...].astype(F32)
    for k in range(GROUP):
        out[:, k * HD : (k + 1) * HD] = wide[:, k, :].astype(BF16)


def add_products(total, rows, w):
    for k, block in enumerate(rows):
        total = total + jnp.dot(block[...], w[k], preferred_element_type=F32)
    return total


def output_near_kernel(place, a, b, wo, x, out, w_next, w, sems, next_sems):
    near = out_copies(place, NEAR, wo, w, sems)
    after = out_copies(place, SIDE, wo, w_next, next_sems)
    for copy in near + after:
        copy.start()
    for copy in near:
        copy.wait()
    out[...] = add_products(x[...].astype(F32), (a, b), w)
    for copy in after:
        copy.wait()


def output_side_kernel(place, total, a, b, c, w, wo, out, w_next, sems):
    after = out_copies(place, ACROSS, wo, w_next, sems)
    for copy in after:
        copy.start()
    out[...] = add_products(total[...], (a, b, c), w)
    for copy in after:
        copy.wait()


def output_across_kernel(total, a, b, c, w, out):
    out[...] = add_products(total[...], (a, b, c), w).astype(BF16)


def shift_x(value, by):
    return lax.ppermute(value, "x", [(i, (i + by) % NX) for i in range(NX)])


def swap_c(value):
    return lax.ppermute(value, "c", [(0, 1), (1, 0)])


def across_z(value):
    return lax.all_to_all(value, "z", 0, 0, tiled=True)


def step(hidden_in, norm_gain, w_q, w_kv, w_o, kv_cache, lengths, slab_index):
    n, depth = hidden_in.shape
    w_q, w_kv, w_o, kv_cache = (
        pltpu.with_memory_space_constraint(v, pltpu.HBM) for v in (w_q, w_kv, w_o, kv_cache)
    )
    place = jnp.stack([lax.axis_index(a) for a in TENSOR]).astype(jnp.int32)

    lane = jnp.arange(HD, dtype=jnp.int32)[None]
    frequency = ROPE_BASE ** (-2.0 * (lane % (HD // 2)).astype(F32) / HD)
    angles = lengths.astype(F32)[:, None] * frequency
    cosine = jnp.cos(angles)
    sine = jnp.sin(angles) * jnp.where(lane < HD // 2, -1.0, 1.0)

    line = struct((1, HD), F32)
    own = call(squares_kernel, line, [VMEM], hidden_in, params=None)
    lines = [own]
    for k in (1, 3, 2):
        lines.append(shift_x(own, k))
    sums = call(spread_kernel, struct((NZ * NC, HD), F32), [VMEM] * NX, *lines)
    sums = lax.all_to_all(
        sums.reshape(NZ * NC, 1, HD), ("z", "c"), 0, 0, tiled=True
    ).reshape(NZ * NC, HD)

    dmas = lambda moves: pltpu.SemaphoreType.DMA((len(moves), 3))
    held = call(
        fetch_in_kernel,
        struct((len(FIRST), depth, PW), BF16),
        [SMEM, HBM, HBM],
        place,
        w_q,
        w_kv,
        scratch=[dmas(FIRST)],
    )

    cache = []
    for moves, staged in ((MOVES[:EARLY], range(1, EARLY)), (MOVES[EARLY:], ())):
        block = kv_cache.shape[1:]
        cache += call(
            functools.partial(fetch_cache_kernel, moves, staged),
            [
                pltpu.HBM(block, BF16) if k in staged else struct(block, BF16)
                for k in range(len(moves))
            ],
            [SMEM, HBM],
            place,
            kv_cache,
            scratch=[
                pltpu.VMEM((len(moves),) + block, BF16),
                pltpu.SemaphoreType.DMA((len(moves),)),
                pltpu.SemaphoreType.DMA((len(moves),)),
            ],
        )

    local = kv_cache.shape[3]
    seen = len(MOVES) * local
    product = struct((NX, n, PW), F32)
    normed, sent = call(
        project_first_kernel,
        [struct((n, depth), BF16), product],
        [VMEM] * 4,
        sums,
        hidden_in,
        norm_gain[None],
        held,
    )
    got = swap_c(sent)
    kept = call(
        project_kernel,
        product,
        [SMEM, VMEM, HBM, HBM],
        place,
        normed,
        w_q,
        w_kv,
        scratch=[pltpu.VMEM((len(REST), depth, PW), BF16), dmas(REST)],
    )
    blocks = call(pair_sum_kernel, [struct((n, PW), F32)] * NX, [VMEM] * 2, kept, got)
    parts = [blocks[0]]
    for k in (1, 3, 2):
        parts.append(shift_x(blocks[k], k))
    rows = call(x_sum_kernel, struct((n * ROWS, HD), F32), [VMEM] * NX, *parts)
    for k, (j, d) in enumerate(MOVES[1:], 1):
        pairs = [
            (x * NC + c, (x + j) % NX * NC + (c + d) % NC)
            for x in range(NX)
            for c in range(NC)
        ]
        cache[k] = lax.ppermute(cache[k], ("x", "c"), pairs)
    rows = across_z(rows.reshape(n, 1, PW)).reshape(n * ROWS, HD)
    q, new_score, new_value = call(
        queries_kernel,
        [struct((n, GROUP, HD), BF16), struct((1, HD), F32), struct((1, HD), F32)],
        [SMEM] + [VMEM] * 3,
        place,
        rows,
        cosine,
        sine,
    )
    q = across_z(q)

    visible = call(
        functools.partial(visible_kernel, local),
        struct((n, seen), F32),
        [SMEM, SMEM, VMEM],
        place,
        lengths,
        q,
    )
    partial = call(
        attend_kernel,
        struct((n * ROWS, HD), F32),
        [SMEM, SMEM] + [VMEM] * (2 + len(MOVES)),
        place,
        slab_index,
        visible,
        q,
        *cache,
        scratch=[pltpu.VMEM((n * GROUP, seen), F32), pltpu.VMEM((n * GROUP, seen), BF16)],
    )
    partial = across_z(partial.reshape(n, 1, PW)).reshape(n * ROWS, HD)
    done = call(
        combine_kernel, struct((n, GROUP, HD), BF16), [VMEM] * 3, partial, new_score, new_value
    )
    done = across_z(done)
    done = call(
        rows_kernel,
        struct((n, QW), BF16),
        [VMEM],
        done,
        scratch=[pltpu.VMEM((n, GROUP, HD), F32)],
    )
    rows = {(0, 0): done}
    for k in (1, 3, 2):
        rows[k, 0] = shift_x(done, -k)
    for k in (0, 1, 3, 2):
        rows[k, 1] = swap_c(rows[k, 0])
    block = (QW, w_o.shape[1])
    part = struct((n, depth), F32)
    total, w_side = call(
        output_near_kernel,
        [part, struct((len(SIDE),) + block, BF16)],
        [SMEM, VMEM, VMEM, HBM, VMEM],
        place,
        *(rows[move] for move in NEAR),
        w_o,
        hidden_in,
        scratch=[
            pltpu.VMEM((len(NEAR),) + block, BF16),
            pltpu.SemaphoreType.DMA((len(NEAR),)),
            pltpu.SemaphoreType.DMA((len(SIDE),)),
        ],
    )
    total, w_across = call(
        output_side_kernel,
        [part, struct((len(ACROSS),) + block, BF16)],
        [SMEM] + [VMEM] * 5 + [HBM],
        place,
        total,
        *(rows[move] for move in SIDE),
        w_side,
        w_o,
        scratch=[pltpu.SemaphoreType.DMA((len(ACROSS),))],
    )
    return call(
        output_across_kernel,
        struct((n, depth), BF16),
        [VMEM] * 5,
        total,
        *(rows[move] for move in ACROSS),
        w_across,
    )


def solution(mesh):
    torus = Mesh(
        mesh.devices.reshape(mesh.shape["groups"], NX, NZ, NC),
        ("groups",) + TENSOR,
    )
    placed = (
        P("groups", TENSOR),
        P(TENSOR),
        P(TENSOR, None),
        P(TENSOR, None),
        P(None, TENSOR),
        P(None, "groups", None, TENSOR, None),
        P("groups"),
        P(None, "groups"),
    )
    return jax.shard_map(
        step, mesh=torus, in_specs=placed, out_specs=P("groups", TENSOR), check_vma=False
    )
```

```python
import functools

import jax
import jax.numpy as jnp
from jax import lax
from jax.experimental import pallas as pl
from jax.experimental.pallas import tpu as pltpu
from jax.sharding import Mesh
from jax.sharding import PartitionSpec as P

NX, NZ, NC = 4, 16, 2
KVH = NX * NC
HD = 128
GROUP = 16
ROWS = GROUP + 2
QW = GROUP * HD
PW = ROWS * HD
MODEL = KVH * QW
TENSOR = ("x", "z", "c")
FIRST = ((0, 1), (1, 1), (2, 1), (3, 1))
REST = ((0, 0), (1, 0), (2, 0), (3, 0))
NEAR = ((0, 0), (0, 1))
FAR = ((1, 0), (3, 0), (2, 0), (1, 1), (3, 1), (2, 1))
MOVES = ((0, 0), (0, 1), (1, 0), (3, 0), (2, 0), (1, 1), (3, 1), (2, 1))
EARLY = 4

EPS = 1e-05
ROPE_BASE = 500000.0
SCALE = 1.0 / HD**0.5
NEG = -1e30


F32, BF16 = jnp.float32, jnp.bfloat16
VMEM = pl.BlockSpec(memory_space=pltpu.VMEM)
SMEM = pl.BlockSpec(memory_space=pltpu.SMEM)
HBM = pl.BlockSpec(memory_space=pltpu.HBM)
LIMIT = pltpu.CompilerParams(vmem_limit_bytes=16 * 2**20)


def struct(shape, dtype):
    return jax.ShapeDtypeStruct(shape, dtype)


def call(kernel, out, specs, *args, scratch=(), params=LIMIT):
    is_out = lambda v: not isinstance(v, (list, tuple))
    outs = jax.tree.map(lambda v: VMEM if isinstance(v, jax.ShapeDtypeStruct) else HBM, out, is_leaf=is_out)
    return pl.pallas_call(
        kernel,
        in_specs=specs,
        out_specs=outs,
        out_shape=out,
        scratch_shapes=scratch,
        compiler_params=params,
    )(*args)


def diagonal(rows):
    lane = lax.broadcasted_iota(jnp.int32, (rows, HD), 1)
    return lane == lax.broadcasted_iota(jnp.int32, (rows, HD), 0)


def column(row, mask):
    return jnp.sum(jnp.where(mask, row, 0.0), axis=1, keepdims=True)


def as_row(col, mask):
    return jnp.sum(jnp.where(mask, col, 0.0), axis=0, keepdims=True)


def squares_kernel(x, out):
    stream = x[...].astype(F32)
    total = jnp.sum(stream * stream, axis=1, keepdims=True)
    out[...] = as_row(total, diagonal(x.shape[0]))


def spread_kernel(a, b, c, d, out):
    out[...] = jnp.broadcast_to((a[...] + b[...]) + (c[...] + d[...]), out.shape)


def head_of(place, j, d):
    core = 1 - place[2] if d else place[2]
    return lax.rem(place[0] + j, NX) * NC + core


def in_copies(place, moves, wq, wkv, out, sems):
    copies = []
    for k, (j, d) in enumerate(moves):
        head = head_of(place, j, d)
        for part, (source, start, width, at) in enumerate(
            (
                (wq, head * QW, QW, 0),
                (wkv, head * HD, HD, QW),
                (wkv, (KVH + head) * HD, HD, QW + HD),
            )
        ):
            copies.append(
                pltpu.make_async_copy(
                    source.at[:, pl.ds(pl.multiple_of(start, HD), width)],
                    out.at[k, :, pl.ds(at, width)],
                    sems.at[k, part],
                )
            )
    return copies


def out_copies(place, moves, wo, out, sems):
    return [
        pltpu.make_async_copy(
            wo.at[pl.ds(pl.multiple_of(head_of(place, j, d) * QW, HD), QW)],
            out.at[k],
            sems.at[k],
        )
        for k, (j, d) in enumerate(moves)
    ]


def run_all(copies):
    for copy in copies:
        copy.start()
    for copy in copies:
        copy.wait()


def fetch_in_kernel(place, wq, wkv, out, sems):
    run_all(in_copies(place, FIRST, wq, wkv, out, sems))


def fetch_cache_kernel(moves, staged, place, cache, *refs):
    outs, held, sems, out_sems = refs[:-3], *refs[-3:]
    first, second = [], []
    for k, (j, d) in enumerate(moves):
        to = held.at[k] if k in staged else outs[k]
        first.append(pltpu.make_async_copy(cache.at[head_of(place, j, d)], to, sems.at[k]))
        first[k].start()
    for k in range(len(moves)):
        first[k].wait()
        if k in staged:
            second.append(pltpu.make_async_copy(held.at[k], outs[k], out_sems.at[k]))
            second[-1].start()
    for copy in second:
        copy.wait()


def project_first_kernel(sums, x, gain, w, normed_out, out):
    squares = column(jnp.sum(sums[...], axis=0, keepdims=True), diagonal(x.shape[0]))
    stream = x[...].astype(F32)
    normed = (stream * lax.rsqrt(squares / MODEL + EPS) * gain[...].astype(F32)).astype(BF16)
    normed_out[...] = normed
    for k in range(NX):
        out[k] = jnp.dot(normed, w[k], preferred_element_type=F32)


def project_kernel(place, normed, wq, wkv, out, w, sems):
    copies = in_copies(place, REST, wq, wkv, w, sems)
    for copy in copies:
        copy.start()
    for k in range(NX):
        for copy in copies[3 * k : 3 * k + 3]:
            copy.wait()
        out[k] = jnp.dot(normed[...], w[k], preferred_element_type=F32)


def pair_sum_kernel(a, b, *outs):
    for k, out in enumerate(outs):
        out[...] = a[k] + b[k]


def x_sum_kernel(a, b, c, d, out):
    n = a.shape[0]
    for k in range(ROWS):
        cut = slice(k * HD, (k + 1) * HD)
        total = (a[:, cut] + b[:, cut]) + (c[:, cut] + d[:, cut])
        out[pl.ds(k, n, stride=ROWS), :] = total


def queries_kernel(place, parts, cosine, sine, q_out, new_score, new_value):
    n = parts.shape[0] // ROWS
    total = parts[:ROWS]
    for k in range(1, n):
        total = total + parts[k * ROWS : (k + 1) * ROWS]
    lead = total[: GROUP + 1]
    mine = pl.ds(place[1], 1)
    turned = lead * cosine[mine] + pltpu.roll(lead, HD // 2, 1) * sine[mine]
    turned = turned.astype(BF16)
    q = turned[:GROUP]
    q_out[...] = jnp.broadcast_to(q[None], q_out.shape)
    key = turned[GROUP : GROUP + 1].astype(F32)
    score = jnp.sum(q.astype(F32) * key, axis=1, keepdims=True) * SCALE
    new_score[...] = as_row(score, diagonal(GROUP))
    new_value[...] = total[GROUP + 1 :].astype(BF16).astype(F32)


def visible_kernel(local, place, lengths, q, out):
    del q
    index = lax.broadcasted_iota(jnp.int32, (1, out.shape[1]), 1)
    position = index % local
    for k, (j, d) in enumerate(MOVES):
        core = 1 - place[2] if d else place[2]
        block = (lax.rem(place[0] + (NX - j), NX) * NZ + place[1]) * NC + core
        position = jnp.where(index // local == k, position + block * local, position)
    for b in range(out.shape[0]):
        out[b : b + 1] = (position < lengths[b]).astype(F32)


def attend_kernel(place, slabs, seen, q, *refs):
    caches, out, scores, weights = refs[: len(MOVES)], *refs[len(MOVES) :]
    n = q.shape[0]
    head = place[0] * NC + place[2]
    mask = diagonal(GROUP)
    for b in range(n):
        slab = slabs[head, b]
        keys = jnp.concatenate([cache[slab, 0] for cache in caches], axis=0)
        scores[b * GROUP : (b + 1) * GROUP] = SCALE * lax.dot_general(
            q[b], keys, (((1,), (1,)), ((), ())), preferred_element_type=F32
        )
    for b in range(n):
        rows = slice(b * GROUP, (b + 1) * GROUP)
        visible = seen[b : b + 1] > 0
        score = jnp.where(visible, scores[rows], NEG)
        top = jnp.max(score, axis=1, keepdims=True)
        weight = jnp.where(visible, jnp.exp(score - top), 0.0)
        total = jnp.sum(weight, axis=1, keepdims=True)
        weights[rows] = weight.astype(BF16)
        at = b * ROWS + GROUP
        out[at : at + 1] = as_row(top, mask)
        out[at + 1 : at + 2] = as_row(total, mask)
    for b in range(n):
        slab = slabs[head, b]
        values = jnp.concatenate([cache[slab, 1] for cache in caches], axis=0)
        out[b * ROWS : b * ROWS + GROUP] = jnp.dot(
            weights[b * GROUP : (b + 1) * GROUP], values, preferred_element_type=F32
        )


def combine_kernel(parts, new_score, new_value, out):
    n = parts.shape[0] // ROWS
    mask = diagonal(GROUP)
    lanes = lax.broadcasted_iota(jnp.int32, (1, HD), 1) < GROUP
    tops = parts[pl.ds(GROUP, n, stride=ROWS), :]
    totals = parts[pl.ds(GROUP + 1, n, stride=ROWS), :]
    fresh = new_score[...]
    top = jnp.maximum(jnp.max(tops, axis=0, keepdims=True), fresh)
    share = jnp.where(lanes, jnp.exp(tops - top), 0.0)
    fresh_weight = jnp.where(lanes, jnp.exp(fresh - top), 0.0)
    total = jnp.sum(share * totals, axis=0, keepdims=True) + fresh_weight
    weighted = column(fresh_weight, mask).astype(BF16).astype(F32) * new_value[...]
    for k in range(n):
        at = k * ROWS
        weighted = weighted + column(share[k : k + 1], mask) * parts[at : at + GROUP]
    done = (weighted / column(total, mask)).astype(BF16)
    out[...] = jnp.broadcast_to(done[None], out.shape)


def rows_kernel(heads, out, wide):
    wide[...] = heads[...].astype(F32)
    for k in range(GROUP):
        out[:, k * HD : (k + 1) * HD] = wide[:, k, :].astype(BF16)


def output_near_kernel(place, a, b, wo, x, out, w_far, w, sems, far_sems):
    near = out_copies(place, NEAR, wo, w, sems)
    far = out_copies(place, FAR, wo, w_far, far_sems)
    for copy in near + far:
        copy.start()
    for copy in near:
        copy.wait()
    total = x[...].astype(F32)
    for k, rows in enumerate((a, b)):
        total = total + jnp.dot(rows[...], w[k], preferred_element_type=F32)
    out[...] = total
    for copy in far:
        copy.wait()


def output_far_kernel(*refs):
    near, *rows, w, out = refs
    total = near[...]
    for k, block in enumerate(rows):
        total = total + jnp.dot(block[...], w[k], preferred_element_type=F32)
    out[...] = total.astype(BF16)


def shift_x(value, by):
    return lax.ppermute(value, "x", [(i, (i + by) % NX) for i in range(NX)])


def swap_c(value):
    return lax.ppermute(value, "c", [(0, 1), (1, 0)])


def across_z(value):
    return lax.all_to_all(value, "z", 0, 0, tiled=True)


def step(hidden_in, norm_gain, w_q, w_kv, w_o, kv_cache, lengths, slab_index):
    n, depth = hidden_in.shape
    w_q, w_kv, w_o, kv_cache = (
        pltpu.with_memory_space_constraint(v, pltpu.HBM) for v in (w_q, w_kv, w_o, kv_cache)
    )
    place = jnp.stack([lax.axis_index(a) for a in TENSOR]).astype(jnp.int32)

    lane = jnp.arange(HD, dtype=jnp.int32)[None]
    frequency = ROPE_BASE ** (-2.0 * (lane % (HD // 2)).astype(F32) / HD)
    angles = lengths.astype(F32)[:, None] * frequency
    cosine = jnp.cos(angles)
    sine = jnp.sin(angles) * jnp.where(lane < HD // 2, -1.0, 1.0)

    line = struct((1, HD), F32)
    own = call(squares_kernel, line, [VMEM], hidden_in, params=None)
    lines = [own]
    for k in (1, 3, 2):
        lines.append(shift_x(own, k))
    sums = call(spread_kernel, struct((NZ * NC, HD), F32), [VMEM] * NX, *lines)
    sums = lax.all_to_all(
        sums.reshape(NZ * NC, 1, HD), ("z", "c"), 0, 0, tiled=True
    ).reshape(NZ * NC, HD)

    dmas = lambda moves: pltpu.SemaphoreType.DMA((len(moves), 3))
    held = call(
        fetch_in_kernel,
        struct((len(FIRST), depth, PW), BF16),
        [SMEM, HBM, HBM],
        place,
        w_q,
        w_kv,
        scratch=[dmas(FIRST)],
    )

    cache = []
    for moves, staged in ((MOVES[:EARLY], range(1, EARLY)), (MOVES[EARLY:], ())):
        block = kv_cache.shape[1:]
        cache += call(
            functools.partial(fetch_cache_kernel, moves, staged),
            [
                pltpu.HBM(block, BF16) if k in staged else struct(block, BF16)
                for k in range(len(moves))
            ],
            [SMEM, HBM],
            place,
            kv_cache,
            scratch=[
                pltpu.VMEM((len(moves),) + block, BF16),
                pltpu.SemaphoreType.DMA((len(moves),)),
                pltpu.SemaphoreType.DMA((len(moves),)),
            ],
        )

    local = kv_cache.shape[3]
    seen = len(MOVES) * local
    product = struct((NX, n, PW), F32)
    normed, sent = call(
        project_first_kernel,
        [struct((n, depth), BF16), product],
        [VMEM] * 4,
        sums,
        hidden_in,
        norm_gain[None],
        held,
    )
    got = swap_c(sent)
    kept = call(
        project_kernel,
        product,
        [SMEM, VMEM, HBM, HBM],
        place,
        normed,
        w_q,
        w_kv,
        scratch=[pltpu.VMEM((len(REST), depth, PW), BF16), dmas(REST)],
    )
    blocks = call(pair_sum_kernel, [struct((n, PW), F32)] * NX, [VMEM] * 2, kept, got)
    parts = [blocks[0]]
    for k in (1, 3, 2):
        parts.append(shift_x(blocks[k], k))
    rows = call(x_sum_kernel, struct((n * ROWS, HD), F32), [VMEM] * NX, *parts)
    for k, (j, d) in enumerate(MOVES[1:], 1):
        pairs = [
            (x * NC + c, (x + j) % NX * NC + (c + d) % NC)
            for x in range(NX)
            for c in range(NC)
        ]
        cache[k] = lax.ppermute(cache[k], ("x", "c"), pairs)
    rows = across_z(rows.reshape(n, 1, PW)).reshape(n * ROWS, HD)
    q, new_score, new_value = call(
        queries_kernel,
        [struct((n, GROUP, HD), BF16), struct((1, HD), F32), struct((1, HD), F32)],
        [SMEM] + [VMEM] * 3,
        place,
        rows,
        cosine,
        sine,
    )
    q = across_z(q)

    visible = call(
        functools.partial(visible_kernel, local),
        struct((n, seen), F32),
        [SMEM, SMEM, VMEM],
        place,
        lengths,
        q,
    )
    partial = call(
        attend_kernel,
        struct((n * ROWS, HD), F32),
        [SMEM, SMEM] + [VMEM] * (2 + len(MOVES)),
        place,
        slab_index,
        visible,
        q,
        *cache,
        scratch=[pltpu.VMEM((n * GROUP, seen), F32), pltpu.VMEM((n * GROUP, seen), BF16)],
    )
    partial = across_z(partial.reshape(n, 1, PW)).reshape(n * ROWS, HD)
    done = call(
        combine_kernel, struct((n, GROUP, HD), BF16), [VMEM] * 3, partial, new_score, new_value
    )
    done = across_z(done)
    done = call(
        rows_kernel,
        struct((n, QW), BF16),
        [VMEM],
        done,
        scratch=[pltpu.VMEM((n, GROUP, HD), F32)],
    )
    rows = {(0, 0): done}
    for k in (1, 3, 2):
        rows[k, 0] = shift_x(done, -k)
    for k in (0, 1, 3, 2):
        rows[k, 1] = swap_c(rows[k, 0])
    total, w_far = call(
        output_near_kernel,
        [struct((n, depth), F32), struct((len(FAR), QW, w_o.shape[1]), BF16)],
        [SMEM, VMEM, VMEM, HBM, VMEM],
        place,
        *(rows[move] for move in NEAR),
        w_o,
        hidden_in,
        scratch=[
            pltpu.VMEM((len(NEAR), QW, w_o.shape[1]), BF16),
            pltpu.SemaphoreType.DMA((len(NEAR),)),
            pltpu.SemaphoreType.DMA((len(FAR),)),
        ],
    )
    return call(
        output_far_kernel,
        struct((n, depth), BF16),
        [VMEM] * (2 + len(FAR)),
        total,
        *(rows[move] for move in FAR),
        w_far,
    )


def solution(mesh):
    torus = Mesh(
        mesh.devices.reshape(mesh.shape["groups"], NX, NZ, NC),
        ("groups",) + TENSOR,
    )
    placed = (
        P("groups", TENSOR),
        P(TENSOR),
        P(TENSOR, None),
        P(TENSOR, None),
        P(None, TENSOR),
        P(None, "groups", None, TENSOR, None),
        P("groups"),
        P(None, "groups"),
    )
    return jax.shard_map(
        step, mesh=torus, in_specs=placed, out_specs=P("groups", TENSOR), check_vma=False
    )
```

```python
import functools

import jax
import jax.numpy as jnp
from jax import lax
from jax.experimental import pallas as pl
from jax.experimental.pallas import tpu as pltpu
from jax.sharding import Mesh
from jax.sharding import PartitionSpec as P

NX, NZ, NC = 4, 16, 2
KVH = NX * NC
HD = 128
GROUP = 16
ROWS = GROUP + 2
QW = GROUP * HD
PW = ROWS * HD
MODEL = KVH * QW
TENSOR = ("x", "z", "c")
FIRST = ((0, 1), (1, 1), (2, 1), (3, 1))
REST = ((0, 0), (1, 0), (2, 0), (3, 0))
NEAR = ((0, 0),)
LAST = ((0, 1),)
FAR = ((1, 0), (3, 0), (2, 0), (1, 1), (3, 1), (2, 1))
MOVES = ((1, 0), (3, 0), (2, 0), (1, 1), (3, 1), (2, 1), (0, 1), (0, 0))
EARLY = 2

EPS = 1e-05
ROPE_BASE = 500000.0
SCALE = 1.0 / HD**0.5
NEG = -1e30


F32, BF16 = jnp.float32, jnp.bfloat16
VMEM = pl.BlockSpec(memory_space=pltpu.VMEM)
SMEM = pl.BlockSpec(memory_space=pltpu.SMEM)
HBM = pl.BlockSpec(memory_space=pltpu.HBM)
LIMIT = pltpu.CompilerParams(vmem_limit_bytes=16 * 2**20)


def struct(shape, dtype):
    return jax.ShapeDtypeStruct(shape, dtype)


def call(kernel, out, specs, *args, scratch=()):
    one = lambda v: HBM if getattr(v, "memory_space", None) == pltpu.HBM else VMEM
    outs = [one(v) for v in out] if isinstance(out, list) else one(out)
    return pl.pallas_call(
        kernel,
        in_specs=specs,
        out_specs=outs,
        out_shape=out,
        scratch_shapes=scratch,
        compiler_params=LIMIT,
    )(*args)


def diagonal(rows):
    lane = lax.broadcasted_iota(jnp.int32, (rows, HD), 1)
    return lane == lax.broadcasted_iota(jnp.int32, (rows, HD), 0)


def column(row, mask):
    return jnp.sum(jnp.where(mask, row, 0.0), axis=1, keepdims=True)


def as_row(col, mask):
    return jnp.sum(jnp.where(mask, col, 0.0), axis=0, keepdims=True)


def squares_kernel(x, out):
    stream = x[...].astype(F32)
    total = jnp.sum(stream * stream, axis=1, keepdims=True)
    out[...] = as_row(total, diagonal(x.shape[0]))


def spread_kernel(a, b, c, d, out):
    out[...] = jnp.broadcast_to((a[...] + b[...]) + (c[...] + d[...]), out.shape)


def head_of(j, d):
    my_x, my_c = lax.axis_index("x"), lax.axis_index("c")
    return lax.rem(my_x + j, NX) * NC + (1 - my_c if d else my_c)


def in_copies(moves, wq, wkv, out, sems):
    copies = []
    for k, (j, d) in enumerate(moves):
        head = head_of(j, d)
        for part, (source, start, width, at) in enumerate(
            (
                (wq, head * QW, QW, 0),
                (wkv, head * HD, HD, QW),
                (wkv, (KVH + head) * HD, HD, QW + HD),
            )
        ):
            copies.append(
                pltpu.make_async_copy(
                    source.at[:, pl.ds(pl.multiple_of(start, HD), width)],
                    out.at[k, :, pl.ds(at, width)],
                    sems.at[k, part],
                )
            )
    return copies


def out_copies(moves, wo, out, sems):
    return [
        pltpu.make_async_copy(
            wo.at[pl.ds(pl.multiple_of(head_of(j, d) * QW, HD), QW)],
            out.at[k],
            sems.at[k],
        )
        for k, (j, d) in enumerate(moves)
    ]


def run_all(copies):
    for copy in copies:
        copy.start()
    for copy in copies:
        copy.wait()


def fetch_in_kernel(wq, wkv, out, sems):
    run_all(in_copies(FIRST, wq, wkv, out, sems))


def fetch_cache_kernel(moves, staged, cache, *refs):
    outs, held, sems, out_sems = refs[:-3], *refs[-3:]
    first, second = [], []
    for k, (j, d) in enumerate(moves):
        to = held.at[k] if k in staged else outs[k]
        first.append(pltpu.make_async_copy(cache.at[head_of(j, d)], to, sems.at[k]))
        first[k].start()
    for k in range(len(moves)):
        first[k].wait()
        if k in staged:
            second.append(pltpu.make_async_copy(held.at[k], outs[k], out_sems.at[k]))
            second[-1].start()
    for copy in second:
        copy.wait()


def project_first_kernel(sums, x, gain, w, normed_out, out):
    squares = column(jnp.sum(sums[...], axis=0, keepdims=True), diagonal(x.shape[0]))
    stream = x[...].astype(F32)
    normed = (stream * lax.rsqrt(squares / MODEL + EPS) * gain[...].astype(F32)).astype(BF16)
    normed_out[...] = normed
    for k in range(NX):
        out[k] = jnp.dot(normed, w[k], preferred_element_type=F32)


def project_kernel(normed, wq, wkv, out, w, sems):
    copies = in_copies(REST, wq, wkv, w, sems)
    for copy in copies:
        copy.start()
    for k in range(NX):
        for copy in copies[3 * k : 3 * k + 3]:
            copy.wait()
        out[k] = jnp.dot(normed[...], w[k], preferred_element_type=F32)


def pair_sum_kernel(a, b, *outs):
    for k, out in enumerate(outs):
        out[...] = a[k] + b[k]


def x_sum_kernel(a, b, c, d, out):
    n = a.shape[0]
    for k in range(ROWS):
        cut = slice(k * HD, (k + 1) * HD)
        total = (a[:, cut] + b[:, cut]) + (c[:, cut] + d[:, cut])
        out[pl.ds(k, n, stride=ROWS), :] = total


def queries_kernel(parts, cosine, sine, q_out, new_score, new_value):
    n = parts.shape[0] // ROWS
    total = parts[:ROWS]
    for k in range(1, n):
        total = total + parts[k * ROWS : (k + 1) * ROWS]
    lead = total[: GROUP + 1]
    turned = lead * cosine[...] + pltpu.roll(lead, HD // 2, 1) * sine[...]
    turned = turned.astype(BF16)
    q = turned[:GROUP]
    q_out[...] = jnp.broadcast_to(q[None], q_out.shape)
    key = turned[GROUP : GROUP + 1].astype(F32)
    score = jnp.sum(q.astype(F32) * key, axis=1, keepdims=True) * SCALE
    new_score[...] = as_row(score, diagonal(GROUP))
    new_value[...] = total[GROUP + 1 :].astype(BF16).astype(F32)


def hold_kernel(q, out):
    out[...] = q[...]


def attend_kernel(lengths, slabs, q, *refs):
    caches, out, scores, weights = refs[: len(MOVES)], *refs[len(MOVES) :]
    n = q.shape[0]
    local = caches[0].shape[2]
    my_x, my_z, my_c = (lax.axis_index(a) for a in TENSOR)
    head = my_x * NC + my_c
    index = lax.broadcasted_iota(jnp.int32, (1, len(MOVES) * local), 1)
    position = index % local
    for k, (j, d) in enumerate(MOVES):
        core = 1 - my_c if d else my_c
        block = (lax.rem(my_x + (NX - j), NX) * NZ + my_z) * NC + core
        position = jnp.where(index // local == k, position + block * local, position)
    mask = diagonal(GROUP)
    for b in range(n):
        slab = slabs[head, b]
        keys = jnp.concatenate([cache[slab, 0] for cache in caches], axis=0)
        scores[b * GROUP : (b + 1) * GROUP] = SCALE * lax.dot_general(
            q[b], keys, (((1,), (1,)), ((), ())), preferred_element_type=F32
        )
    for b in range(n):
        rows = slice(b * GROUP, (b + 1) * GROUP)
        visible = position < lengths[b]
        score = jnp.where(visible, scores[rows], NEG)
        top = jnp.max(score, axis=1, keepdims=True)
        weight = jnp.where(visible, jnp.exp(score - top), 0.0)
        total = jnp.sum(weight, axis=1, keepdims=True)
        weights[rows] = weight.astype(BF16)
        at = b * ROWS + GROUP
        out[at : at + 1] = as_row(top, mask)
        out[at + 1 : at + 2] = as_row(total, mask)
    for b in range(n):
        slab = slabs[head, b]
        values = jnp.concatenate([cache[slab, 1] for cache in caches], axis=0)
        out[b * ROWS : b * ROWS + GROUP] = jnp.dot(
            weights[b * GROUP : (b + 1) * GROUP], values, preferred_element_type=F32
        )


def combine_kernel(parts, new_score, new_value, out):
    n = parts.shape[0] // ROWS
    mask = diagonal(GROUP)
    lanes = lax.broadcasted_iota(jnp.int32, (1, HD), 1) < GROUP
    tops = parts[pl.ds(GROUP, n, stride=ROWS), :]
    totals = parts[pl.ds(GROUP + 1, n, stride=ROWS), :]
    fresh = new_score[...]
    top = jnp.maximum(jnp.max(tops, axis=0, keepdims=True), fresh)
    share = jnp.where(lanes, jnp.exp(tops - top), 0.0)
    fresh_weight = jnp.where(lanes, jnp.exp(fresh - top), 0.0)
    total = jnp.sum(share * totals, axis=0, keepdims=True) + fresh_weight
    weighted = column(fresh_weight, mask).astype(BF16).astype(F32) * new_value[...]
    for k in range(n):
        at = k * ROWS
        weighted = weighted + column(share[k : k + 1], mask) * parts[at : at + GROUP]
    done = (weighted / column(total, mask)).astype(BF16)
    out[...] = jnp.broadcast_to(done[None], out.shape)


def rows_kernel(heads, out, wide):
    wide[...] = heads[...].astype(F32)
    for k in range(GROUP):
        out[:, k * HD : (k + 1) * HD] = wide[:, k, :].astype(BF16)


def output_near_kernel(rows, wo, x, out, w_far, w, sem, far_sems):
    near = out_copies(NEAR, wo, w, sem)
    far = out_copies(FAR, wo, w_far, far_sems)
    for copy in near + far:
        copy.start()
    for copy in near:
        copy.wait()
    out[...] = x[...].astype(F32) + jnp.dot(rows[...], w[0], preferred_element_type=F32)
    for copy in far:
        copy.wait()


def output_far_kernel(near, *refs):
    rows, (last, w_far, wo, out, w, sem) = refs[: len(FAR)], refs[len(FAR) :]
    copies = out_copies(LAST, wo, w, sem)
    copies[0].start()
    total = near[...]
    for k, block in enumerate(rows):
        total = total + jnp.dot(block[...], w_far[k], preferred_element_type=F32)
    copies[0].wait()
    total = total + jnp.dot(last[...], w[0], preferred_element_type=F32)
    out[...] = total.astype(BF16)


def shift_x(value, by):
    return lax.ppermute(value, "x", [(i, (i + by) % NX) for i in range(NX)])


def swap_c(value):
    return lax.ppermute(value, "c", [(0, 1), (1, 0)])


def across_z(value):
    return lax.all_to_all(value, "z", 0, 0, tiled=True)


def step(hidden_in, norm_gain, w_q, w_kv, w_o, kv_cache, lengths, slab_index):
    n, depth = hidden_in.shape
    w_q, w_kv, w_o, kv_cache = (
        pltpu.with_memory_space_constraint(v, pltpu.HBM) for v in (w_q, w_kv, w_o, kv_cache)
    )

    lane = jnp.arange(HD, dtype=jnp.int32)[None]
    frequency = ROPE_BASE ** (-2.0 * (lane % (HD // 2)).astype(F32) / HD)
    angles = lengths.astype(F32)[:, None] * frequency
    mine = jnp.arange(n, dtype=jnp.int32)[:, None] == lax.axis_index("z")
    chosen = lambda table: jnp.sum(jnp.where(mine, table, 0.0), axis=0, keepdims=True)
    cosine = chosen(jnp.cos(angles))
    sine = chosen(jnp.sin(angles) * jnp.where(lane < HD // 2, -1.0, 1.0))

    line = struct((1, HD), F32)
    own = call(squares_kernel, line, [VMEM], hidden_in)
    lines = [own]
    for k in (1, 3, 2):
        lines.append(shift_x(own, k))
    sums = call(spread_kernel, struct((NZ * NC, HD), F32), [VMEM] * NX, *lines)
    sums = lax.all_to_all(
        sums.reshape(NZ * NC, 1, HD), ("z", "c"), 0, 0, tiled=True
    ).reshape(NZ * NC, HD)

    dmas = lambda moves: pltpu.SemaphoreType.DMA((len(moves), 3))
    held = call(
        fetch_in_kernel,
        struct((len(FIRST), depth, PW), BF16),
        [HBM, HBM],
        w_q,
        w_kv,
        scratch=[dmas(FIRST)],
    )

    cache = []
    for moves, staged in ((MOVES[:EARLY], range(EARLY)), (MOVES[EARLY:], ())):
        block = kv_cache.shape[1:]
        cache += call(
            functools.partial(fetch_cache_kernel, moves, staged),
            [
                pltpu.HBM(block, BF16) if k in staged else struct(block, BF16)
                for k in range(len(moves))
            ],
            [HBM],
            kv_cache,
            scratch=[
                pltpu.VMEM((len(moves),) + block, BF16),
                pltpu.SemaphoreType.DMA((len(moves),)),
                pltpu.SemaphoreType.DMA((len(moves),)),
            ],
        )

    local = kv_cache.shape[3]
    seen = len(MOVES) * local
    product = struct((NX, n, PW), F32)
    normed, sent = call(
        project_first_kernel,
        [struct((n, depth), BF16), pltpu.VMEM((NX, n, PW), F32)],
        [VMEM] * 4,
        sums,
        hidden_in,
        norm_gain[None],
        held,
    )
    got = swap_c(sent)
    kept = call(
        project_kernel,
        product,
        [VMEM, HBM, HBM],
        normed,
        w_q,
        w_kv,
        scratch=[pltpu.VMEM((len(REST), depth, PW), BF16), dmas(REST)],
    )
    blocks = call(pair_sum_kernel, [struct((n, PW), F32)] * NX, [VMEM] * 2, kept, got)
    parts = [blocks[0]]
    for k in (1, 3, 2):
        parts.append(shift_x(blocks[k], k))
    rows = call(x_sum_kernel, struct((n * ROWS, HD), F32), [VMEM] * NX, *parts)
    for k, (j, d) in enumerate(MOVES[:-1]):
        pairs = [
            (x * NC + c, (x + j) % NX * NC + (c + d) % NC)
            for x in range(NX)
            for c in range(NC)
        ]
        cache[k] = lax.ppermute(cache[k], ("x", "c"), pairs)
    rows = across_z(rows.reshape(n, 1, PW)).reshape(n * ROWS, HD)
    q, new_score, new_value = call(
        queries_kernel,
        [struct((n, GROUP, HD), BF16), struct((1, HD), F32), struct((1, HD), F32)],
        [VMEM] * 3,
        rows,
        cosine,
        sine,
    )
    q = across_z(q)

    q = call(hold_kernel, struct(q.shape, BF16), [VMEM], q)
    partial = call(
        attend_kernel,
        struct((n * ROWS, HD), F32),
        [SMEM, SMEM] + [VMEM] * (1 + len(MOVES)),
        lengths,
        slab_index,
        q,
        *cache,
        scratch=[pltpu.VMEM((n * GROUP, seen), F32), pltpu.VMEM((n * GROUP, seen), BF16)],
    )
    partial = across_z(partial.reshape(n, 1, PW)).reshape(n * ROWS, HD)
    done = call(
        combine_kernel, struct((n, GROUP, HD), BF16), [VMEM] * 3, partial, new_score, new_value
    )
    done = across_z(done)
    done = call(
        rows_kernel,
        struct((n, QW), BF16),
        [VMEM],
        done,
        scratch=[pltpu.VMEM((n, GROUP, HD), F32)],
    )
    rows = {(0, 0): done}
    for k in (1, 3, 2):
        rows[k, 0] = shift_x(done, -k)
    for k in (0, 1, 3, 2):
        rows[k, 1] = swap_c(rows[k, 0])
    block = (QW, w_o.shape[1])
    read = [pltpu.VMEM((1,) + block, BF16), pltpu.SemaphoreType.DMA((1,))]
    total, w_far = call(
        output_near_kernel,
        [struct((n, depth), F32), struct((len(FAR),) + block, BF16)],
        [VMEM, HBM, VMEM],
        rows[0, 0],
        w_o,
        hidden_in,
        scratch=read + [pltpu.SemaphoreType.DMA((len(FAR),))],
    )
    return call(
        output_far_kernel,
        struct((n, depth), BF16),
        [VMEM] * (3 + len(FAR)) + [HBM],
        total,
        *(rows[move] for move in FAR),
        rows[0, 1],
        w_far,
        w_o,
        scratch=read,
    )


def solution(mesh):
    torus = Mesh(
        mesh.devices.reshape(mesh.shape["groups"], NX, NZ, NC),
        ("groups",) + TENSOR,
    )
    placed = (
        P("groups", TENSOR),
        P(TENSOR),
        P(TENSOR, None),
        P(TENSOR, None),
        P(None, TENSOR),
        P(None, "groups", None, TENSOR, None),
        P("groups"),
        P(None, "groups"),
    )
    return jax.shard_map(
        step, mesh=torus, in_specs=placed, out_specs=P("groups", TENSOR), check_vma=False
    )
```

```python
import functools

import jax
import jax.numpy as jnp
from jax import lax
from jax.experimental import pallas as pl
from jax.experimental.pallas import tpu as pltpu
from jax.sharding import Mesh
from jax.sharding import PartitionSpec as P

NX, NZ, NC = 4, 16, 2
KVH = NX * NC
HD = 128
GROUP = 16
ROWS = GROUP + 2
QW = GROUP * HD
PW = ROWS * HD
MODEL = KVH * QW
TENSOR = ("x", "z", "c")
FIRST = ((0, 1), (1, 1), (2, 1), (3, 1))
REST = ((0, 0), (1, 0), (2, 0), (3, 0))
NEAR = ((0, 0), (0, 1))
FAR = ((1, 0), (3, 0), (2, 0), (1, 1), (3, 1), (2, 1))
MOVES = ((0, 1), (1, 0), (3, 0), (2, 0), (1, 1), (3, 1), (2, 1), (0, 0))
EARLY = 3

EPS = 1e-05
ROPE_BASE = 500000.0
SCALE = 1.0 / HD**0.5
NEG = -1e30


F32, BF16 = jnp.float32, jnp.bfloat16
VMEM = pl.BlockSpec(memory_space=pltpu.VMEM)
SMEM = pl.BlockSpec(memory_space=pltpu.SMEM)
HBM = pl.BlockSpec(memory_space=pltpu.HBM)
LIMIT = pltpu.CompilerParams(vmem_limit_bytes=16 * 2**20)


def struct(shape, dtype):
    return jax.ShapeDtypeStruct(shape, dtype)


def call(kernel, out, specs, *args, scratch=()):
    one = lambda v: HBM if getattr(v, "memory_space", None) == pltpu.HBM else VMEM
    outs = [one(v) for v in out] if isinstance(out, list) else one(out)
    return pl.pallas_call(
        kernel,
        in_specs=specs,
        out_specs=outs,
        out_shape=out,
        scratch_shapes=scratch,
        compiler_params=LIMIT,
    )(*args)


def diagonal(rows):
    lane = lax.broadcasted_iota(jnp.int32, (rows, HD), 1)
    return lane == lax.broadcasted_iota(jnp.int32, (rows, HD), 0)


def column(row, mask):
    return jnp.sum(jnp.where(mask, row, 0.0), axis=1, keepdims=True)


def as_row(col, mask):
    return jnp.sum(jnp.where(mask, col, 0.0), axis=0, keepdims=True)


def squares_kernel(x, out):
    stream = x[...].astype(F32)
    total = jnp.sum(stream * stream, axis=1, keepdims=True)
    out[...] = as_row(total, diagonal(x.shape[0]))


def spread_kernel(a, b, c, d, out):
    out[...] = jnp.broadcast_to((a[...] + b[...]) + (c[...] + d[...]), out.shape)


def head_of(j, d):
    my_x, my_c = lax.axis_index("x"), lax.axis_index("c")
    return lax.rem(my_x + j, NX) * NC + (1 - my_c if d else my_c)


def in_copies(moves, wq, wkv, out, sems):
    copies = []
    for k, (j, d) in enumerate(moves):
        head = head_of(j, d)
        for part, (source, start, width, at) in enumerate(
            (
                (wq, head * QW, QW, 0),
                (wkv, head * HD, HD, QW),
                (wkv, (KVH + head) * HD, HD, QW + HD),
            )
        ):
            copies.append(
                pltpu.make_async_copy(
                    source.at[:, pl.ds(pl.multiple_of(start, HD), width)],
                    out.at[k, :, pl.ds(at, width)],
                    sems.at[k, part],
                )
            )
    return copies


def out_copies(moves, wo, out, sems):
    return [
        pltpu.make_async_copy(
            wo.at[pl.ds(pl.multiple_of(head_of(j, d) * QW, HD), QW)],
            out.at[k],
            sems.at[k],
        )
        for k, (j, d) in enumerate(moves)
    ]


def run_all(copies):
    for copy in copies:
        copy.start()
    for copy in copies:
        copy.wait()


def fetch_in_kernel(wq, wkv, out, sems):
    run_all(in_copies(FIRST, wq, wkv, out, sems))


def fetch_cache_kernel(moves, staged, cache, *refs):
    outs, held, sems, out_sems = refs[:-3], *refs[-3:]
    first, second = [], []
    for k, (j, d) in enumerate(moves):
        to = held.at[k] if k in staged else outs[k]
        first.append(pltpu.make_async_copy(cache.at[head_of(j, d)], to, sems.at[k]))
        first[k].start()
    for k in range(len(moves)):
        first[k].wait()
        if k in staged:
            second.append(pltpu.make_async_copy(held.at[k], outs[k], out_sems.at[k]))
            second[-1].start()
    for copy in second:
        copy.wait()


def project_first_kernel(sums, x, gain, w, normed_out, out):
    squares = column(jnp.sum(sums[...], axis=0, keepdims=True), diagonal(x.shape[0]))
    stream = x[...].astype(F32)
    normed = (stream * lax.rsqrt(squares / MODEL + EPS) * gain[...].astype(F32)).astype(BF16)
    normed_out[...] = normed
    for k in range(NX):
        out[k] = jnp.dot(normed, w[k], preferred_element_type=F32)


def project_kernel(normed, wq, wkv, out, w, sems):
    copies = in_copies(REST, wq, wkv, w, sems)
    for copy in copies:
        copy.start()
    for k in range(NX):
        for copy in copies[3 * k : 3 * k + 3]:
            copy.wait()
        out[k] = jnp.dot(normed[...], w[k], preferred_element_type=F32)


def pair_sum_kernel(a, b, *outs):
    for k, out in enumerate(outs):
        out[...] = a[k] + b[k]


def x_sum_kernel(a, b, c, d, out):
    n = a.shape[0]
    for k in range(ROWS):
        cut = slice(k * HD, (k + 1) * HD)
        total = (a[:, cut] + b[:, cut]) + (c[:, cut] + d[:, cut])
        out[pl.ds(k, n, stride=ROWS), :] = total


def queries_kernel(parts, cosine, sine, q_out, new_score, new_value):
    n = parts.shape[0] // ROWS
    total = parts[:ROWS]
    for k in range(1, n):
        total = total + parts[k * ROWS : (k + 1) * ROWS]
    lead = total[: GROUP + 1]
    turned = lead * cosine[...] + pltpu.roll(lead, HD // 2, 1) * sine[...]
    turned = turned.astype(BF16)
    q = turned[:GROUP]
    q_out[...] = jnp.broadcast_to(q[None], q_out.shape)
    key = turned[GROUP : GROUP + 1].astype(F32)
    score = jnp.sum(q.astype(F32) * key, axis=1, keepdims=True) * SCALE
    new_score[...] = as_row(score, diagonal(GROUP))
    new_value[...] = total[GROUP + 1 :].astype(BF16).astype(F32)


def hold_kernel(q, out):
    out[...] = q[...]


def attend_kernel(lengths, slabs, q, *refs):
    caches, out, scores, weights = refs[: len(MOVES)], *refs[len(MOVES) :]
    n = q.shape[0]
    local = caches[0].shape[2]
    my_x, my_z, my_c = (lax.axis_index(a) for a in TENSOR)
    head = my_x * NC + my_c
    index = lax.broadcasted_iota(jnp.int32, (1, len(MOVES) * local), 1)
    position = index % local
    for k, (j, d) in enumerate(MOVES):
        core = 1 - my_c if d else my_c
        block = (lax.rem(my_x + (NX - j), NX) * NZ + my_z) * NC + core
        position = jnp.where(index // local == k, position + block * local, position)
    mask = diagonal(GROUP)
    for b in range(n):
        slab = slabs[head, b]
        keys = jnp.concatenate([cache[slab, 0] for cache in caches], axis=0)
        scores[b * GROUP : (b + 1) * GROUP] = SCALE * lax.dot_general(
            q[b], keys, (((1,), (1,)), ((), ())), preferred_element_type=F32
        )
    for b in range(n):
        rows = slice(b * GROUP, (b + 1) * GROUP)
        visible = position < lengths[b]
        score = jnp.where(visible, scores[rows], NEG)
        top = jnp.max(score, axis=1, keepdims=True)
        weight = jnp.where(visible, jnp.exp(score - top), 0.0)
        total = jnp.sum(weight, axis=1, keepdims=True)
        weights[rows] = weight.astype(BF16)
        at = b * ROWS + GROUP
        out[at : at + 1] = as_row(top, mask)
        out[at + 1 : at + 2] = as_row(total, mask)
    for b in range(n):
        slab = slabs[head, b]
        values = jnp.concatenate([cache[slab, 1] for cache in caches], axis=0)
        out[b * ROWS : b * ROWS + GROUP] = jnp.dot(
            weights[b * GROUP : (b + 1) * GROUP], values, preferred_element_type=F32
        )


def combine_kernel(parts, new_score, new_value, out):
    n = parts.shape[0] // ROWS
    mask = diagonal(GROUP)
    lanes = lax.broadcasted_iota(jnp.int32, (1, HD), 1) < GROUP
    tops = parts[pl.ds(GROUP, n, stride=ROWS), :]
    totals = parts[pl.ds(GROUP + 1, n, stride=ROWS), :]
    fresh = new_score[...]
    top = jnp.maximum(jnp.max(tops, axis=0, keepdims=True), fresh)
    share = jnp.where(lanes, jnp.exp(tops - top), 0.0)
    fresh_weight = jnp.where(lanes, jnp.exp(fresh - top), 0.0)
    total = jnp.sum(share * totals, axis=0, keepdims=True) + fresh_weight
    weighted = column(fresh_weight, mask).astype(BF16).astype(F32) * new_value[...]
    for k in range(n):
        at = k * ROWS
        weighted = weighted + column(share[k : k + 1], mask) * parts[at : at + GROUP]
    done = (weighted / column(total, mask)).astype(BF16)
    out[...] = jnp.broadcast_to(done[None], out.shape)


def rows_kernel(heads, out, wide):
    wide[...] = heads[...].astype(F32)
    for k in range(GROUP):
        out[:, k * HD : (k + 1) * HD] = wide[:, k, :].astype(BF16)


def output_near_kernel(a, b, wo, x, out, w_far, w, sems, far_sems):
    near = out_copies(NEAR, wo, w, sems)
    far = out_copies(FAR, wo, w_far, far_sems)
    for copy in near + far:
        copy.start()
    for copy in near:
        copy.wait()
    total = x[...].astype(F32)
    for k, rows in enumerate((a, b)):
        total = total + jnp.dot(rows[...], w[k], preferred_element_type=F32)
    out[...] = total
    for copy in far:
        copy.wait()


def output_far_kernel(*refs):
    near, *rows, w, out = refs
    total = near[...]
    for k, block in enumerate(rows):
        total = total + jnp.dot(block[...], w[k], preferred_element_type=F32)
    out[...] = total.astype(BF16)


def shift_x(value, by):
    return lax.ppermute(value, "x", [(i, (i + by) % NX) for i in range(NX)])


def swap_c(value):
    return lax.ppermute(value, "c", [(0, 1), (1, 0)])


def across_z(value):
    return lax.all_to_all(value, "z", 0, 0, tiled=True)


def step(hidden_in, norm_gain, w_q, w_kv, w_o, kv_cache, lengths, slab_index):
    n, depth = hidden_in.shape
    w_q, w_kv, w_o, kv_cache = (
        pltpu.with_memory_space_constraint(v, pltpu.HBM) for v in (w_q, w_kv, w_o, kv_cache)
    )

    lane = jnp.arange(HD, dtype=jnp.int32)[None]
    frequency = ROPE_BASE ** (-2.0 * (lane % (HD // 2)).astype(F32) / HD)
    angles = lengths.astype(F32)[:, None] * frequency
    mine = jnp.arange(n, dtype=jnp.int32)[:, None] == lax.axis_index("z")
    chosen = lambda table: jnp.sum(jnp.where(mine, table, 0.0), axis=0, keepdims=True)
    cosine = chosen(jnp.cos(angles))
    sine = chosen(jnp.sin(angles) * jnp.where(lane < HD // 2, -1.0, 1.0))

    line = struct((1, HD), F32)
    own = call(squares_kernel, line, [VMEM], hidden_in)
    lines = [own]
    for k in (1, 3, 2):
        lines.append(shift_x(own, k))
    sums = call(spread_kernel, struct((NZ * NC, HD), F32), [VMEM] * NX, *lines)
    sums = lax.all_to_all(
        sums.reshape(NZ * NC, 1, HD), ("z", "c"), 0, 0, tiled=True
    ).reshape(NZ * NC, HD)

    dmas = lambda moves: pltpu.SemaphoreType.DMA((len(moves), 3))
    held = call(
        fetch_in_kernel,
        struct((len(FIRST), depth, PW), BF16),
        [HBM, HBM],
        w_q,
        w_kv,
        scratch=[dmas(FIRST)],
    )

    cache = []
    for moves, staged in ((MOVES[:EARLY], range(EARLY)), (MOVES[EARLY:], ())):
        block = kv_cache.shape[1:]
        cache += call(
            functools.partial(fetch_cache_kernel, moves, staged),
            [
                pltpu.HBM(block, BF16) if k in staged else struct(block, BF16)
                for k in range(len(moves))
            ],
            [HBM],
            kv_cache,
            scratch=[
                pltpu.VMEM((len(moves),) + block, BF16),
                pltpu.SemaphoreType.DMA((len(moves),)),
                pltpu.SemaphoreType.DMA((len(moves),)),
            ],
        )

    local = kv_cache.shape[3]
    seen = len(MOVES) * local
    product = struct((NX, n, PW), F32)
    normed, sent = call(
        project_first_kernel,
        [struct((n, depth), BF16), product],
        [VMEM] * 4,
        sums,
        hidden_in,
        norm_gain[None],
        held,
    )
    got = swap_c(sent)
    kept = call(
        project_kernel,
        product,
        [VMEM, HBM, HBM],
        normed,
        w_q,
        w_kv,
        scratch=[pltpu.VMEM((len(REST), depth, PW), BF16), dmas(REST)],
    )
    blocks = call(pair_sum_kernel, [struct((n, PW), F32)] * NX, [VMEM] * 2, kept, got)
    parts = [blocks[0]]
    for k in (1, 3, 2):
        parts.append(shift_x(blocks[k], k))
    rows = call(x_sum_kernel, struct((n * ROWS, HD), F32), [VMEM] * NX, *parts)
    for k, (j, d) in enumerate(MOVES[:-1]):
        pairs = [
            (x * NC + c, (x + j) % NX * NC + (c + d) % NC)
            for x in range(NX)
            for c in range(NC)
        ]
        cache[k] = lax.ppermute(cache[k], ("x", "c"), pairs)
    rows = across_z(rows.reshape(n, 1, PW)).reshape(n * ROWS, HD)
    q, new_score, new_value = call(
        queries_kernel,
        [struct((n, GROUP, HD), BF16), struct((1, HD), F32), struct((1, HD), F32)],
        [VMEM] * 3,
        rows,
        cosine,
        sine,
    )
    q = across_z(q)

    q = call(hold_kernel, struct(q.shape, BF16), [VMEM], q)
    partial = call(
        attend_kernel,
        struct((n * ROWS, HD), F32),
        [SMEM, SMEM] + [VMEM] * (1 + len(MOVES)),
        lengths,
        slab_index,
        q,
        *cache,
        scratch=[pltpu.VMEM((n * GROUP, seen), F32), pltpu.VMEM((n * GROUP, seen), BF16)],
    )
    partial = across_z(partial.reshape(n, 1, PW)).reshape(n * ROWS, HD)
    done = call(
        combine_kernel, struct((n, GROUP, HD), BF16), [VMEM] * 3, partial, new_score, new_value
    )
    done = across_z(done)
    done = call(
        rows_kernel,
        struct((n, QW), BF16),
        [VMEM],
        done,
        scratch=[pltpu.VMEM((n, GROUP, HD), F32)],
    )
    rows = {(0, 0): done}
    for k in (1, 3, 2):
        rows[k, 0] = shift_x(done, -k)
    for k in (0, 1, 3, 2):
        rows[k, 1] = swap_c(rows[k, 0])
    total, w_far = call(
        output_near_kernel,
        [struct((n, depth), F32), struct((len(FAR), QW, w_o.shape[1]), BF16)],
        [VMEM, VMEM, HBM, VMEM],
        *(rows[move] for move in NEAR),
        w_o,
        hidden_in,
        scratch=[
            pltpu.VMEM((len(NEAR), QW, w_o.shape[1]), BF16),
            pltpu.SemaphoreType.DMA((len(NEAR),)),
            pltpu.SemaphoreType.DMA((len(FAR),)),
        ],
    )
    return call(
        output_far_kernel,
        struct((n, depth), BF16),
        [VMEM] * (2 + len(FAR)),
        total,
        *(rows[move] for move in FAR),
        w_far,
    )


def solution(mesh):
    torus = Mesh(
        mesh.devices.reshape(mesh.shape["groups"], NX, NZ, NC),
        ("groups",) + TENSOR,
    )
    placed = (
        P("groups", TENSOR),
        P(TENSOR),
        P(TENSOR, None),
        P(TENSOR, None),
        P(None, TENSOR),
        P(None, "groups", None, TENSOR, None),
        P("groups"),
        P(None, "groups"),
    )
    return jax.shard_map(
        step, mesh=torus, in_specs=placed, out_specs=P("groups", TENSOR), check_vma=False
    )
```

```python
import functools

import jax
import jax.numpy as jnp
from jax import lax
from jax.experimental import pallas as pl
from jax.experimental.pallas import tpu as pltpu
from jax.sharding import Mesh
from jax.sharding import PartitionSpec as P

NX, NZ, NC = 4, 16, 2
KVH = NX * NC
HD = 128
GROUP = 16
ROWS = GROUP + 2
QW = GROUP * HD
PW = ROWS * HD
MODEL = KVH * QW
TENSOR = ("x", "z", "c")
FIRST = ((0, 1), (1, 1), (2, 1), (3, 1))
REST = ((0, 0), (1, 0), (2, 0), (3, 0))
NEAR = ((0, 0), (0, 1))
FAR = ((1, 0), (3, 0), (2, 0), (1, 1), (3, 1), (2, 1))
MOVES = ((1, 0), (3, 0), (2, 0), (2, 1), (1, 1), (3, 1), (0, 1), (0, 0))
EARLY = 2

EPS = 1e-05
ROPE_BASE = 500000.0
SCALE = 1.0 / HD**0.5
NEG = -1e30


F32, BF16 = jnp.float32, jnp.bfloat16
VMEM = pl.BlockSpec(memory_space=pltpu.VMEM)
SMEM = pl.BlockSpec(memory_space=pltpu.SMEM)
HBM = pl.BlockSpec(memory_space=pltpu.HBM)
LIMIT = pltpu.CompilerParams(vmem_limit_bytes=16 * 2**20)


def struct(shape, dtype):
    return jax.ShapeDtypeStruct(shape, dtype)


def call(kernel, out, specs, *args, scratch=()):
    one = lambda v: HBM if getattr(v, "memory_space", None) == pltpu.HBM else VMEM
    outs = [one(v) for v in out] if isinstance(out, list) else one(out)
    return pl.pallas_call(
        kernel,
        in_specs=specs,
        out_specs=outs,
        out_shape=out,
        scratch_shapes=scratch,
        compiler_params=LIMIT,
    )(*args)


def diagonal(rows):
    lane = lax.broadcasted_iota(jnp.int32, (rows, HD), 1)
    return lane == lax.broadcasted_iota(jnp.int32, (rows, HD), 0)


def column(row, mask):
    return jnp.sum(jnp.where(mask, row, 0.0), axis=1, keepdims=True)


def as_row(col, mask):
    return jnp.sum(jnp.where(mask, col, 0.0), axis=0, keepdims=True)


def squares_kernel(x, out):
    stream = x[...].astype(F32)
    total = jnp.sum(stream * stream, axis=1, keepdims=True)
    out[...] = as_row(total, diagonal(x.shape[0]))


def spread_kernel(a, b, c, d, out):
    out[...] = jnp.broadcast_to((a[...] + b[...]) + (c[...] + d[...]), out.shape)


def head_of(j, d):
    my_x, my_c = lax.axis_index("x"), lax.axis_index("c")
    return lax.rem(my_x + j, NX) * NC + (1 - my_c if d else my_c)


def in_copies(moves, wq, wkv, out, sems):
    copies = []
    for k, (j, d) in enumerate(moves):
        head = head_of(j, d)
        for part, (source, start, width, at) in enumerate(
            (
                (wq, head * QW, QW, 0),
                (wkv, head * HD, HD, QW),
                (wkv, (KVH + head) * HD, HD, QW + HD),
            )
        ):
            copies.append(
                pltpu.make_async_copy(
                    source.at[:, pl.ds(pl.multiple_of(start, HD), width)],
                    out.at[k, :, pl.ds(at, width)],
                    sems.at[k, part],
                )
            )
    return copies


def out_copies(moves, wo, out, sems):
    return [
        pltpu.make_async_copy(
            wo.at[pl.ds(pl.multiple_of(head_of(j, d) * QW, HD), QW)],
            out.at[k],
            sems.at[k],
        )
        for k, (j, d) in enumerate(moves)
    ]


def run_all(copies):
    for copy in copies:
        copy.start()
    for copy in copies:
        copy.wait()


def fetch_in_kernel(wq, wkv, out, sems):
    run_all(in_copies(FIRST, wq, wkv, out, sems))


def fetch_cache_kernel(moves, staged, cache, *refs):
    outs, held, sems, out_sems = refs[:-3], *refs[-3:]
    first, second = [], []
    for k, (j, d) in enumerate(moves):
        to = held.at[k] if k in staged else outs[k]
        first.append(pltpu.make_async_copy(cache.at[head_of(j, d)], to, sems.at[k]))
        first[k].start()
    for k in range(len(moves)):
        first[k].wait()
        if k in staged:
            second.append(pltpu.make_async_copy(held.at[k], outs[k], out_sems.at[k]))
            second[-1].start()
    for copy in second:
        copy.wait()


def project_first_kernel(sums, x, gain, w, normed_out, out):
    squares = column(jnp.sum(sums[...], axis=0, keepdims=True), diagonal(x.shape[0]))
    stream = x[...].astype(F32)
    normed = (stream * lax.rsqrt(squares / MODEL + EPS) * gain[...].astype(F32)).astype(BF16)
    normed_out[...] = normed
    for k in range(NX):
        out[k] = jnp.dot(normed, w[k], preferred_element_type=F32)


def project_kernel(normed, wq, wkv, out, w, sems):
    copies = in_copies(REST, wq, wkv, w, sems)
    for copy in copies:
        copy.start()
    for k in range(NX):
        for copy in copies[3 * k : 3 * k + 3]:
            copy.wait()
        out[k] = jnp.dot(normed[...], w[k], preferred_element_type=F32)


def pair_sum_kernel(a, b, *outs):
    for k, out in enumerate(outs):
        out[...] = a[k] + b[k]


def x_sum_kernel(a, b, c, d, out):
    n = a.shape[0]
    for k in range(ROWS):
        cut = slice(k * HD, (k + 1) * HD)
        total = (a[:, cut] + b[:, cut]) + (c[:, cut] + d[:, cut])
        out[pl.ds(k, n, stride=ROWS), :] = total


def queries_kernel(parts, cosine, sine, q_out, new_score, new_value):
    n = parts.shape[0] // ROWS
    total = parts[:ROWS]
    for k in range(1, n):
        total = total + parts[k * ROWS : (k + 1) * ROWS]
    lead = total[: GROUP + 1]
    turned = lead * cosine[...] + pltpu.roll(lead, HD // 2, 1) * sine[...]
    turned = turned.astype(BF16)
    q = turned[:GROUP]
    q_out[...] = jnp.broadcast_to(q[None], q_out.shape)
    key = turned[GROUP : GROUP + 1].astype(F32)
    score = jnp.sum(q.astype(F32) * key, axis=1, keepdims=True) * SCALE
    new_score[...] = as_row(score, diagonal(GROUP))
    new_value[...] = total[GROUP + 1 :].astype(BF16).astype(F32)


def hold_kernel(q, out):
    out[...] = q[...]


def attend_kernel(lengths, slabs, q, *refs):
    caches, out, scores, weights = refs[: len(MOVES)], *refs[len(MOVES) :]
    n = q.shape[0]
    local = caches[0].shape[2]
    my_x, my_z, my_c = (lax.axis_index(a) for a in TENSOR)
    head = my_x * NC + my_c
    index = lax.broadcasted_iota(jnp.int32, (1, len(MOVES) * local), 1)
    position = index % local
    for k, (j, d) in enumerate(MOVES):
        core = 1 - my_c if d else my_c
        block = (lax.rem(my_x + (NX - j), NX) * NZ + my_z) * NC + core
        position = jnp.where(index // local == k, position + block * local, position)
    mask = diagonal(GROUP)
    for b in range(n):
        slab = slabs[head, b]
        keys = jnp.concatenate([cache[slab, 0] for cache in caches], axis=0)
        scores[b * GROUP : (b + 1) * GROUP] = SCALE * lax.dot_general(
            q[b], keys, (((1,), (1,)), ((), ())), preferred_element_type=F32
        )
    for b in range(n):
        rows = slice(b * GROUP, (b + 1) * GROUP)
        visible = position < lengths[b]
        score = jnp.where(visible, scores[rows], NEG)
        top = jnp.max(score, axis=1, keepdims=True)
        weight = jnp.where(visible, jnp.exp(score - top), 0.0)
        total = jnp.sum(weight, axis=1, keepdims=True)
        weights[rows] = weight.astype(BF16)
        at = b * ROWS + GROUP
        out[at : at + 1] = as_row(top, mask)
        out[at + 1 : at + 2] = as_row(total, mask)
    for b in range(n):
        slab = slabs[head, b]
        values = jnp.concatenate([cache[slab, 1] for cache in caches], axis=0)
        out[b * ROWS : b * ROWS + GROUP] = jnp.dot(
            weights[b * GROUP : (b + 1) * GROUP], values, preferred_element_type=F32
        )


def combine_kernel(parts, new_score, new_value, out):
    n = parts.shape[0] // ROWS
    mask = diagonal(GROUP)
    lanes = lax.broadcasted_iota(jnp.int32, (1, HD), 1) < GROUP
    tops = parts[pl.ds(GROUP, n, stride=ROWS), :]
    totals = parts[pl.ds(GROUP + 1, n, stride=ROWS), :]
    fresh = new_score[...]
    top = jnp.maximum(jnp.max(tops, axis=0, keepdims=True), fresh)
    share = jnp.where(lanes, jnp.exp(tops - top), 0.0)
    fresh_weight = jnp.where(lanes, jnp.exp(fresh - top), 0.0)
    total = jnp.sum(share * totals, axis=0, keepdims=True) + fresh_weight
    weighted = column(fresh_weight, mask).astype(BF16).astype(F32) * new_value[...]
    for k in range(n):
        at = k * ROWS
        weighted = weighted + column(share[k : k + 1], mask) * parts[at : at + GROUP]
    done = (weighted / column(total, mask)).astype(BF16)
    out[...] = jnp.broadcast_to(done[None], out.shape)


def rows_kernel(heads, out, wide):
    wide[...] = heads[...].astype(F32)
    for k in range(GROUP):
        out[:, k * HD : (k + 1) * HD] = wide[:, k, :].astype(BF16)


def output_near_kernel(a, b, wo, x, out, w_far, w, sems, far_sems):
    near = out_copies(NEAR, wo, w, sems)
    far = out_copies(FAR, wo, w_far, far_sems)
    for copy in near + far:
        copy.start()
    for copy in near:
        copy.wait()
    total = x[...].astype(F32)
    for k, rows in enumerate((a, b)):
        total = total + jnp.dot(rows[...], w[k], preferred_element_type=F32)
    out[...] = total
    for copy in far:
        copy.wait()


def output_far_kernel(*refs):
    near, *rows, w, out = refs
    total = near[...]
    for k, block in enumerate(rows):
        total = total + jnp.dot(block[...], w[k], preferred_element_type=F32)
    out[...] = total.astype(BF16)


def shift_x(value, by):
    return lax.ppermute(value, "x", [(i, (i + by) % NX) for i in range(NX)])


def swap_c(value):
    return lax.ppermute(value, "c", [(0, 1), (1, 0)])


def across_z(value):
    return lax.all_to_all(value, "z", 0, 0, tiled=True)


def step(hidden_in, norm_gain, w_q, w_kv, w_o, kv_cache, lengths, slab_index):
    n, depth = hidden_in.shape
    w_q, w_kv, w_o, kv_cache = (
        pltpu.with_memory_space_constraint(v, pltpu.HBM) for v in (w_q, w_kv, w_o, kv_cache)
    )

    lane = jnp.arange(HD, dtype=jnp.int32)[None]
    frequency = ROPE_BASE ** (-2.0 * (lane % (HD // 2)).astype(F32) / HD)
    angles = lengths.astype(F32)[:, None] * frequency
    mine = jnp.arange(n, dtype=jnp.int32)[:, None] == lax.axis_index("z")
    chosen = lambda table: jnp.sum(jnp.where(mine, table, 0.0), axis=0, keepdims=True)
    cosine = chosen(jnp.cos(angles))
    sine = chosen(jnp.sin(angles) * jnp.where(lane < HD // 2, -1.0, 1.0))

    line = struct((1, HD), F32)
    own = call(squares_kernel, line, [VMEM], hidden_in)
    lines = [own]
    for k in (1, 3, 2):
        lines.append(shift_x(own, k))
    sums = call(spread_kernel, struct((NZ * NC, HD), F32), [VMEM] * NX, *lines)
    sums = lax.all_to_all(
        sums.reshape(NZ * NC, 1, HD), ("z", "c"), 0, 0, tiled=True
    ).reshape(NZ * NC, HD)

    dmas = lambda moves: pltpu.SemaphoreType.DMA((len(moves), 3))
    held = call(
        fetch_in_kernel,
        struct((len(FIRST), depth, PW), BF16),
        [HBM, HBM],
        w_q,
        w_kv,
        scratch=[dmas(FIRST)],
    )

    cache = []
    for moves, staged in ((MOVES[:EARLY], range(EARLY)), (MOVES[EARLY:], ())):
        block = kv_cache.shape[1:]
        cache += call(
            functools.partial(fetch_cache_kernel, moves, staged),
            [
                pltpu.HBM(block, BF16) if k in staged else struct(block, BF16)
                for k in range(len(moves))
            ],
            [HBM],
            kv_cache,
            scratch=[
                pltpu.VMEM((len(moves),) + block, BF16),
                pltpu.SemaphoreType.DMA((len(moves),)),
                pltpu.SemaphoreType.DMA((len(moves),)),
            ],
        )

    local = kv_cache.shape[3]
    seen = len(MOVES) * local
    product = struct((NX, n, PW), F32)
    normed, sent = call(
        project_first_kernel,
        [struct((n, depth), BF16), pltpu.VMEM((NX, n, PW), F32)],
        [VMEM] * 4,
        sums,
        hidden_in,
        norm_gain[None],
        held,
    )
    got = swap_c(sent)
    kept = call(
        project_kernel,
        product,
        [VMEM, HBM, HBM],
        normed,
        w_q,
        w_kv,
        scratch=[pltpu.VMEM((len(REST), depth, PW), BF16), dmas(REST)],
    )
    blocks = call(pair_sum_kernel, [struct((n, PW), F32)] * NX, [VMEM] * 2, kept, got)
    parts = [blocks[0]]
    for k in (1, 3, 2):
        parts.append(shift_x(blocks[k], k))
    rows = call(x_sum_kernel, struct((n * ROWS, HD), F32), [VMEM] * NX, *parts)
    for k, (j, d) in enumerate(MOVES[:-1]):
        pairs = [
            (x * NC + c, (x + j) % NX * NC + (c + d) % NC)
            for x in range(NX)
            for c in range(NC)
        ]
        cache[k] = lax.ppermute(cache[k], ("x", "c"), pairs)
    rows = across_z(rows.reshape(n, 1, PW)).reshape(n * ROWS, HD)
    q, new_score, new_value = call(
        queries_kernel,
        [struct((n, GROUP, HD), BF16), struct((1, HD), F32), struct((1, HD), F32)],
        [VMEM] * 3,
        rows,
        cosine,
        sine,
    )
    q = across_z(q)

    q = call(hold_kernel, struct(q.shape, BF16), [VMEM], q)
    partial = call(
        attend_kernel,
        struct((n * ROWS, HD), F32),
        [SMEM, SMEM] + [VMEM] * (1 + len(MOVES)),
        lengths,
        slab_index,
        q,
        *cache,
        scratch=[pltpu.VMEM((n * GROUP, seen), F32), pltpu.VMEM((n * GROUP, seen), BF16)],
    )
    partial = across_z(partial.reshape(n, 1, PW)).reshape(n * ROWS, HD)
    done = call(
        combine_kernel, struct((n, GROUP, HD), BF16), [VMEM] * 3, partial, new_score, new_value
    )
    done = across_z(done)
    done = call(
        rows_kernel,
        struct((n, QW), BF16),
        [VMEM],
        done,
        scratch=[pltpu.VMEM((n, GROUP, HD), F32)],
    )
    rows = {(0, 0): done}
    for k in (1, 3, 2):
        rows[k, 0] = shift_x(done, -k)
    for k in (0, 1, 3, 2):
        rows[k, 1] = swap_c(rows[k, 0])
    total, w_far = call(
        output_near_kernel,
        [struct((n, depth), F32), struct((len(FAR), QW, w_o.shape[1]), BF16)],
        [VMEM, VMEM, HBM, VMEM],
        *(rows[move] for move in NEAR),
        w_o,
        hidden_in,
        scratch=[
            pltpu.VMEM((len(NEAR), QW, w_o.shape[1]), BF16),
            pltpu.SemaphoreType.DMA((len(NEAR),)),
            pltpu.SemaphoreType.DMA((len(FAR),)),
        ],
    )
    return call(
        output_far_kernel,
        struct((n, depth), BF16),
        [VMEM] * (2 + len(FAR)),
        total,
        *(rows[move] for move in FAR),
        w_far,
    )


def solution(mesh):
    torus = Mesh(
        mesh.devices.reshape(mesh.shape["groups"], NX, NZ, NC),
        ("groups",) + TENSOR,
    )
    placed = (
        P("groups", TENSOR),
        P(TENSOR),
        P(TENSOR, None),
        P(TENSOR, None),
        P(None, TENSOR),
        P(None, "groups", None, TENSOR, None),
        P("groups"),
        P(None, "groups"),
    )
    return jax.shard_map(
        step, mesh=torus, in_specs=placed, out_specs=P("groups", TENSOR), check_vma=False
    )
```
